128 devices in a mesh: ka: 4 (over x_lo, core), rows: 32 (over x_hi, y, z).
Axes of the slice: x: 4 (x_hi: 2, x_lo: 2; x = x_hi * 2 + x_lo), y: 4, z: 4, core: 2. Of those that a mesh axis runs over, the one named last changes fastest.
Arguments:
- hoppings: bfloat16 [32, 384, 128, 128], P('rows', 'ka'), may hold values from -0.046875 to 0.046875
- tile_rows: int32 [32, 384], P('rows', 'ka'), may hold values from 0 to 95, as said below
- tile_cols: int32 [32, 384], P('rows', 'ka'), may hold values from 0 to 95, as said below
- tile_lats: int32 [32, 384], P('rows', 'ka'), may hold values from 0 to 8
- tile_counts: int32 [32, 4], P('rows', 'ka'), may hold values from 48 to 96, as said below
- phase_angle: float32 [8, 9], P('ka'), may hold values from -3.140625 to 3.140625
- vectors: bfloat16 [8, 2, 12288, 256], P('ka', None, 'rows'), may hold values from -6 to 6
Outputs:
- bloch_product: float32 [8, 2, 12288, 256], P('ka', None, 'rows')
The draws below stay inside these ranges and needn't reach their ends.
Inputs may be any that keep to these rules, and one draw needn't show every extreme that they name: `tile_rows`: slots of row block r (first index) hold tile rows r * 3 to (r + 1) * 3 - 1; several slots may name the same block. `tile_cols`: the cyclic distance between a slot's tile column and its tile row is at most 16, and both distances 16 occur in every row block. `tile_counts`: the live slots of a device are the first ones of its part of the list; some device has all 96 live.
All inputs are finite; a program needn't handle non-finite values.
Results may differ from the reference program's by a relative error of at most 0.0029.
Values may be sent and summed in bfloat16 or wider, within the bound.
A program may use at most 128 MiB of HBM per device.

```python
import jax
import jax.numpy as jnp
from jax import lax

TS = 128
TORB = 96
NLAT = 9
BAND = 16
NVEC = 256
TILE_DEV = 96
TR = 3
LISTS = 384
ORB = 12288
KPTS = 8
N_KA = 4
N_ROWS = 32


def tile_coordinates(key):
    folded_rows = jax.random.fold_in(key, 17)
    first_key, second_key = jax.random.split(folded_rows)
    row_position = jax.random.randint(first_key, (N_ROWS, TILE_DEV * N_KA), 0, TR)
    row_position = row_position + (jnp.arange(N_ROWS, dtype=jnp.int32) * TR)[:, None]
    column_step = jax.random.randint(second_key, (N_ROWS, TILE_DEV * N_KA), -BAND, BAND + 1)
    column_step = column_step.at[:, 0].set(BAND).at[:, 1].set(-BAND)
    col_index = jnp.mod(row_position + column_step, TORB)
    return (row_position.astype(jnp.int32), col_index.astype(jnp.int32))


def draw_tile_rows(key, part):
    return tile_coordinates(key)[0]


def draw_tile_cols(key, part):
    return tile_coordinates(key)[1]


def draw_tile_counts(key, part):
    folded_rows = jax.random.fold_in(key, 29)
    first_key, second_key = jax.random.split(folded_rows)
    counts = jax.random.randint(first_key, (N_ROWS * N_KA,), (TILE_DEV + 1) // 2, TILE_DEV + 1)
    full_slot = jax.random.randint(second_key, (), 0, N_ROWS * N_KA)
    counts = counts.at[full_slot].set(TILE_DEV)
    return counts.reshape(N_ROWS, N_KA).astype(jnp.int32)


def plant(result, rng, low, largest):
    longest = result.shape.index(max(result.shape))
    spots = []
    for shift in (0, 1):
        where = [jax.random.randint(jax.random.fold_in(rng, axis), (), 0, length) for axis, length in enumerate(result.shape)]
        where[longest] = (where[longest] + shift) % result.shape[longest]
        spots.append(tuple(where))
    return result.at[spots[0]].set(low).at[spots[1]].set(largest)


def shard_levels(key, extent, cuts, least, high):
    def one(dim, parts):
        steps = jax.random.uniform(jax.random.fold_in(jax.random.fold_in(key, 6), dim), (parts,), jnp.float32, least / len(cuts), high / len(cuts))
        return jnp.repeat(jnp.exp(steps), extent[dim] // parts).reshape((-1,) + (1,) * (len(extent) - dim - 1))

    factor_of = one(*cuts[0])
    for cut in cuts[1:]:
        factor_of = factor_of * one(*cut)
    return factor_of


def centred(rng, dims, spread, most, cuts=(), held_as=jnp.bfloat16):
    result = jax.random.normal(rng, dims, jnp.float32) * spread
    if len(cuts) > 0:
        result = shard_levels(rng, dims, cuts, -0.22, 0.18) * result
    return jnp.clip(result, min=-most, max=most).astype(held_as)


def setup_inputs(seed: int = 0) -> dict:
    streams_of = jax.random.split(jax.random.key(seed), 8)
    return {
        "hoppings": centred(streams_of[0], (N_ROWS, LISTS, TS, TS), (TS * TILE_DEV * N_KA // TR) ** -0.5, 0.046875, ((0, 32), (1, 4))),
        "tile_rows": draw_tile_rows(jax.random.fold_in(streams_of[7], 71), 0),
        "tile_cols": draw_tile_cols(jax.random.fold_in(streams_of[7], 71), 0),
        "tile_lats": plant(jax.random.randint(streams_of[3], (N_ROWS, LISTS), 0, NLAT), jax.random.fold_in(streams_of[3], 1), 0, NLAT - 1).astype(jnp.int32),
        "tile_counts": draw_tile_counts(jax.random.fold_in(streams_of[7], 71), 0),
        "phase_angle": jnp.clip(jax.random.uniform(streams_of[5], (KPTS, NLAT), jnp.float32, -3.140625, 3.140625), -3.140625, 3.140625),
        "vectors": centred(streams_of[6], (KPTS, 2, ORB, NVEC), 1.0, 6.0, ((0, 4), (2, 32))),
    }


def reference(hoppings, tile_rows, tile_cols, tile_lats, tile_counts, phase_angle, vectors):
    list_count = hoppings.shape[1]
    slot_index = jnp.arange(list_count, dtype=jnp.int32)
    live_mask = (slot_index[None, :] % TILE_DEV) < tile_counts[:, slot_index // TILE_DEV]
    live_f32 = live_mask.astype(jnp.float32)
    block_ids = (tile_rows * TORB + tile_cols).astype(jnp.int32)

    def one_point(point_data):
        angles, point_vectors = point_data
        cos_weight = jnp.cos(angles)[tile_lats] * live_f32
        sin_weight = jnp.sin(angles)[tile_lats] * live_f32

        def add_row_block(block, carry):
            real_acc, imag_acc = carry
            tile_block = lax.dynamic_index_in_dim(hoppings, block, 0, keepdims=False).astype(jnp.float32)
            destination_rows = lax.dynamic_index_in_dim(block_ids, block, 0, keepdims=False)
            cos_row = lax.dynamic_index_in_dim(cos_weight, block, 0, keepdims=False)
            sin_row = lax.dynamic_index_in_dim(sin_weight, block, 0, keepdims=False)
            real_acc = real_acc.at[destination_rows].add(cos_row[:, None, None] * tile_block)
            imag_acc = imag_acc.at[destination_rows].add(sin_row[:, None, None] * tile_block)
            return (real_acc, imag_acc)

        empty_blocks = jnp.zeros((TORB * TORB, TS, TS), jnp.float32)
        real_acc, imag_acc = lax.fori_loop(0, N_ROWS, add_row_block, (empty_blocks, empty_blocks))
        matrix = jnp.stack([real_acc, imag_acc]).astype(jnp.bfloat16)
        matrix = lax.optimization_barrier(matrix).astype(jnp.float32).reshape(2, TORB, TORB, TS, TS)
        vector_f32 = point_vectors.astype(jnp.float32).reshape(2, TORB, TS, NVEC)
        product = jnp.einsum('pijab,qjbv->piaqv', matrix, vector_f32, precision=lax.Precision.HIGHEST)
        real_part = product[0, :, :, 0] - product[1, :, :, 1]
        imag_part = product[0, :, :, 1] + product[1, :, :, 0]
        return jnp.stack([real_part, imag_part]).reshape(2, TORB * TS, NVEC)

    return lax.map(one_point, (phase_angle, vectors))
```

```python
import functools

import jax
import jax.numpy as jnp
from jax import lax
from jax.experimental import pallas as pl
from jax.experimental.pallas import tpu as pltpu
from jax.sharding import PartitionSpec as P

MESH = pl.DeviceIdType.MESH
BAND = 16
NLAT = 9
TS = 128
NV = 256
TR = 3
BLK = TR * TS
SLOTS = 96
CHUNKS = 8
PER = SLOTS // CHUNKS
WIDE = 2 * BAND + 1
SPAN = WIDE + TR - 1
TORB = 96
HALVES = (0, 1)


class Net:
    def __init__(self, send_sem, recv_sem):
        self.send_sem, self.recv_sem = send_sem, recv_sem
        self.index, self.sent = {}, []

    def copy(self, name, src, dst, device):
        at = self.index.setdefault(name, len(self.index))
        return pltpu.make_async_remote_copy(
            src_ref=src, dst_ref=dst, send_sem=self.send_sem.at[at], recv_sem=self.recv_sem.at[at],
            device_id=device, device_id_type=MESH,
        )

    def send(self, name, when, src, dst, device):
        copy = self.copy(name, src, dst, device)
        self.sent.append((when, copy))
        guarded(when, copy.start)

    def recv(self, name, when, dst, device):
        guarded(when, self.copy(name, dst, dst, device).wait_recv)

    def finish(self):
        for when, copy in self.sent:
            guarded(when, copy.wait_send)


def guarded(when, action):
    if when is None:
        action()
    else:
        pl.when(when)(action)


def gather_kernel(hop, coords, vec, G, W, C, S, X, E, send_sem, recv_sem, local_sem):
    ka = lax.axis_index("ka")
    row = lax.axis_index("rows")
    xh, y, z = row // 16, (row // 4) % 4, row % 4
    zp, zm, z2 = (z + 1) % 4, (z + 3) % 4, (z + 2) % 4
    yp, ym = (y + 1) % 4, (y + 3) % 4

    def at(h, i, j):
        return (ka, h * 16 + i * 4 + j)

    def along(flip):
        other = (1 - ka % 2) if flip % 2 else ka % 2
        pair = (1 - ka // 2) if flip // 2 else ka // 2
        return (pair * 2 + other, row)

    up_z, down_z, up_y, down_y = at(xh, y, zp), at(xh, y, zm), at(xh, yp, z), at(xh, ym, z)
    mirror = at(1 - xh, y, z)
    peers = [along(1), along(2), along(3), up_z, down_z, up_y, down_y, mirror]
    barrier = pltpu.get_barrier_semaphore()
    for peer in peers:
        pl.semaphore_signal(barrier, inc=1, device_id=peer, device_id_type=MESH)
    first_part = (y == 1) & (z == 1)
    last_part = (y == 2) & (z == 2)
    first_hold = (y == 1) & (z == 0)
    last_hold = (y == 2) & (z == 3)
    part_sender, part_holder = first_part | last_part, first_hold | last_hold
    part_to = at(1 - xh, y, jnp.where(y == 1, 0, 3))
    part_from = at(1 - xh, y, jnp.where(y == 1, 1, 2))

    @pl.when(part_sender)
    def _():
        pl.semaphore_signal(barrier, inc=1, device_id=part_to, device_id_type=MESH)

    @pl.when(part_holder)
    def _():
        pl.semaphore_signal(barrier, inc=1, device_id=part_from, device_id_type=MESH)

    pl.semaphore_wait(barrier, len(peers) + jnp.where(part_sender | part_holder, 1, 0))

    net = Net(send_sem, recv_sem)
    send, recv = net.send, net.recv
    edge = (y == 0) | (y == 3)
    mirrored = edge | part_holder
    low, high = z == 0, z == 3
    rim = low | high
    tail = pl.ds(pl.multiple_of(jnp.where(low, 0, 2 * TS), TS), TS)
    side = pl.ds(pl.multiple_of(jnp.where(y == 1, 0, 2 * TS), TS), TS)
    HEAD, LAST = pl.ds(0, TS), pl.ds(2 * TS, TS)

    local = pltpu.make_async_copy(coords, C.at[0], local_sem)
    local.start()
    for flip in (1, 2, 3):
        send(f"c{flip}", None, coords, C.at[flip], along(flip))
    for h in HALVES:
        send(f"m{h}", mirrored, vec.at[h], S.at[z, h], mirror)
    for h in HALVES:
        send(f"mp{h}", part_sender, vec.at[h, :, side], S.at[z, h, :, side], part_to)

    def z_own(u, h):
        if u < 0:
            send(f"z-{h}", None, vec.at[h], W.at[6 + z - zp, h], up_z)
        else:
            send(f"z+{h}", None, vec.at[h], W.at[6 + z - zm, h], down_z)

    def z_shadow(u, h):
        if u < 0:
            send(f"s-{h}", edge, S.at[z, h], S.at[z, h], up_z)
        else:
            send(f"s+{h}", edge, S.at[z, h], S.at[z, h], down_z)

    member = {0: z, -1: zm, 1: zp, 2: z2}

    def y_copies(u, h, shadow):
        m = member[u]
        dz = m - z
        if shadow:
            src = S.at[m, h]
            down_ok, up_ok = y == 0, y == 3
        else:
            src = vec.at[h] if u == 0 else W.at[6 + dz, h]
            down_ok, up_ok = y > 0, y < 3
        down_dst, up_dst = W.at[10 + dz, h], W.at[2 + dz, h]
        if u == 0:
            send(f"y-{u}{h}", down_ok, src, down_dst, down_y)
            send(f"y+{u}{h}", up_ok, src, up_dst, up_y)
        elif u == -1:
            send(f"y-{u}{h}", down_ok & (z != 0), src, down_dst, down_y)
            send(f"y+{u}{h}", up_ok, src, up_dst, up_y)
        elif u == 1:
            send(f"y-{u}{h}", down_ok, src, down_dst, down_y)
            send(f"y+{u}{h}", up_ok & (z != 3), src, up_dst, up_y)
        else:
            send(f"y-{u}{h}", down_ok & (z >= 2), src, down_dst, down_y)
            send(f"y-{u}{h}", down_ok & (z < 2), src.at[:, HEAD], down_dst.at[:, HEAD], down_y)
            send(f"y+{u}{h}", up_ok & (z < 2), src, up_dst, up_y)
            send(f"y+{u}{h}", up_ok & (z >= 2), src.at[:, LAST], up_dst.at[:, LAST], up_y)

    def y_arrived(u, h):
        dz = member[u] - z
        down_dst, up_dst = W.at[10 + dz, h], W.at[2 + dz, h]
        if u == 2:
            recv(f"y-{u}{h}", z >= 2, down_dst, up_y)
            recv(f"y-{u}{h}", z < 2, down_dst.at[:, HEAD], up_y)
            recv(f"y+{u}{h}", z < 2, up_dst, down_y)
            recv(f"y+{u}{h}", z >= 2, up_dst.at[:, LAST], down_y)
        else:
            recv(f"y-{u}{h}", (z != 0) if u == -1 else None, down_dst, up_y)
            recv(f"y+{u}{h}", (z != 3) if u == 1 else None, up_dst, down_y)

    z_own(-1, 0)
    z_own(1, 1)
    for h in HALVES:
        y_copies(0, h, False)
    for c in range(CHUNKS):
        part = pl.ds(c * PER, PER)
        send(f"x{c}", None, hop.at[part], G.at[1, part], along(2))
    send("sib", None, hop, G.at[0], along(1))

    recv("m0", mirrored, S.at[z, 0], mirror)
    z_shadow(-1, 0)
    z_own(-1, 1)
    z_own(1, 0)
    z_shadow(1, 0)
    y_copies(0, 0, True)
    recv("z-0", None, W.at[6 + zm - z, 0], down_z)
    send("w0", None, W.at[6 + zm - z, 0], W.at[6 + zm - zp, 0], up_z)
    y_copies(-1, 0, False)
    recv("z+1", None, W.at[6 + zp - z, 1], up_z)
    send("w1", None, W.at[6 + zp - z, 1], W.at[6 + zp - zm, 1], down_z)
    y_copies(1, 1, False)
    y_near = jnp.where(low, ym, yp)
    near = at(xh, y_near, z)
    near_src = at(xh, jnp.where(low, yp, ym), z)
    hold = jnp.where(y == 1, 0, 3)
    hold_part = jnp.where(y == 1, 1, 2)
    hold_to = at(xh, jnp.where(y == 1, 0, 3), z)
    hold_from = at(xh, jnp.where(y == 0, 1, 2), z)
    relay_rim = ((y == 0) & low) | ((y == 3) & high)
    real_rim = (low & (y > 0)) | (high & (y < 3))
    send("e0", part_holder, S.at[hold, 0], E.at[0, 0], hold_to)

    recv("m1", mirrored, S.at[z, 1], mirror)
    z_shadow(1, 1)
    z_shadow(-1, 1)
    y_copies(0, 1, True)
    send("e1", part_holder, S.at[hold, 1], E.at[0, 1], hold_to)
    recv("z-1", None, W.at[6 + zm - z, 1], down_z)
    y_copies(-1, 1, False)
    recv("z+0", None, W.at[6 + zp - z, 0], up_z)
    y_copies(1, 0, False)
    for h in HALVES:
        recv(f"mp{h}", part_holder, S.at[hold_part, h, :, side], part_from)
        send(f"ep{h}", part_holder, S.at[hold_part, h, :, side], E.at[1, h, :, side], hold_to)

    block = jnp.where(low, 10, 2)
    beside = jnp.where(low, 11, 1)
    for h in HALVES:
        y_arrived(0, h)
        send(f"d{h}", real_rim, W.at[block, h], X.at[0, h], near)
    recv("w0", None, W.at[6 + z2 - z, 0], down_z)
    y_copies(2, 0, False)
    recv("w1", None, W.at[6 + z2 - z, 1], up_z)
    y_copies(2, 1, False)
    recv("s-0", edge, S.at[zm, 0], down_z)
    send("v0", edge, S.at[zm, 0], S.at[zm, 0], up_z)
    y_copies(-1, 0, True)
    recv("s+0", edge, S.at[zp, 0], up_z)
    y_copies(1, 0, True)
    for h in HALVES:
        recv(f"e{h}", relay_rim, E.at[0, h], hold_from)
        send(f"d{h}", relay_rim, E.at[0, h], X.at[0, h], near)
    recv("s+1", edge, S.at[zp, 1], up_z)
    send("v1", edge, S.at[zp, 1], S.at[zp, 1], down_z)
    y_copies(1, 1, True)
    recv("s-1", edge, S.at[zm, 1], down_z)
    y_copies(-1, 1, True)
    for h in HALVES:
        recv(f"ep{h}", relay_rim, E.at[1, h, :, tail], hold_from)
        send(f"dp{h}", relay_rim, E.at[1, h, :, tail], X.at[1, h, :, tail], near)
    rim_to = at(xh, y, jnp.where(low, 3, 0))
    far = jnp.where(low, 11, 1)
    far_part = jnp.where(low, 12, 0)
    for h in HALVES:
        recv(f"d{h}", rim, X.at[0, h], near_src)
        send(f"f{h}", rim, X.at[0, h], W.at[far, h], rim_to)
    for h in HALVES:
        y_arrived(1, h)
        y_arrived(-1, h)
        send(f"dp{h}", real_rim, W.at[beside, h, :, tail], X.at[1, h, :, tail], near)
    recv("v0", edge, S.at[z2, 0], down_z)
    y_copies(2, 0, True)
    recv("v1", edge, S.at[z2, 1], up_z)
    y_copies(2, 1, True)

    def forward(c):
        part = pl.ds(c * PER, PER)
        recv(f"x{c}", None, G.at[1, part], along(2))
        send(f"o{c}", None, G.at[1, part], G.at[2, part], along(1))

    for c in range(3):
        forward(c)
    for h in HALVES:
        recv(f"dp{h}", rim, X.at[1, h, :, tail], near_src)
        send(f"fp{h}", rim, X.at[1, h, :, tail], W.at[far_part, h, :, tail], rim_to)
    forward(3)
    got = jnp.where(low, 1, 11)
    got_part = jnp.where(low, 0, 12)
    got_tail = pl.ds(pl.multiple_of(jnp.where(low, 2 * TS, 0), TS), TS)
    next_to = at(xh, y, jnp.where(low, 1, 2))
    for h in HALVES:
        recv(f"f{h}", rim, W.at[got, h], rim_to)
        send(f"l{h}", rim, W.at[got, h, :, got_tail], W.at[got_part, h, :, got_tail], next_to)
    for c in range(4, CHUNKS - 1):
        forward(c)
    inner = (z == 1) | (z == 2)
    inner_part = jnp.where(z == 1, 0, 12)
    inner_tail = pl.ds(pl.multiple_of(jnp.where(z == 1, 2 * TS, 0), TS), TS)
    inner_from = at(xh, y, jnp.where(z == 1, 0, 3))
    for h in HALVES:
        y_arrived(2, h)
        recv(f"fp{h}", rim, W.at[got_part, h, :, got_tail], rim_to)
        recv(f"l{h}", inner, W.at[inner_part, h, :, inner_tail], inner_from)
    for flip in (1, 2, 3):
        recv(f"c{flip}", None, C.at[flip], along(flip))
    recv("sib", None, G.at[0], along(1))
    forward(CHUNKS - 1)
    for c in range(CHUNKS):
        recv(f"o{c}", None, G.at[2, pl.ds(c * PER, PER)], along(1))
    net.finish()
    local.wait()


def gather_all(hop, coords, vec):
    block = vec.shape
    any_space = pl.BlockSpec(memory_space=pl.ANY)
    sems = 80
    return pl.pallas_call(
        gather_kernel,
        out_shape=(
            jax.ShapeDtypeStruct((3,) + hop.shape, hop.dtype),
            jax.ShapeDtypeStruct((13,) + block, vec.dtype),
            jax.ShapeDtypeStruct((4,) + coords.shape, coords.dtype),
            jax.ShapeDtypeStruct((4,) + block, vec.dtype),
            jax.ShapeDtypeStruct((2,) + block, vec.dtype),
            jax.ShapeDtypeStruct((2,) + block, vec.dtype),
        ),
        in_specs=[any_space] * 3,
        out_specs=(any_space,) * 6,
        scratch_shapes=[
            pltpu.SemaphoreType.DMA((sems,)),
            pltpu.SemaphoreType.DMA((sems,)),
            pltpu.SemaphoreType.DMA,
        ],
        compiler_params=pltpu.CompilerParams(collective_id=0, has_side_effects=True),
        name="gather",
    )(hop, coords, vec)[:3]


def product_kernel(C, table, hop, G, vec, W, out, T, V, H, head, chain, sems):
    row = lax.axis_index("rows")
    copies = [pltpu.make_async_copy(hop, T.at[pl.ds(0, SLOTS)], sems.at[0])]
    for m in range(3):
        copies.append(
            pltpu.make_async_copy(G.at[m], T.at[pl.ds((m + 1) * SLOTS, SLOTS)], sems.at[m + 1])
        )
    windows = []
    for j in range(13):
        for q in range(2):
            lanes = pl.ds(q * NV, NV)
            if j == 0:
                src, start, size = W.at[j, :, q, pl.ds(2 * TS, TS)], 0, TS
            elif j == 12:
                src, start, size = W.at[j, :, q, pl.ds(0, TS)], (SPAN - 1) * TS, TS
            else:
                src = vec.at[:, q] if j == 6 else W.at[j, :, q]
                start, size = (TR * (j - 6) + BAND) * TS, BLK
            windows.append(
                pltpu.make_async_copy(src, V.at[:, pl.ds(start, size), lanes], sems.at[4 + 2 * j + q])
            )
    for copy in copies + windows:
        copy.start()

    def clear(b, _):
        head[b] = -1
        return 0

    lax.fori_loop(0, TR * WIDE, clear, 0)
    for m in range(4):

        def link(i, _, m=m):
            r = C[m, 0, i] - row * TR
            w = C[m, 1, i] - (row * TR + r - BAND)
            w = jnp.where(w < 0, w + TORB, w)
            w = jnp.where(w >= TORB, w - TORB, w)
            b = r * WIDE + w
            chain[m * SLOTS + i] = head[b]
            head[b] = m * SLOTS + i
            return 0

        lax.fori_loop(0, C[m, 3, 0], link, 0)
    for copy in copies:
        copy.wait()

    half = TS // 2

    def weights(s, ok):
        m = s // SLOTS
        lat = C[m, 2, s - m * SLOTS]
        return [jnp.where(ok, table[i, lat], 0.0) for i in range(4)]

    for r in range(TR):

        def build(w, _, r=r):
            cols = pl.ds(pl.multiple_of(w * TS, TS), TS)
            first = head[r * WIDE + w]
            for part in range(2):
                rows = pl.ds(part * half, half)

                def step(carry):
                    s, accs = carry[0], carry[1:]
                    s2 = chain[s]
                    ok = s2 >= 0
                    s2 = jnp.where(ok, s2, s)
                    after = jnp.where(ok, chain[s2], -1)
                    one = T[s, rows, :].astype(jnp.float32)
                    two = T[s2, rows, :].astype(jnp.float32)
                    w1, w2 = weights(s, True), weights(s2, ok)
                    return (after,) + tuple(
                        acc + (one * a + two * b) for acc, a, b in zip(accs, w1, w2)
                    )

                zero = jnp.zeros((half, TS), jnp.float32)
                res = lax.while_loop(lambda c: c[0] >= 0, step, (first, zero, zero, zero, zero))
                for k in range(2):
                    for p in range(2):
                        H[k, r, pl.ds(p * TS + part * half, half), cols] = res[1 + 2 * k + p].astype(
                            jnp.bfloat16
                        )
            return 0

        lax.fori_loop(0, WIDE, build, 0)
    for copy in windows:
        copy.wait()
    for k in range(2):
        for r in range(TR):
            o = jnp.dot(
                H[k, r], V[k, pl.ds(r * TS, WIDE * TS), :], preferred_element_type=jnp.float32
            )
            rows = pl.ds(r * TS, TS)
            out[k, 0, rows, :] = o[:TS, :NV] - o[TS:, NV:]
            out[k, 1, rows, :] = o[:TS, NV:] + o[TS:, :NV]


def product(C, table, hop, G, vec, W):
    any_space = pl.BlockSpec(memory_space=pl.ANY)
    smem = pl.BlockSpec(memory_space=pltpu.SMEM)
    return pl.pallas_call(
        product_kernel,
        out_shape=jax.ShapeDtypeStruct((2, 2, BLK, NV), jnp.float32),
        in_specs=[smem, smem] + [any_space] * 4,
        out_specs=pl.BlockSpec(memory_space=pltpu.VMEM),
        scratch_shapes=[
            pltpu.VMEM((4 * SLOTS, TS, TS), jnp.bfloat16),
            pltpu.VMEM((2, SPAN * TS, 2 * NV), jnp.bfloat16),
            pltpu.VMEM((2, TR, 2 * TS, WIDE * TS), jnp.bfloat16),
            pltpu.SMEM((128,), jnp.int32),
            pltpu.SMEM((4 * SLOTS,), jnp.int32),
            pltpu.SemaphoreType.DMA((30,)),
        ],
        compiler_params=pltpu.CompilerParams(vmem_limit_bytes=56 * 1024 * 1024),
        name="product",
    )(C, table, hop, G, vec, W)


def body(hoppings, tile_rows, tile_cols, tile_lats, tile_counts, phase_angle, vectors):
    hop = hoppings[0]
    counts = jnp.broadcast_to(tile_counts, (1, SLOTS))
    coords = jnp.concatenate([tile_rows, tile_cols, tile_lats, counts], axis=0)
    coords = jnp.pad(coords, ((0, 4), (0, 128 - SLOTS)))
    table = jnp.stack([jnp.cos(phase_angle), jnp.sin(phase_angle)], axis=1).reshape(4, NLAT)
    G, W, C = gather_all(hop, coords, vectors)
    return product(C, table, hop, G, vectors, W)


def solution(mesh):
    return jax.shard_map(
        body,
        mesh=mesh,
        in_specs=(
            P("rows", "ka", None, None),
            P("rows", "ka"),
            P("rows", "ka"),
            P("rows", "ka"),
            P("rows", "ka"),
            P("ka", None),
            P("ka", None, "rows", None),
        ),
        out_specs=P("ka", None, "rows", None),
        check_vma=False,
    )
```

```python
import functools

import jax
import jax.numpy as jnp
from jax import lax
from jax.experimental import pallas as pl
from jax.experimental.pallas import tpu as pltpu
from jax.sharding import PartitionSpec as P

MESH = pl.DeviceIdType.MESH
BAND = 16
NLAT = 9
TS = 128
NV = 256
TR = 3
BLK = TR * TS
SLOTS = 96
CHUNKS = 8
PER = SLOTS // CHUNKS
WIDE = 2 * BAND + 1
SPAN = WIDE + TR - 1
TORB = 96
HALVES = (0, 1)


class Net:
    def __init__(self, send_sem, recv_sem):
        self.send_sem, self.recv_sem = send_sem, recv_sem
        self.index, self.sent = {}, []

    def copy(self, name, src, dst, device):
        at = self.index.setdefault(name, len(self.index))
        return pltpu.make_async_remote_copy(
            src_ref=src, dst_ref=dst, send_sem=self.send_sem.at[at], recv_sem=self.recv_sem.at[at],
            device_id=device, device_id_type=MESH,
        )

    def send(self, name, when, src, dst, device):
        copy = self.copy(name, src, dst, device)
        self.sent.append((when, copy))
        guarded(when, copy.start)

    def recv(self, name, when, dst, device):
        guarded(when, self.copy(name, dst, dst, device).wait_recv)

    def finish(self):
        for when, copy in self.sent:
            guarded(when, copy.wait_send)


def guarded(when, action):
    if when is None:
        action()
    else:
        pl.when(when)(action)


def gather_kernel(hop, rows, cols, lats, live, vec, G, W, CR, CC, CL, CN, S, X, E, send_sem, recv_sem, local_sem):
    ka = lax.axis_index("ka")
    row = lax.axis_index("rows")
    xh, y, z = row // 16, (row // 4) % 4, row % 4
    zp, zm, z2 = (z + 1) % 4, (z + 3) % 4, (z + 2) % 4
    yp, ym = (y + 1) % 4, (y + 3) % 4

    def at(h, i, j):
        return (ka, h * 16 + i * 4 + j)

    def along(flip):
        other = (1 - ka % 2) if flip % 2 else ka % 2
        pair = (1 - ka // 2) if flip // 2 else ka // 2
        return (pair * 2 + other, row)

    up_z, down_z, up_y, down_y = at(xh, y, zp), at(xh, y, zm), at(xh, yp, z), at(xh, ym, z)
    mirror = at(1 - xh, y, z)
    peers = [along(1), along(2), along(3), up_z, down_z, up_y, down_y, mirror]
    barrier = pltpu.get_barrier_semaphore()
    for peer in peers:
        pl.semaphore_signal(barrier, inc=1, device_id=peer, device_id_type=MESH)
    first_part = (y == 1) & (z == 1)
    last_part = (y == 2) & (z == 2)
    first_hold = (y == 1) & (z == 0)
    last_hold = (y == 2) & (z == 3)
    part_sender, part_holder = first_part | last_part, first_hold | last_hold
    part_to = at(1 - xh, y, jnp.where(y == 1, 0, 3))
    part_from = at(1 - xh, y, jnp.where(y == 1, 1, 2))

    @pl.when(part_sender)
    def _():
        pl.semaphore_signal(barrier, inc=1, device_id=part_to, device_id_type=MESH)

    @pl.when(part_holder)
    def _():
        pl.semaphore_signal(barrier, inc=1, device_id=part_from, device_id_type=MESH)

    pl.semaphore_wait(barrier, len(peers) + jnp.where(part_sender | part_holder, 1, 0))

    net = Net(send_sem, recv_sem)
    send, recv = net.send, net.recv
    edge = (y == 0) | (y == 3)
    mirrored = edge | part_holder
    low, high = z == 0, z == 3
    rim = low | high
    tail = pl.ds(pl.multiple_of(jnp.where(low, 0, 2 * TS), TS), TS)
    side = pl.ds(pl.multiple_of(jnp.where(y == 1, 0, 2 * TS), TS), TS)
    HEAD, LAST = pl.ds(0, TS), pl.ds(2 * TS, TS)

    lists = ((rows, CR), (cols, CC), (lats, CL), (live, CN))
    local = [pltpu.make_async_copy(src, dst.at[0], local_sem.at[i]) for i, (src, dst) in enumerate(lists)]
    for copy in local:
        copy.start()
    for flip in (1, 2, 3):
        for i, (src, dst) in enumerate(lists):
            send(f"c{flip}{i}", None, src, dst.at[flip], along(flip))
    for h in HALVES:
        send(f"m{h}", mirrored, vec.at[h], S.at[z, h], mirror)
    for h in HALVES:
        send(f"mp{h}", part_sender, vec.at[h, :, side], S.at[z, h, :, side], part_to)

    def z_own(u, h):
        if u < 0:
            send(f"z-{h}", None, vec.at[h], W.at[6 + z - zp, h], up_z)
        else:
            send(f"z+{h}", None, vec.at[h], W.at[6 + z - zm, h], down_z)

    def z_shadow(u, h):
        if u < 0:
            send(f"s-{h}", edge, S.at[z, h], S.at[z, h], up_z)
        else:
            send(f"s+{h}", edge, S.at[z, h], S.at[z, h], down_z)

    member = {0: z, -1: zm, 1: zp, 2: z2}

    def y_copies(u, h, shadow):
        m = member[u]
        dz = m - z
        if shadow:
            src = S.at[m, h]
            down_ok, up_ok = y == 0, y == 3
        else:
            src = vec.at[h] if u == 0 else W.at[6 + dz, h]
            down_ok, up_ok = y > 0, y < 3
        down_dst, up_dst = W.at[10 + dz, h], W.at[2 + dz, h]
        if u == 0:
            send(f"y-{u}{h}", down_ok, src, down_dst, down_y)
            send(f"y+{u}{h}", up_ok, src, up_dst, up_y)
        elif u == -1:
            send(f"y-{u}{h}", down_ok & (z != 0), src, down_dst, down_y)
            send(f"y+{u}{h}", up_ok, src, up_dst, up_y)
        elif u == 1:
            send(f"y-{u}{h}", down_ok, src, down_dst, down_y)
            send(f"y+{u}{h}", up_ok & (z != 3), src, up_dst, up_y)
        else:
            send(f"y-{u}{h}", down_ok & (z >= 2), src, down_dst, down_y)
            send(f"y-{u}{h}", down_ok & (z < 2), src.at[:, HEAD], down_dst.at[:, HEAD], down_y)
            send(f"y+{u}{h}", up_ok & (z < 2), src, up_dst, up_y)
            send(f"y+{u}{h}", up_ok & (z >= 2), src.at[:, LAST], up_dst.at[:, LAST], up_y)

    def y_arrived(u, h):
        dz = member[u] - z
        down_dst, up_dst = W.at[10 + dz, h], W.at[2 + dz, h]
        if u == 2:
            recv(f"y-{u}{h}", z >= 2, down_dst, up_y)
            recv(f"y-{u}{h}", z < 2, down_dst.at[:, HEAD], up_y)
            recv(f"y+{u}{h}", z < 2, up_dst, down_y)
            recv(f"y+{u}{h}", z >= 2, up_dst.at[:, LAST], down_y)
        else:
            recv(f"y-{u}{h}", (z != 0) if u == -1 else None, down_dst, up_y)
            recv(f"y+{u}{h}", (z != 3) if u == 1 else None, up_dst, down_y)

    z_own(-1, 0)
    z_own(1, 1)
    for h in HALVES:
        y_copies(0, h, False)
    for c in range(CHUNKS):
        part = pl.ds(c * PER, PER)
        send(f"x{c}", None, hop.at[part], G.at[1, part], along(2))
    send("sib", None, hop, G.at[0], along(1))

    recv("m0", mirrored, S.at[z, 0], mirror)
    z_shadow(-1, 0)
    z_own(-1, 1)
    z_own(1, 0)
    z_shadow(1, 0)
    y_copies(0, 0, True)
    recv("z-0", None, W.at[6 + zm - z, 0], down_z)
    send("w0", None, W.at[6 + zm - z, 0], W.at[6 + zm - zp, 0], up_z)
    y_copies(-1, 0, False)
    recv("z+1", None, W.at[6 + zp - z, 1], up_z)
    send("w1", None, W.at[6 + zp - z, 1], W.at[6 + zp - zm, 1], down_z)
    y_copies(1, 1, False)
    y_near = jnp.where(low, ym, yp)
    near = at(xh, y_near, z)
    near_src = at(xh, jnp.where(low, yp, ym), z)
    hold = jnp.where(y == 1, 0, 3)
    hold_part = jnp.where(y == 1, 1, 2)
    hold_to = at(xh, jnp.where(y == 1, 0, 3), z)
    hold_from = at(xh, jnp.where(y == 0, 1, 2), z)
    relay_rim = ((y == 0) & low) | ((y == 3) & high)
    real_rim = (low & (y > 0)) | (high & (y < 3))
    send("e0", part_holder, S.at[hold, 0], E.at[0, 0], hold_to)

    recv("m1", mirrored, S.at[z, 1], mirror)
    z_shadow(1, 1)
    z_shadow(-1, 1)
    y_copies(0, 1, True)
    send("e1", part_holder, S.at[hold, 1], E.at[0, 1], hold_to)
    recv("z-1", None, W.at[6 + zm - z, 1], down_z)
    y_copies(-1, 1, False)
    recv("z+0", None, W.at[6 + zp - z, 0], up_z)
    y_copies(1, 0, False)
    for h in HALVES:
        recv(f"mp{h}", part_holder, S.at[hold_part, h, :, side], part_from)
        send(f"ep{h}", part_holder, S.at[hold_part, h, :, side], E.at[1, h, :, side], hold_to)

    block = jnp.where(low, 10, 2)
    beside = jnp.where(low, 11, 1)
    for h in HALVES:
        y_arrived(0, h)
        send(f"d{h}", real_rim, W.at[block, h], X.at[0, h], near)
    recv("w0", None, W.at[6 + z2 - z, 0], down_z)
    y_copies(2, 0, False)
    recv("w1", None, W.at[6 + z2 - z, 1], up_z)
    y_copies(2, 1, False)
    recv("s-0", edge, S.at[zm, 0], down_z)
    send("v0", edge, S.at[zm, 0], S.at[zm, 0], up_z)
    y_copies(-1, 0, True)
    recv("s+0", edge, S.at[zp, 0], up_z)
    y_copies(1, 0, True)
    for h in HALVES:
        recv(f"e{h}", relay_rim, E.at[0, h], hold_from)
        send(f"d{h}", relay_rim, E.at[0, h], X.at[0, h], near)
    recv("s+1", edge, S.at[zp, 1], up_z)
    send("v1", edge, S.at[zp, 1], S.at[zp, 1], down_z)
    y_copies(1, 1, True)
    recv("s-1", edge, S.at[zm, 1], down_z)
    y_copies(-1, 1, True)
    for h in HALVES:
        recv(f"ep{h}", relay_rim, E.at[1, h, :, tail], hold_from)
        send(f"dp{h}", relay_rim, E.at[1, h, :, tail], X.at[1, h, :, tail], near)
    rim_to = at(xh, y, jnp.where(low, 3, 0))
    far = jnp.where(low, 11, 1)
    far_part = jnp.where(low, 12, 0)
    for h in HALVES:
        recv(f"d{h}", rim, X.at[0, h], near_src)
        send(f"f{h}", rim, X.at[0, h], W.at[far, h], rim_to)
    for h in HALVES:
        y_arrived(1, h)
        y_arrived(-1, h)
        send(f"dp{h}", real_rim, W.at[beside, h, :, tail], X.at[1, h, :, tail], near)
    recv("v0", edge, S.at[z2, 0], down_z)
    y_copies(2, 0, True)
    recv("v1", edge, S.at[z2, 1], up_z)
    y_copies(2, 1, True)

    def forward(c):
        part = pl.ds(c * PER, PER)
        recv(f"x{c}", None, G.at[1, part], along(2))
        send(f"o{c}", None, G.at[1, part], G.at[2, part], along(1))

    for c in range(3):
        forward(c)
    for h in HALVES:
        recv(f"dp{h}", rim, X.at[1, h, :, tail], near_src)
        send(f"fp{h}", rim, X.at[1, h, :, tail], W.at[far_part, h, :, tail], rim_to)
    forward(3)
    got = jnp.where(low, 1, 11)
    got_part = jnp.where(low, 0, 12)
    got_tail = pl.ds(pl.multiple_of(jnp.where(low, 2 * TS, 0), TS), TS)
    next_to = at(xh, y, jnp.where(low, 1, 2))
    for h in HALVES:
        recv(f"f{h}", rim, W.at[got, h], rim_to)
        send(f"l{h}", rim, W.at[got, h, :, got_tail], W.at[got_part, h, :, got_tail], next_to)
    for c in range(4, CHUNKS - 1):
        forward(c)
    inner = (z == 1) | (z == 2)
    inner_part = jnp.where(z == 1, 0, 12)
    inner_tail = pl.ds(pl.multiple_of(jnp.where(z == 1, 2 * TS, 0), TS), TS)
    inner_from = at(xh, y, jnp.where(z == 1, 0, 3))
    for h in HALVES:
        y_arrived(2, h)
        recv(f"fp{h}", rim, W.at[got_part, h, :, got_tail], rim_to)
        recv(f"l{h}", inner, W.at[inner_part, h, :, inner_tail], inner_from)
    for flip in (1, 2, 3):
        for i, (_, dst) in enumerate(lists):
            recv(f"c{flip}{i}", None, dst.at[flip], along(flip))
    recv("sib", None, G.at[0], along(1))
    forward(CHUNKS - 1)
    for c in range(CHUNKS):
        recv(f"o{c}", None, G.at[2, pl.ds(c * PER, PER)], along(1))
    net.finish()
    for copy in local:
        copy.wait()


def gather_all(hop, lists, vec):
    block = vec.shape
    any_space = pl.BlockSpec(memory_space=pl.ANY)
    sems = 96
    return pl.pallas_call(
        gather_kernel,
        out_shape=(
            jax.ShapeDtypeStruct((3,) + hop.shape, hop.dtype),
            jax.ShapeDtypeStruct((13,) + block, vec.dtype),
            *[jax.ShapeDtypeStruct((4,) + a.shape, a.dtype) for a in lists],
            jax.ShapeDtypeStruct((4,) + block, vec.dtype),
            jax.ShapeDtypeStruct((2,) + block, vec.dtype),
            jax.ShapeDtypeStruct((2,) + block, vec.dtype),
        ),
        in_specs=[any_space] * 6,
        out_specs=(any_space,) * 9,
        scratch_shapes=[
            pltpu.SemaphoreType.DMA((sems,)),
            pltpu.SemaphoreType.DMA((sems,)),
            pltpu.SemaphoreType.DMA((4,)),
        ],
        compiler_params=pltpu.CompilerParams(collective_id=0, has_side_effects=True),
        name="gather",
    )(hop, *lists, vec)[:6]


def product_kernel(cosine, sine, hop, G, vec, W, CR, CC, CL, CN, out, T, V, H, NR, NC, NL, NN, sems):
    row = lax.axis_index("rows")
    copies = [pltpu.make_async_copy(hop, T.at[pl.ds(0, SLOTS)], sems.at[0])]
    for m in range(3):
        copies.append(
            pltpu.make_async_copy(G.at[m], T.at[pl.ds((m + 1) * SLOTS, SLOTS)], sems.at[m + 1])
        )
    windows = []
    for j in range(13):
        for q in range(2):
            lanes = pl.ds(q * NV, NV)
            if j == 0:
                src, start, size = W.at[j, :, q, pl.ds(2 * TS, TS)], 0, TS
            elif j == 12:
                src, start, size = W.at[j, :, q, pl.ds(0, TS)], (SPAN - 1) * TS, TS
            else:
                src = vec.at[:, q] if j == 6 else W.at[j, :, q]
                start, size = (TR * (j - 6) + BAND) * TS, BLK
            windows.append(
                pltpu.make_async_copy(src, V.at[:, pl.ds(start, size), lanes], sems.at[4 + 2 * j + q])
            )
    scalars = [
        pltpu.make_async_copy(src, dst, sems.at[30 + i])
        for i, (src, dst) in enumerate(((CR, NR), (CC, NC), (CL, NL), (CN, NN)))
    ]
    for copy in scalars + copies + windows:
        copy.start()

    def clear(i, _):
        rows = pl.ds(pl.multiple_of(i * 8, 8), 8)
        for k in range(2):
            for r in range(TR):
                H[k, r, rows, :] = jnp.zeros((8, WIDE * TS), jnp.float32)
        return 0

    lax.fori_loop(0, 2 * TS // 8, clear, 0)
    for copy in scalars:
        copy.wait()
    part = 32
    for m in range(4):
        copies[m].wait()
        count = NN[m, 0, 0]

        def add(i, _, m=m, count=count):
            for one in (2 * i, 2 * i + 1):
                r = jnp.clip(NR[m, 0, one] - row * TR, 0, TR - 1)
                w = NC[m, 0, one] - (row * TR + r - BAND)
                w = jnp.where(w < 0, w + TORB, w)
                w = jnp.clip(jnp.where(w >= TORB, w - TORB, w), 0, WIDE - 1)
                cols = pl.ds(pl.multiple_of(w * TS, TS), TS)
                lat = NL[m, 0, one]
                scale = [jnp.where(one < count, t[k, lat], 0.0) for k in range(2) for t in (cosine, sine)]
                for at in range(0, TS, part):
                    tile = T[m * SLOTS + one, pl.ds(at, part), :].astype(jnp.float32)
                    for k in range(2):
                        for p in range(2):
                            H[k, r, pl.ds(p * TS + at, part), cols] += tile * scale[2 * k + p]
            return 0

        lax.fori_loop(0, (count + 1) // 2, add, 0)
    for copy in windows:
        copy.wait()
    for k in range(2):
        for r in range(TR):
            o = jnp.dot(
                H[k, r].astype(jnp.bfloat16), V[k, pl.ds(r * TS, WIDE * TS), :], preferred_element_type=jnp.float32
            )
            rows = pl.ds(r * TS, TS)
            out[k, 0, rows, :] = o[:TS, :NV] - o[TS:, NV:]
            out[k, 1, rows, :] = o[:TS, NV:] + o[TS:, :NV]


def product(cosine, sine, hop, G, vec, W, lists):
    any_space = pl.BlockSpec(memory_space=pl.ANY)
    smem = pl.BlockSpec(memory_space=pltpu.SMEM)
    return pl.pallas_call(
        product_kernel,
        out_shape=jax.ShapeDtypeStruct((2, 2, BLK, NV), jnp.float32),
        in_specs=[smem, smem] + [any_space] * 8,
        out_specs=pl.BlockSpec(memory_space=pltpu.VMEM),
        scratch_shapes=[
            pltpu.VMEM((4 * SLOTS, TS, TS), jnp.bfloat16),
            pltpu.VMEM((2, SPAN * TS, 2 * NV), jnp.bfloat16),
            pltpu.VMEM((2, TR, 2 * TS, WIDE * TS), jnp.float32),
            *[pltpu.SMEM((4, 1, SLOTS), jnp.int32)] * 4,
            pltpu.SemaphoreType.DMA((34,)),
        ],
        compiler_params=pltpu.CompilerParams(vmem_limit_bytes=60 * 1024 * 1024),
        name="product",
    )(cosine, sine, hop, G, vec, W, *lists)


def body(hoppings, tile_rows, tile_cols, tile_lats, tile_counts, phase_angle, vectors):
    hop = hoppings[0]
    live = jnp.broadcast_to(tile_counts, (1, SLOTS))
    G, W, *lists = gather_all(hop, (tile_rows, tile_cols, tile_lats, live), vectors)
    return product(jnp.cos(phase_angle), jnp.sin(phase_angle), hop, G, vectors, W, lists)


def solution(mesh):
    return jax.shard_map(
        body,
        mesh=mesh,
        in_specs=(
            P("rows", "ka", None, None),
            P("rows", "ka"),
            P("rows", "ka"),
            P("rows", "ka"),
            P("rows", "ka"),
            P("ka", None),
            P("ka", None, "rows", None),
        ),
        out_specs=P("ka", None, "rows", None),
        check_vma=False,
    )
```

```python
import functools

import jax
import jax.numpy as jnp
from jax import lax
from jax.experimental import pallas as pl
from jax.experimental.pallas import tpu as pltpu
from jax.sharding import PartitionSpec as P

MESH = pl.DeviceIdType.MESH
BAND = 16
NLAT = 9
TS = 128
NV = 256
TR = 3
BLK = TR * TS
SLOTS = 96
CHUNKS = 8
PER = SLOTS // CHUNKS
AROUND = 8
WIDE = 2 * BAND + 1
SPAN = WIDE + TR - 1
TORB = 96
HALVES = (0, 1)


class Net:
    def __init__(self, send_sem, recv_sem):
        self.send_sem, self.recv_sem = send_sem, recv_sem
        self.index, self.sent = {}, []

    def copy(self, name, src, dst, device):
        at = self.index.setdefault(name, len(self.index))
        return pltpu.make_async_remote_copy(
            src_ref=src, dst_ref=dst, send_sem=self.send_sem.at[at], recv_sem=self.recv_sem.at[at],
            device_id=device, device_id_type=MESH,
        )

    def send(self, name, when, src, dst, device):
        copy = self.copy(name, src, dst, device)
        self.sent.append((when, copy))
        guarded(when, copy.start)

    def recv(self, name, when, dst, device):
        guarded(when, self.copy(name, dst, dst, device).wait_recv)

    def finish(self):
        for when, copy in self.sent:
            guarded(when, copy.wait_send)


def guarded(when, action):
    if when is None:
        action()
    else:
        pl.when(when)(action)


def gather_kernel(hop, rows, cols, lats, live, vec, G, W, CR, CC, CL, CN, S, X, E, R, send_sem, recv_sem, local_sem):
    ka = lax.axis_index("ka")
    row = lax.axis_index("rows")
    xh, y, z = row // 16, (row // 4) % 4, row % 4
    zp, zm, z2 = (z + 1) % 4, (z + 3) % 4, (z + 2) % 4
    yp, ym = (y + 1) % 4, (y + 3) % 4

    def at(h, i, j):
        return (ka, h * 16 + i * 4 + j)

    def along(flip):
        other = (1 - ka % 2) if flip % 2 else ka % 2
        pair = (1 - ka // 2) if flip // 2 else ka // 2
        return (pair * 2 + other, row)

    up_z, down_z, up_y, down_y = at(xh, y, zp), at(xh, y, zm), at(xh, yp, z), at(xh, ym, z)
    mirror = at(1 - xh, y, z)
    low, high = z == 0, z == 3
    mid = (z == 1) | (z == 2)
    top, base = y == 3, y == 0
    down_y = at(jnp.where(base, 1 - xh, xh), ym, z)
    up_y = at(jnp.where(top, 1 - xh, xh), yp, z)
    inner_y = at(xh, jnp.where(base, 3, jnp.where(top, 0, y)), z)
    crossing = ((y == 1) & high) | ((y == 2) & low)
    part_sender = ((y == 1) & (z == 1)) | ((y == 2) & (z == 2))
    part_to = at(1 - xh, y, jnp.where(y == 1, 3, 0))
    part_from = at(1 - xh, y, jnp.where(y == 1, 1, 2))
    split = ((y == 1) & low) | ((y == 2) & high)
    outer = base | top
    beside_y = at(xh, jnp.where(y < 2, 1 - y, 5 - y), z)
    over = at(xh, jnp.where(y == 1, 0, 3), jnp.where(y == 1, 3, 0))
    over_from = at(xh, jnp.where(base, 1, 2), z)
    split_from = at(xh, jnp.where(base, 1, 2), 3 - z)
    relay = (base & high) | (top & low)
    relayed = (top & high) | (base & low)
    barrier = pltpu.get_barrier_semaphore()

    def greet(peer):
        pl.semaphore_signal(barrier, inc=1, device_id=peer, device_id_type=MESH)

    for peer in (along(1), along(2), along(3), up_z, down_z, up_y, down_y):
        greet(peer)
    pl.when(part_sender)(lambda: greet(part_to))
    pl.when(crossing)(lambda: greet(part_from))
    pl.when(crossing | split)(lambda: greet(mirror))
    pl.when(split)(lambda: greet(over))
    pl.when(relay)(lambda: greet(split_from))
    pl.when(relay | relayed)(lambda: greet(inner_y))
    extra = jnp.where(part_sender, 1, 0) + jnp.where(crossing | split, 2, 0)
    extra = extra + jnp.where(relay | relayed, 1, 0) + jnp.where(relay, 1, 0)
    pl.semaphore_wait(barrier, 7 + extra)

    net = Net(send_sem, recv_sem)
    send, recv = net.send, net.recv
    HEAD, LAST = pl.ds(0, TS), pl.ds(2 * TS, TS)

    def tail(first):
        return pl.ds(pl.multiple_of(jnp.where(first, 0, 2 * TS), TS), TS)

    lists = ((rows, CR), (cols, CC), (lats, CL), (live, CN))
    local = [pltpu.make_async_copy(src, dst.at[0], local_sem.at[i]) for i, (src, dst) in enumerate(lists)]
    for copy in local:
        copy.start()

    member = {0: z, -1: zm, 1: zp, 2: z2}

    def y_sends(u, h):
        dz = member[u] - z
        src = vec.at[h] if u == 0 else W.at[6 + dz, h]
        down_dst, up_dst = W.at[10 + dz, h], W.at[2 + dz, h]
        down_ok, up_ok = (None, None) if u == 0 else (y > 0, y < 3)
        if u == 2:
            send(f"y-{u}{h}", down_ok & (z >= 2), src, down_dst, down_y)
            send(f"y-{u}{h}", down_ok & (z < 2), src.at[:, HEAD], down_dst.at[:, HEAD], down_y)
            send(f"y+{u}{h}", up_ok & (z < 2), src, up_dst, up_y)
            send(f"y+{u}{h}", up_ok & (z >= 2), src.at[:, LAST], up_dst.at[:, LAST], up_y)
        else:
            send(f"y-{u}{h}", down_ok & (z != 0) if u == -1 else down_ok, src, down_dst, down_y)
            send(f"y+{u}{h}", up_ok & (z != 3) if u == 1 else up_ok, src, up_dst, up_y)

    def y_recvs(u, h):
        dz = member[u] - z
        down_dst, up_dst = W.at[10 + dz, h], W.at[2 + dz, h]
        down_ok, up_ok = (None, None) if u == 0 else (y < 3, y > 0)
        if u == 2:
            recv(f"y-{u}{h}", down_ok & (z >= 2), down_dst, up_y)
            recv(f"y-{u}{h}", down_ok & (z < 2), down_dst.at[:, HEAD], up_y)
            recv(f"y+{u}{h}", up_ok & (z < 2), up_dst, down_y)
            recv(f"y+{u}{h}", up_ok & (z >= 2), up_dst.at[:, LAST], down_y)
        else:
            recv(f"y-{u}{h}", down_ok & (z != 0) if u == -1 else down_ok, down_dst, up_y)
            recv(f"y+{u}{h}", up_ok & (z != 3) if u == 1 else up_ok, up_dst, down_y)

    def both(when, ok):
        return ok if when is None else when & ok

    def spread(h):
        a, b = (None, None) if h else (top, base)
        send(f"a1{h}", both(a, z < 3), W.at[10, h], W.at[9, h], up_z)
        send(f"b1{h}", both(b, z > 0), W.at[2, h], W.at[3, h], down_z)
        send(f"a2{h}", a, W.at[10, h], W.at[jnp.where(low, 7, 11), h], down_z)
        send(f"b2{h}", b, W.at[2, h], W.at[jnp.where(high, 5, 1), h], up_z)

    def spread_on(h):
        a, b = (None, None) if h else (top, base)
        recv(f"a1{h}", both(a, z > 0), W.at[9, h], down_z)
        recv(f"b1{h}", both(b, z < 3), W.at[3, h], up_z)
        recv(f"a2{h}", a, W.at[jnp.where(high, 7, 11), h], up_z)
        recv(f"b2{h}", b, W.at[jnp.where(low, 5, 1), h], down_z)
        if h:
            send(f"a3{h}", mid, W.at[9, h], W.at[8, h], up_z)
            send(f"b3{h}", mid, W.at[3, h], W.at[4, h], down_z)
        else:
            send(f"a3{h}", both(a, low | high), W.at[jnp.where(low, 11, 7), h], W.at[8, h], down_z)
            send(f"b3{h}", both(b, low | high), W.at[jnp.where(low, 5, 1), h], W.at[4, h], up_z)
        send(f"a4{h}", both(a, mid), W.at[11, h, :, HEAD], W.at[12, h, :, HEAD], down_z)
        send(f"b4{h}", both(b, mid), W.at[1, h, :, LAST], W.at[0, h, :, LAST], up_z)

    def spread_last(h):
        a, b = (None, None) if h else (top, base)
        recv(f"a3{h}", both(a, z >= 2), W.at[8, h], down_z)
        recv(f"b3{h}", both(b, z < 2), W.at[4, h], down_z)
        recv(f"a4{h}", both(a, z < 2), W.at[12, h, :, HEAD], up_z)
        recv(f"b4{h}", both(b, z >= 2), W.at[0, h, :, LAST], down_z)

    near_to, near_from = (low & (y > 0)) | (high & (y < 3)), (low & (y < 3)) | (high & (y > 0))
    near = at(xh, jnp.where(low, ym, yp), z)
    near_src = at(xh, jnp.where(low, yp, ym), z)
    across = at(xh, y, jnp.where(low, 3, 0))
    across_from = (high & (y < 3)) | (low & (y > 0))
    block, beside = jnp.where(low, 10, 2), jnp.where(low, 11, 1)
    far, far_part = jnp.where(low, 11, 1), jnp.where(low, 12, 0)
    got, got_part = jnp.where(low, 1, 11), jnp.where(low, 0, 12)

    def second(h):
        send(f"d{h}", near_to, W.at[block, h], X.at[0, h], near)

    def second_part(h, ok):
        send(f"dp{h}", near_to & ok, W.at[beside, h, :, tail(low)], X.at[1, h, :, tail(low)], near)

    crossed = jnp.where(y == 1, 3, 9)

    def cross():
        send("g0", crossing, W.at[crossed, 0], S.at[0, 0], mirror)

    z_dst_up, z_dst_down = W.at[6 + z - zp], W.at[6 + z - zm]
    y_sends(0, 1)
    send("z-0", None, vec.at[0], z_dst_up.at[0], up_z)
    send("z+1", None, vec.at[1], z_dst_down.at[1], down_z)
    y_sends(0, 0)
    send("z-1", None, vec.at[1], z_dst_up.at[1], up_z)
    send("z+0", None, vec.at[0], z_dst_down.at[0], down_z)
    for h in HALVES:
        send(f"gp{h}", part_sender, vec.at[h, :, tail(y == 1)], S.at[1, h, :, tail(y == 1)], part_to)

    def pieces(c):
        if c < CHUNKS - 1:
            return ((f"{c}", None, pl.ds(c * PER, PER)),)
        end = SLOTS - AROUND
        return (("e", None, pl.ds(c * PER, end - c * PER)), ("f", ~outer, pl.ds(end, AROUND)))

    def chunk(c):
        for name, when, part in pieces(c):
            send(f"x{name}", when, hop.at[part], G.at[1, part], along(2))

    def forward(c):
        for name, when, part in pieces(c):
            recv(f"x{name}", when, G.at[1, part], along(2))
            send(f"o{name}", when, G.at[1, part], G.at[2, part], along(1))

    around = pl.ds(SLOTS - AROUND, AROUND)
    send("g1", split, vec.at[1], S.at[0, 1], mirror)
    send("r", outer, hop.at[around], R.at[0], beside_y)
    for c in range(3):
        chunk(c)
    for flip in (1, 2, 3):
        for i, (src, dst) in enumerate(lists):
            send(f"c{flip}{i}", None, src, dst.at[flip], along(flip))
    send("sib", None, hop, G.at[0], along(1))

    recv("z-0", None, W.at[6 + zm - z, 0], down_z)
    send("w0", None, W.at[6 + zm - z, 0], W.at[6 + zm - zp, 0], up_z)
    y_sends(-1, 0)
    recv("z+1", None, W.at[6 + zp - z, 1], up_z)
    send("w1", None, W.at[6 + zp - z, 1], W.at[6 + zp - zm, 1], down_z)
    y_recvs(0, 1)
    spread(1)
    second(1)
    recv("z+0", None, W.at[6 + zp - z, 0], up_z)
    y_sends(1, 0)
    recv("z-1", None, W.at[6 + zm - z, 1], down_z)
    cross()
    recv("r", ~outer, R.at[0], beside_y)
    send("q", ~outer, R.at[0], R.at[1], along(2))
    for c in range(3, CHUNKS):
        chunk(c)
    recv("g1", split, S.at[0, 1], mirror)
    send("e1", split, S.at[0, 1], E.at[0, 1], over)
    y_recvs(0, 0)
    second(0)
    spread(0)
    recv("w0", None, W.at[6 + z2 - z, 0], down_z)
    y_sends(2, 0)
    recv("w1", None, W.at[6 + z2 - z, 1], up_z)
    for h in HALVES:
        recv(f"d{h}", near_from, X.at[0, h], near_src)
        send(f"f{h}", near_from, X.at[0, h], W.at[far, h], across)
    recv("g0", crossing, S.at[0, 0], mirror)
    send("e0", crossing, S.at[0, 0], E.at[0, 0], beside_y)
    for h in HALVES:
        recv(f"gp{h}", crossing, S.at[1, h, :, tail(y == 1)], part_from)
        send(f"ep{h}", crossing, S.at[1, h, :, tail(y == 1)], E.at[1, h, :, tail(y == 1)], beside_y)
    y_recvs(-1, 0)
    y_recvs(1, 0)
    second_part(0, (low & (y < 3)) | (high & (y > 0)))
    spread_on(1)
    second_part(1, low | high)
    spread_on(0)
    second_part(0, (low & top) | (high & base))
    for h in HALVES:
        recv(f"e{h}", relay, E.at[0, h], split_from if h else over_from)
        send(f"f{h}", relay, E.at[0, h], W.at[got, h], inner_y)
        recv(f"ep{h}", relay, E.at[1, h, :, tail(high)], over_from)
        send(f"fp{h}", relay, E.at[1, h, :, tail(high)], W.at[got_part, h, :, tail(high)], inner_y)
    recv("q", ~outer, R.at[1], along(2))
    send("p", ~outer, R.at[1], G.at[1, around], beside_y)
    for c in range(3):
        forward(c)
    for h in HALVES:
        recv(f"dp{h}", near_from, X.at[1, h, :, tail(low)], near_src)
        send(f"fp{h}", near_from, X.at[1, h, :, tail(low)], W.at[far_part, h, :, tail(low)], across)
    rim = low | high
    next_to = at(xh, y, jnp.where(low, 1, 2))
    for h in HALVES:
        recv(f"f{h}", rim, W.at[got, h], across)
        send(f"l{h}", rim, W.at[got, h, :, tail(high)], W.at[got_part, h, :, tail(high)], next_to)
    for c in range(3, CHUNKS - 2):
        forward(c)
    y_recvs(2, 0)
    for h in HALVES:
        spread_last(h)
        recv(f"fp{h}", rim, W.at[got_part, h, :, tail(high)], across)
        recv(f"l{h}", mid, W.at[jnp.where(z == 1, 0, 12), h, :, tail(z == 2)], at(xh, y, jnp.where(z == 1, 0, 3)))
    for flip in (1, 2, 3):
        for i, (_, dst) in enumerate(lists):
            recv(f"c{flip}{i}", None, dst.at[flip], along(flip))
    recv("sib", None, G.at[0], along(1))
    recv("p", outer, G.at[1, around], beside_y)
    send("of", outer, G.at[1, around], G.at[2, around], along(1))
    for c in range(CHUNKS - 2, CHUNKS):
        forward(c)
    for c in range(CHUNKS):
        for name, _, part in pieces(c):
            recv(f"o{name}", None, G.at[2, part], along(1))
    net.finish()
    for copy in local:
        copy.wait()


def gather_all(hop, lists, vec):
    block = vec.shape
    any_space = pl.BlockSpec(memory_space=pl.ANY)
    sems = 104
    return pl.pallas_call(
        gather_kernel,
        out_shape=(
            jax.ShapeDtypeStruct((3,) + hop.shape, hop.dtype),
            jax.ShapeDtypeStruct((13,) + block, vec.dtype),
            *[jax.ShapeDtypeStruct((4,) + a.shape, a.dtype) for a in lists],
            *[jax.ShapeDtypeStruct((2,) + block, vec.dtype)] * 3,
            jax.ShapeDtypeStruct((2, AROUND) + hop.shape[1:], hop.dtype),
        ),
        in_specs=[any_space] * 6,
        out_specs=(any_space,) * 10,
        scratch_shapes=[
            pltpu.SemaphoreType.DMA((sems,)),
            pltpu.SemaphoreType.DMA((sems,)),
            pltpu.SemaphoreType.DMA((4,)),
        ],
        compiler_params=pltpu.CompilerParams(collective_id=0, has_side_effects=True),
        name="gather",
    )(hop, *lists, vec)[:6]


def product_kernel(cosine, sine, hop, G, vec, W, CR, CC, CL, CN, out, T, V, H, NR, NC, NL, NN, sems):
    row = lax.axis_index("rows")
    copies = [pltpu.make_async_copy(hop, T.at[pl.ds(0, SLOTS)], sems.at[0])]
    for m in range(3):
        copies.append(
            pltpu.make_async_copy(G.at[m], T.at[pl.ds((m + 1) * SLOTS, SLOTS)], sems.at[m + 1])
        )
    windows = []
    for j in range(13):
        for q in range(2):
            lanes = pl.ds(q * NV, NV)
            if j == 0:
                src, start, size = W.at[j, :, q, pl.ds(2 * TS, TS)], 0, TS
            elif j == 12:
                src, start, size = W.at[j, :, q, pl.ds(0, TS)], (SPAN - 1) * TS, TS
            else:
                src = vec.at[:, q] if j == 6 else W.at[j, :, q]
                start, size = (TR * (j - 6) + BAND) * TS, BLK
            windows.append(
                pltpu.make_async_copy(src, V.at[:, pl.ds(start, size), lanes], sems.at[4 + 2 * j + q])
            )
    scalars = [
        pltpu.make_async_copy(src, dst, sems.at[30 + i])
        for i, (src, dst) in enumerate(((CR, NR), (CC, NC), (CL, NL), (CN, NN)))
    ]
    for copy in scalars + copies + windows:
        copy.start()

    def clear(i, _):
        rows = pl.ds(pl.multiple_of(i * 8, 8), 8)
        for k in range(2):
            for r in range(TR):
                H[k, r, rows, :] = jnp.zeros((8, WIDE * TS), jnp.float32)
        return 0

    lax.fori_loop(0, 2 * TS // 8, clear, 0)
    for copy in scalars:
        copy.wait()
    part = 32
    for m in range(4):
        copies[m].wait()
        count = NN[m, 0, 0]

        def add(i, _, m=m, count=count):
            for one in (2 * i, 2 * i + 1):
                r = jnp.clip(NR[m, 0, one] - row * TR, 0, TR - 1)
                w = NC[m, 0, one] - (row * TR + r - BAND)
                w = jnp.where(w < 0, w + TORB, w)
                w = jnp.clip(jnp.where(w >= TORB, w - TORB, w), 0, WIDE - 1)
                cols = pl.ds(pl.multiple_of(w * TS, TS), TS)
                lat = NL[m, 0, one]
                scale = [jnp.where(one < count, t[k, lat], 0.0) for k in range(2) for t in (cosine, sine)]
                for at in range(0, TS, part):
                    tile = T[m * SLOTS + one, pl.ds(at, part), :].astype(jnp.float32)
                    for k in range(2):
                        for p in range(2):
                            H[k, r, pl.ds(p * TS + at, part), cols] += tile * scale[2 * k + p]
            return 0

        lax.fori_loop(0, (count + 1) // 2, add, 0)
    for copy in windows:
        copy.wait()
    for k in range(2):
        for r in range(TR):
            o = jnp.dot(
                H[k, r].astype(jnp.bfloat16), V[k, pl.ds(r * TS, WIDE * TS), :], preferred_element_type=jnp.float32
            )
            rows = pl.ds(r * TS, TS)
            out[k, 0, rows, :] = o[:TS, :NV] - o[TS:, NV:]
            out[k, 1, rows, :] = o[:TS, NV:] + o[TS:, :NV]


def product(cosine, sine, hop, G, vec, W, lists):
    any_space = pl.BlockSpec(memory_space=pl.ANY)
    smem = pl.BlockSpec(memory_space=pltpu.SMEM)
    return pl.pallas_call(
        product_kernel,
        out_shape=jax.ShapeDtypeStruct((2, 2, BLK, NV), jnp.float32),
        in_specs=[smem, smem] + [any_space] * 8,
        out_specs=pl.BlockSpec(memory_space=pltpu.VMEM),
        scratch_shapes=[
            pltpu.VMEM((4 * SLOTS, TS, TS), jnp.bfloat16),
            pltpu.VMEM((2, SPAN * TS, 2 * NV), jnp.bfloat16),
            pltpu.VMEM((2, TR, 2 * TS, WIDE * TS), jnp.float32),
            *[pltpu.SMEM((4, 1, SLOTS), jnp.int32)] * 4,
            pltpu.SemaphoreType.DMA((34,)),
        ],
        compiler_params=pltpu.CompilerParams(vmem_limit_bytes=60 * 1024 * 1024),
        name="product",
    )(cosine, sine, hop, G, vec, W, *lists)


def body(hoppings, tile_rows, tile_cols, tile_lats, tile_counts, phase_angle, vectors):
    hop = hoppings[0]
    live = jnp.broadcast_to(tile_counts, (1, SLOTS))
    G, W, *lists = gather_all(hop, (tile_rows, tile_cols, tile_lats, live), vectors)
    return product(jnp.cos(phase_angle), jnp.sin(phase_angle), hop, G, vectors, W, lists)


def solution(mesh):
    return jax.shard_map(
        body,
        mesh=mesh,
        in_specs=(
            P("rows", "ka", None, None),
            P("rows", "ka"),
            P("rows", "ka"),
            P("rows", "ka"),
            P("rows", "ka"),
            P("ka", None),
            P("ka", None, "rows", None),
        ),
        out_specs=P("ka", None, "rows", None),
        check_vma=False,
    )
```

```python
import functools

import jax
import jax.numpy as jnp
from jax import lax
from jax.experimental import pallas as pl
from jax.experimental.pallas import tpu as pltpu
from jax.sharding import PartitionSpec as P

MESH = pl.DeviceIdType.MESH
BAND = 16
NLAT = 9
TS = 128
NV = 256
TR = 3
BLK = TR * TS
SLOTS = 96
CHUNKS = 8
PER = SLOTS // CHUNKS
AROUND = 6
GROUP = 4
WIDE = 2 * BAND + 1
SPAN = WIDE + TR - 1
TORB = 96
HALVES = (0, 1)


class Net:
    def __init__(self, send_sem, recv_sem):
        self.send_sem, self.recv_sem = send_sem, recv_sem
        self.index, self.sent = {}, []

    def copy(self, name, src, dst, device):
        at = self.index.setdefault(name, len(self.index))
        return pltpu.make_async_remote_copy(
            src_ref=src, dst_ref=dst, send_sem=self.send_sem.at[at], recv_sem=self.recv_sem.at[at],
            device_id=device, device_id_type=MESH,
        )

    def send(self, name, when, src, dst, device):
        copy = self.copy(name, src, dst, device)
        self.sent.append((when, copy))
        guarded(when, copy.start)

    def recv(self, name, when, dst, device):
        guarded(when, self.copy(name, dst, dst, device).wait_recv)

    def finish(self):
        for when, copy in self.sent:
            guarded(when, copy.wait_send)


def guarded(when, action):
    if when is None:
        action()
    else:
        pl.when(when)(action)


def gather_kernel(hop, rows, cols, lats, live, vec, G, W, CR, CC, CL, CN, S, X, E, R, send_sem, recv_sem, local_sem):
    ka = lax.axis_index("ka")
    row = lax.axis_index("rows")
    xh, y, z = row // 16, (row // 4) % 4, row % 4
    zp, zm, z2 = (z + 1) % 4, (z + 3) % 4, (z + 2) % 4
    yp, ym = (y + 1) % 4, (y + 3) % 4

    def at(h, i, j):
        return (ka, h * 16 + i * 4 + j)

    def along(flip):
        other = (1 - ka % 2) if flip % 2 else ka % 2
        pair = (1 - ka // 2) if flip // 2 else ka // 2
        return (pair * 2 + other, row)

    up_z, down_z, up_y, down_y = at(xh, y, zp), at(xh, y, zm), at(xh, yp, z), at(xh, ym, z)
    mirror = at(1 - xh, y, z)
    low, high = z == 0, z == 3
    mid = (z == 1) | (z == 2)
    top, base = y == 3, y == 0
    down_y = at(jnp.where(base, 1 - xh, xh), ym, z)
    up_y = at(jnp.where(top, 1 - xh, xh), yp, z)
    inner_y = at(xh, jnp.where(base, 3, jnp.where(top, 0, y)), z)
    crossing = ((y == 1) & high) | ((y == 2) & low)
    part_sender = ((y == 1) & (z == 1)) | ((y == 2) & (z == 2))
    part_to = at(1 - xh, y, jnp.where(y == 1, 3, 0))
    part_from = at(1 - xh, y, jnp.where(y == 1, 1, 2))
    split = ((y == 1) & low) | ((y == 2) & high)
    outer = base | top
    beside_y = at(xh, jnp.where(y < 2, 1 - y, 5 - y), z)
    over = at(xh, jnp.where(y == 1, 0, 3), jnp.where(y == 1, 3, 0))
    over_from = at(xh, jnp.where(base, 1, 2), z)
    split_from = at(xh, jnp.where(base, 1, 2), 3 - z)
    relay = (base & high) | (top & low)
    relayed = (top & high) | (base & low)
    barrier = pltpu.get_barrier_semaphore()

    def greet(peer):
        pl.semaphore_signal(barrier, inc=1, device_id=peer, device_id_type=MESH)

    for peer in (along(1), along(2), along(3), up_z, down_z, up_y, down_y):
        greet(peer)
    pl.when(part_sender)(lambda: greet(part_to))
    pl.when(crossing)(lambda: greet(part_from))
    pl.when(crossing | split)(lambda: greet(mirror))
    pl.when(split)(lambda: greet(over))
    pl.when(relay)(lambda: greet(split_from))
    pl.when(relay | relayed)(lambda: greet(inner_y))
    extra = jnp.where(part_sender, 1, 0) + jnp.where(crossing | split, 2, 0)
    extra = extra + jnp.where(relay | relayed, 1, 0) + jnp.where(relay, 1, 0)
    pl.semaphore_wait(barrier, 7 + extra)

    net = Net(send_sem, recv_sem)
    send, recv = net.send, net.recv
    HEAD, LAST = pl.ds(0, TS), pl.ds(2 * TS, TS)

    def tail(first):
        return pl.ds(pl.multiple_of(jnp.where(first, 0, 2 * TS), TS), TS)

    lists = ((rows, CR), (cols, CC), (lats, CL), (live, CN))
    local = [pltpu.make_async_copy(src, dst.at[0], local_sem.at[i]) for i, (src, dst) in enumerate(lists)]
    for copy in local:
        copy.start()

    member = {0: z, -1: zm, 1: zp, 2: z2}

    def y_sends(u, h, only=None):
        dz = member[u] - z
        src = vec.at[h] if u == 0 else W.at[6 + dz, h]
        down_dst, up_dst = W.at[10 + dz, h], W.at[2 + dz, h]
        down_ok, up_ok = (None, None) if u == 0 else (y > 0, y < 3)
        if only is not None:
            down_ok, up_ok = down_ok & only, up_ok & only
        if u == 2:
            send(f"y-{u}{h}", down_ok & (z >= 2), src, down_dst, down_y)
            send(f"y-{u}{h}", down_ok & (z < 2), src.at[:, HEAD], down_dst.at[:, HEAD], down_y)
            send(f"y+{u}{h}", up_ok & (z < 2), src, up_dst, up_y)
            send(f"y+{u}{h}", up_ok & (z >= 2), src.at[:, LAST], up_dst.at[:, LAST], up_y)
        else:
            send(f"y-{u}{h}", down_ok & (z != 0) if u == -1 else down_ok, src, down_dst, down_y)
            send(f"y+{u}{h}", up_ok & (z != 3) if u == 1 else up_ok, src, up_dst, up_y)

    def y_recvs(u, h):
        dz = member[u] - z
        down_dst, up_dst = W.at[10 + dz, h], W.at[2 + dz, h]
        down_ok, up_ok = (None, None) if u == 0 else (y < 3, y > 0)
        if u == 2:
            recv(f"y-{u}{h}", down_ok & (z >= 2), down_dst, up_y)
            recv(f"y-{u}{h}", down_ok & (z < 2), down_dst.at[:, HEAD], up_y)
            recv(f"y+{u}{h}", up_ok & (z < 2), up_dst, down_y)
            recv(f"y+{u}{h}", up_ok & (z >= 2), up_dst.at[:, LAST], down_y)
        else:
            recv(f"y-{u}{h}", down_ok & (z != 0) if u == -1 else down_ok, down_dst, up_y)
            recv(f"y+{u}{h}", up_ok & (z != 3) if u == 1 else up_ok, up_dst, down_y)

    def both(when, ok):
        return ok if when is None else when & ok

    def spread(h):
        a, b = (None, None) if h else (top, base)
        send(f"a1{h}", both(a, z < 3), W.at[10, h], W.at[9, h], up_z)
        send(f"b1{h}", both(b, z > 0), W.at[2, h], W.at[3, h], down_z)
        send(f"a2{h}", a, W.at[10, h], W.at[jnp.where(low, 7, 11), h], down_z)
        send(f"b2{h}", b, W.at[2, h], W.at[jnp.where(high, 5, 1), h], up_z)

    def spread_on(h):
        a, b = (None, None) if h else (top, base)
        recv(f"a1{h}", both(a, z > 0), W.at[9, h], down_z)
        recv(f"b1{h}", both(b, z < 3), W.at[3, h], up_z)
        recv(f"a2{h}", a, W.at[jnp.where(high, 7, 11), h], up_z)
        recv(f"b2{h}", b, W.at[jnp.where(low, 5, 1), h], down_z)
        if h:
            send(f"a3{h}", mid, W.at[9, h], W.at[8, h], up_z)
            send(f"b3{h}", mid, W.at[3, h], W.at[4, h], down_z)
        else:
            send(f"a3{h}", both(a, low | high), W.at[jnp.where(low, 11, 7), h], W.at[8, h], down_z)
            send(f"b3{h}", both(b, low | high), W.at[jnp.where(low, 5, 1), h], W.at[4, h], up_z)
        send(f"a4{h}", both(a, mid), W.at[11, h, :, HEAD], W.at[12, h, :, HEAD], down_z)
        send(f"b4{h}", both(b, mid), W.at[1, h, :, LAST], W.at[0, h, :, LAST], up_z)

    def spread_last(h):
        a, b = (None, None) if h else (top, base)
        recv(f"a3{h}", both(a, z >= 2), W.at[8, h], down_z)
        recv(f"b3{h}", both(b, z < 2), W.at[4, h], down_z)
        recv(f"a4{h}", both(a, z < 2), W.at[12, h, :, HEAD], up_z)
        recv(f"b4{h}", both(b, z >= 2), W.at[0, h, :, LAST], down_z)

    near_to, near_from = (low & (y > 0)) | (high & (y < 3)), (low & (y < 3)) | (high & (y > 0))
    near = at(xh, jnp.where(low, ym, yp), z)
    near_src = at(xh, jnp.where(low, yp, ym), z)
    across = at(xh, y, jnp.where(low, 3, 0))
    across_from = (high & (y < 3)) | (low & (y > 0))
    block, beside = jnp.where(low, 10, 2), jnp.where(low, 11, 1)
    far, far_part = jnp.where(low, 11, 1), jnp.where(low, 12, 0)
    got, got_part = jnp.where(low, 1, 11), jnp.where(low, 0, 12)

    def second(h):
        send(f"d{h}", near_to, W.at[block, h], X.at[0, h], near)

    def second_part(h, ok):
        send(f"dp{h}", near_to & ok, W.at[beside, h, :, tail(low)], X.at[1, h, :, tail(low)], near)

    crossed = jnp.where(y == 1, 3, 9)

    def cross():
        send("g0", crossing, W.at[crossed, 0], S.at[0, 0], mirror)

    z_dst_up, z_dst_down = W.at[6 + z - zp], W.at[6 + z - zm]
    y_sends(0, 1)
    send("z-0", None, vec.at[0], z_dst_up.at[0], up_z)
    send("z+1", None, vec.at[1], z_dst_down.at[1], down_z)
    y_sends(0, 0)
    send("z-1", None, vec.at[1], z_dst_up.at[1], up_z)
    send("z+0", None, vec.at[0], z_dst_down.at[0], down_z)
    for h in HALVES:
        send(f"gp{h}", part_sender, vec.at[h, :, tail(y == 1)], S.at[1, h, :, tail(y == 1)], part_to)

    def pieces(c):
        if c < CHUNKS - 1:
            return ((f"{c}", None, pl.ds(c * PER, PER)),)
        end = SLOTS - AROUND
        return (("e", None, pl.ds(c * PER, end - c * PER)), ("f", ~outer, pl.ds(end, AROUND)))

    def chunk(c):
        for name, when, part in pieces(c):
            send(f"x{name}", when, hop.at[part], G.at[1, part], along(2))

    def forward(c):
        for name, when, part in pieces(c):
            recv(f"x{name}", when, G.at[1, part], along(2))
            send(f"o{name}", when, G.at[1, part], G.at[2, part], along(1))

    around = pl.ds(SLOTS - AROUND, AROUND)
    send("g1", split, vec.at[1], S.at[0, 1], mirror)
    send("r", outer, hop.at[around], R.at[0], beside_y)
    for c in range(3):
        chunk(c)
    for flip in (1, 2, 3):
        for i, (src, dst) in enumerate(lists):
            send(f"c{flip}{i}", None, src, dst.at[flip], along(flip))
    send("sib", None, hop, G.at[0], along(1))

    recv("z-0", None, W.at[6 + zm - z, 0], down_z)
    send("w0", None, W.at[6 + zm - z, 0], W.at[6 + zm - zp, 0], up_z)
    y_sends(-1, 0)
    recv("z+1", None, W.at[6 + zp - z, 1], up_z)
    send("w1", None, W.at[6 + zp - z, 1], W.at[6 + zp - zm, 1], down_z)
    recv("g1", split, S.at[0, 1], mirror)
    send("e1", split, S.at[0, 1], E.at[0, 1], over)
    y_recvs(0, 1)
    spread(1)
    second(1)
    recv("z+0", None, W.at[6 + zp - z, 0], up_z)
    y_sends(1, 0)
    recv("z-1", None, W.at[6 + zm - z, 1], down_z)
    cross()
    recv("r", ~outer, R.at[0], beside_y)
    send("q", ~outer, R.at[0], R.at[1], along(2))
    for c in range(3, CHUNKS):
        chunk(c)
    y_recvs(0, 0)
    second(0)
    spread(0)
    recv("w0", None, W.at[6 + z2 - z, 0], down_z)
    y_sends(2, 0, ~crossing)
    recv("w1", None, W.at[6 + z2 - z, 1], up_z)
    for h in (1, 0):
        recv(f"d{h}", near_from, X.at[0, h], near_src)
        send(f"f{h}", near_from, X.at[0, h], W.at[far, h], across)
    recv("g0", crossing, S.at[0, 0], mirror)
    send("e0", crossing, S.at[0, 0], E.at[0, 0], beside_y)
    y_sends(2, 0, crossing)
    for h in HALVES:
        recv(f"gp{h}", crossing, S.at[1, h, :, tail(y == 1)], part_from)
        send(f"ep{h}", crossing, S.at[1, h, :, tail(y == 1)], E.at[1, h, :, tail(y == 1)], beside_y)
    def onward(h):
        recv(f"e{h}", relay, E.at[0, h], split_from if h else over_from)
        send(f"f{h}", relay, E.at[0, h], W.at[got, h], inner_y)

    def onward_part(h):
        recv(f"ep{h}", relay, E.at[1, h, :, tail(high)], over_from)
        send(f"fp{h}", relay, E.at[1, h, :, tail(high)], W.at[got_part, h, :, tail(high)], inner_y)

    y_recvs(-1, 0)
    y_recvs(1, 0)
    second_part(0, (low & (y < 3)) | (high & (y > 0)))
    spread_on(1)
    second_part(1, low | high)
    onward(1)
    onward(0)
    spread_on(0)
    second_part(0, (low & top) | (high & base))
    for h in HALVES:
        onward_part(h)
    recv("q", ~outer, R.at[1], along(2))
    send("p", ~outer, R.at[1], G.at[1, around], beside_y)
    for c in range(3):
        forward(c)
    for h in HALVES:
        recv(f"dp{h}", near_from, X.at[1, h, :, tail(low)], near_src)
        send(f"fp{h}", near_from, X.at[1, h, :, tail(low)], W.at[far_part, h, :, tail(low)], across)
    rim = low | high
    next_to = at(xh, y, jnp.where(low, 1, 2))
    for h in (1, 0):
        recv(f"f{h}", rim, W.at[got, h], across)
        send(f"l{h}", rim, W.at[got, h, :, tail(high)], W.at[got_part, h, :, tail(high)], next_to)
    for c in range(3, CHUNKS - 2):
        forward(c)
    y_recvs(2, 0)
    for h in HALVES:
        spread_last(h)
        recv(f"fp{h}", rim, W.at[got_part, h, :, tail(high)], across)
        recv(f"l{h}", mid, W.at[jnp.where(z == 1, 0, 12), h, :, tail(z == 2)], at(xh, y, jnp.where(z == 1, 0, 3)))
    for flip in (1, 2, 3):
        for i, (_, dst) in enumerate(lists):
            recv(f"c{flip}{i}", None, dst.at[flip], along(flip))
    recv("sib", None, G.at[0], along(1))
    recv("p", outer, G.at[1, around], beside_y)
    send("of", outer, G.at[1, around], G.at[2, around], along(1))
    for c in range(CHUNKS - 2, CHUNKS):
        forward(c)
    for c in range(CHUNKS):
        for name, _, part in pieces(c):
            recv(f"o{name}", None, G.at[2, part], along(1))
    net.finish()
    for copy in local:
        copy.wait()


def gather_all(hop, lists, vec):
    block = vec.shape
    any_space = pl.BlockSpec(memory_space=pl.ANY)
    sems = 104
    return pl.pallas_call(
        gather_kernel,
        out_shape=(
            jax.ShapeDtypeStruct((3,) + hop.shape, hop.dtype),
            jax.ShapeDtypeStruct((13,) + block, vec.dtype),
            *[jax.ShapeDtypeStruct((4,) + a.shape, a.dtype) for a in lists],
            *[jax.ShapeDtypeStruct((2,) + block, vec.dtype)] * 3,
            jax.ShapeDtypeStruct((2, AROUND) + hop.shape[1:], hop.dtype),
        ),
        in_specs=[any_space] * 6,
        out_specs=(any_space,) * 10,
        scratch_shapes=[
            pltpu.SemaphoreType.DMA((sems,)),
            pltpu.SemaphoreType.DMA((sems,)),
            pltpu.SemaphoreType.DMA((4,)),
        ],
        compiler_params=pltpu.CompilerParams(collective_id=0, has_side_effects=True),
        name="gather",
    )(hop, *lists, vec)[:6]


def product_kernel(phase, hop, G, vec, W, CR, CC, CL, CN, out, T, V, H0, H1, O, NR, NC, NL, NN, factor, table, sems):
    row = lax.axis_index("rows")
    copies = [pltpu.make_async_copy(hop, T.at[pl.ds(0, SLOTS)], sems.at[0])]
    for m in range(3):
        copies.append(
            pltpu.make_async_copy(G.at[m], T.at[pl.ds((m + 1) * SLOTS, SLOTS)], sems.at[m + 1])
        )
    H = (H0, H1)
    windows = []
    for j in range(13):
        for q in range(2):
            lanes = pl.ds(q * NV, NV)
            if j == 0:
                src, start, size = W.at[j, :, q, pl.ds(2 * TS, TS)], 0, TS
            elif j == 12:
                src, start, size = W.at[j, :, q, pl.ds(0, TS)], (SPAN - 1) * TS, TS
            else:
                src = vec.at[:, q] if j == 6 else W.at[j, :, q]
                start, size = (TR * (j - 6) + BAND) * TS, BLK
            windows.append(
                pltpu.make_async_copy(src, V.at[:, pl.ds(start, size), lanes], sems.at[4 + 2 * j + q])
            )
    scalars = [
        pltpu.make_async_copy(src, dst, sems.at[30 + i])
        for i, (src, dst) in enumerate(((CR, NR), (CC, NC), (CL, NL), (CN, NN)))
    ]
    for copy in scalars + copies:
        copy.start()
    factor[0:2, :] = jnp.cos(phase[...])
    factor[2:4, :] = jnp.sin(phase[...])
    factors = pltpu.make_async_copy(factor, table, sems.at[34])
    factors.start()

    def clear(i, _):
        rows = pl.ds(pl.multiple_of(i * 8, 8), 8)
        for k in range(2):
            for r in range(TR):
                H[k][r, rows, :] = jnp.zeros((8, WIDE * TS), jnp.float32)
        return 0

    lax.fori_loop(0, 2 * TS // 8, clear, 0)
    for copy in scalars + [factors]:
        copy.wait()
    part = 32
    for m in range(4):
        copies[m].wait()
        if m == 1:
            for copy in windows:
                copy.start()
        count = NN[m, 0, 0]

        def add(i, _, m=m, count=count):
            for one in [GROUP * i + j for j in range(GROUP)]:
                r = jnp.clip(NR[m, 0, one] - row * TR, 0, TR - 1)
                w = NC[m, 0, one] - (row * TR + r - BAND)
                w = jnp.where(w < 0, w + TORB, w)
                w = jnp.clip(jnp.where(w >= TORB, w - TORB, w), 0, WIDE - 1)
                cols = pl.ds(pl.multiple_of(w * TS, TS), TS)
                lat = NL[m, 0, one]
                scale = [jnp.where(one < count, table[2 * p + k, lat], 0.0) for k in range(2) for p in range(2)]
                for at in range(0, TS, part):
                    tile = T[m * SLOTS + one, pl.ds(at, part), :].astype(jnp.float32)
                    for k in range(2):
                        for p in range(2):
                            H[k][r, pl.ds(p * TS + at, part), cols] += tile * scale[2 * k + p]
            return 0

        lax.fori_loop(0, (count + GROUP - 1) // GROUP, add, 0)
    for copy in windows:
        copy.wait()
    done = []
    for k in range(2):
        for r in range(TR):
            o = jnp.dot(
                H[k][r].astype(jnp.bfloat16), V[k, pl.ds(r * TS, WIDE * TS), :], preferred_element_type=jnp.float32
            )
            rows = pl.ds(r * TS, TS)
            O[k, 0, rows, :] = o[:TS, :NV] - o[TS:, NV:]
            O[k, 1, rows, :] = o[:TS, NV:] + o[TS:, :NV]
            done.append(pltpu.make_async_copy(O.at[k, :, rows], out.at[k, :, rows], sems.at[35 + TR * k + r]))
            done[-1].start()
    for copy in done:
        copy.wait()


def product(phase, hop, G, vec, W, lists):
    any_space = pl.BlockSpec(memory_space=pl.ANY)
    return pl.pallas_call(
        product_kernel,
        out_shape=jax.ShapeDtypeStruct((2, 2, BLK, NV), jnp.float32),
        in_specs=[pl.BlockSpec(memory_space=pltpu.VMEM)] + [any_space] * 8,
        out_specs=any_space,
        scratch_shapes=[
            pltpu.VMEM((4 * SLOTS, TS, TS), jnp.bfloat16),
            pltpu.VMEM((2, SPAN * TS, 2 * NV), jnp.bfloat16),
            *[pltpu.VMEM((TR, 2 * TS, WIDE * TS), jnp.float32)] * 2,
            pltpu.VMEM((2, 2, BLK, NV), jnp.float32),
            *[pltpu.SMEM((4, 1, SLOTS), jnp.int32)] * 3,
            pltpu.SMEM((4, 1, 1), jnp.int32),
            pltpu.VMEM((4, NLAT), jnp.float32),
            pltpu.SMEM((4, NLAT), jnp.float32),
            pltpu.SemaphoreType.DMA((41,)),
        ],
        compiler_params=pltpu.CompilerParams(vmem_limit_bytes=60 * 1024 * 1024),
        name="product",
    )(phase, hop, G, vec, W, *lists)


def body(hoppings, tile_rows, tile_cols, tile_lats, tile_counts, phase_angle, vectors):
    hop = hoppings[0]
    G, W, *lists = gather_all(hop, (tile_rows, tile_cols, tile_lats, tile_counts), vectors)
    return product(phase_angle, hop, G, vectors, W, lists)


def solution(mesh):
    return jax.shard_map(
        body,
        mesh=mesh,
        in_specs=(
            P("rows", "ka", None, None),
            P("rows", "ka"),
            P("rows", "ka"),
            P("rows", "ka"),
            P("rows", "ka"),
            P("ka", None),
            P("ka", None, "rows", None),
        ),
        out_specs=P("ka", None, "rows", None),
        check_vma=False,
    )
```

```python
import functools

import jax
import jax.numpy as jnp
from jax import lax
from jax.experimental import pallas as pl
from jax.experimental.pallas import tpu as pltpu
from jax.sharding import PartitionSpec as P

MESH = pl.DeviceIdType.MESH
BAND = 16
NLAT = 9
TS = 128
NV = 256
TR = 3
BLK = TR * TS
SLOTS = 96
CHUNKS = 8
PER = SLOTS // CHUNKS
AROUND = 6
GROUP = 4
WIDE = 2 * BAND + 1
SPAN = WIDE + TR - 1
TORB = 96
HALVES = (0, 1)


class Net:
    def __init__(self, send_sem, recv_sem):
        self.send_sem, self.recv_sem = send_sem, recv_sem
        self.index, self.sent = {}, []

    def copy(self, name, src, dst, device):
        at = self.index.setdefault(name, len(self.index))
        return pltpu.make_async_remote_copy(
            src_ref=src, dst_ref=dst, send_sem=self.send_sem.at[at], recv_sem=self.recv_sem.at[at],
            device_id=device, device_id_type=MESH,
        )

    def send(self, name, when, src, dst, device):
        copy = self.copy(name, src, dst, device)
        self.sent.append((when, copy))
        guarded(when, copy.start)

    def recv(self, name, when, dst, device):
        guarded(when, self.copy(name, dst, dst, device).wait_recv)

    def finish(self):
        for when, copy in self.sent:
            guarded(when, copy.wait_send)


def guarded(when, action):
    if when is None:
        action()
    else:
        pl.when(when)(action)


def gather_kernel(hop, rows, cols, lats, live, vec, G, W, CR, CC, CL, CN, S, X, E, R, send_sem, recv_sem, local_sem):
    ka = lax.axis_index("ka")
    row = lax.axis_index("rows")
    xh, y, z = row // 16, (row // 4) % 4, row % 4
    zp, zm, z2 = (z + 1) % 4, (z + 3) % 4, (z + 2) % 4
    yp, ym = (y + 1) % 4, (y + 3) % 4

    def at(h, i, j):
        return (ka, h * 16 + i * 4 + j)

    def along(flip):
        other = (1 - ka % 2) if flip % 2 else ka % 2
        pair = (1 - ka // 2) if flip // 2 else ka // 2
        return (pair * 2 + other, row)

    up_z, down_z, up_y, down_y = at(xh, y, zp), at(xh, y, zm), at(xh, yp, z), at(xh, ym, z)
    mirror = at(1 - xh, y, z)
    low, high = z == 0, z == 3
    mid = (z == 1) | (z == 2)
    top, base = y == 3, y == 0
    down_y = at(jnp.where(base, 1 - xh, xh), ym, z)
    up_y = at(jnp.where(top, 1 - xh, xh), yp, z)
    inner_y = at(xh, jnp.where(base, 3, jnp.where(top, 0, y)), z)
    crossing = ((y == 1) & high) | ((y == 2) & low)
    part_sender = ((y == 1) & (z == 1)) | ((y == 2) & (z == 2))
    part_to = at(1 - xh, y, jnp.where(y == 1, 3, 0))
    part_from = at(1 - xh, y, jnp.where(y == 1, 1, 2))
    split = ((y == 1) & low) | ((y == 2) & high)
    outer = base | top
    beside_y = at(xh, jnp.where(y < 2, 1 - y, 5 - y), z)
    over = at(xh, jnp.where(y == 1, 0, 3), jnp.where(y == 1, 3, 0))
    over_from = at(xh, jnp.where(base, 1, 2), z)
    split_from = at(xh, jnp.where(base, 1, 2), 3 - z)
    relay = (base & high) | (top & low)
    relayed = (top & high) | (base & low)
    barrier = pltpu.get_barrier_semaphore()

    def greet(peer):
        pl.semaphore_signal(barrier, inc=1, device_id=peer, device_id_type=MESH)

    for peer in (along(1), along(2), along(3), up_z, down_z, up_y, down_y):
        greet(peer)
    pl.when(part_sender)(lambda: greet(part_to))
    pl.when(crossing)(lambda: greet(part_from))
    pl.when(crossing | split)(lambda: greet(mirror))
    pl.when(split)(lambda: greet(over))
    pl.when(relay)(lambda: greet(split_from))
    pl.when(relay | relayed)(lambda: greet(inner_y))
    extra = jnp.where(part_sender, 1, 0) + jnp.where(crossing | split, 2, 0)
    extra = extra + jnp.where(relay | relayed, 1, 0) + jnp.where(relay, 1, 0)
    pl.semaphore_wait(barrier, 7 + extra)

    net = Net(send_sem, recv_sem)
    send, recv = net.send, net.recv
    HEAD, LAST = pl.ds(0, TS), pl.ds(2 * TS, TS)

    def tail(first):
        return pl.ds(pl.multiple_of(jnp.where(first, 0, 2 * TS), TS), TS)

    lists = ((rows, CR), (cols, CC), (lats, CL), (live, CN))
    local = [pltpu.make_async_copy(src, dst.at[0], local_sem.at[i]) for i, (src, dst) in enumerate(lists)]
    local += [pltpu.make_async_copy(vec.at[h], W.at[h, :, 6], local_sem.at[4 + h]) for h in HALVES]
    for copy in local:
        copy.start()

    member = {0: z, -1: zm, 1: zp, 2: z2}

    def y_sends(u, h, only=None):
        dz = member[u] - z
        src = vec.at[h] if u == 0 else W.at[h, :, 6 + dz]
        down_dst, up_dst = W.at[h, :, 10 + dz], W.at[h, :, 2 + dz]
        down_ok, up_ok = (None, None) if u == 0 else (y > 0, y < 3)
        if only is not None:
            down_ok, up_ok = down_ok & only, up_ok & only
        if u == 2:
            send(f"y-{u}{h}", down_ok & (z >= 2), src, down_dst, down_y)
            send(f"y-{u}{h}", down_ok & (z < 2), src.at[:, HEAD], down_dst.at[:, HEAD], down_y)
            send(f"y+{u}{h}", up_ok & (z < 2), src, up_dst, up_y)
            send(f"y+{u}{h}", up_ok & (z >= 2), src.at[:, LAST], up_dst.at[:, LAST], up_y)
        else:
            send(f"y-{u}{h}", down_ok & (z != 0) if u == -1 else down_ok, src, down_dst, down_y)
            send(f"y+{u}{h}", up_ok & (z != 3) if u == 1 else up_ok, src, up_dst, up_y)

    def y_recvs(u, h):
        dz = member[u] - z
        down_dst, up_dst = W.at[h, :, 10 + dz], W.at[h, :, 2 + dz]
        down_ok, up_ok = (None, None) if u == 0 else (y < 3, y > 0)
        if u == 2:
            recv(f"y-{u}{h}", down_ok & (z >= 2), down_dst, up_y)
            recv(f"y-{u}{h}", down_ok & (z < 2), down_dst.at[:, HEAD], up_y)
            recv(f"y+{u}{h}", up_ok & (z < 2), up_dst, down_y)
            recv(f"y+{u}{h}", up_ok & (z >= 2), up_dst.at[:, LAST], down_y)
        else:
            recv(f"y-{u}{h}", down_ok & (z != 0) if u == -1 else down_ok, down_dst, up_y)
            recv(f"y+{u}{h}", up_ok & (z != 3) if u == 1 else up_ok, up_dst, down_y)

    def both(when, ok):
        return ok if when is None else when & ok

    def spread(h):
        a, b = (None, None) if h else (top, base)
        send(f"a1{h}", both(a, z < 3), W.at[h, :, 10], W.at[h, :, 9], up_z)
        send(f"b1{h}", both(b, z > 0), W.at[h, :, 2], W.at[h, :, 3], down_z)
        send(f"a2{h}", a, W.at[h, :, 10], W.at[h, :, jnp.where(low, 7, 11)], down_z)
        send(f"b2{h}", b, W.at[h, :, 2], W.at[h, :, jnp.where(high, 5, 1)], up_z)

    def spread_on(h):
        a, b = (None, None) if h else (top, base)
        recv(f"a1{h}", both(a, z > 0), W.at[h, :, 9], down_z)
        recv(f"b1{h}", both(b, z < 3), W.at[h, :, 3], up_z)
        recv(f"a2{h}", a, W.at[h, :, jnp.where(high, 7, 11)], up_z)
        recv(f"b2{h}", b, W.at[h, :, jnp.where(low, 5, 1)], down_z)
        if h:
            send(f"a3{h}", mid, W.at[h, :, 9], W.at[h, :, 8], up_z)
            send(f"b3{h}", mid, W.at[h, :, 3], W.at[h, :, 4], down_z)
        else:
            send(f"a3{h}", both(a, low | high), W.at[h, :, jnp.where(low, 11, 7)], W.at[h, :, 8], down_z)
            send(f"b3{h}", both(b, low | high), W.at[h, :, jnp.where(low, 5, 1)], W.at[h, :, 4], up_z)
        send(f"a4{h}", both(a, mid), W.at[h, :, 11, HEAD], W.at[h, :, 12, HEAD], down_z)
        send(f"b4{h}", both(b, mid), W.at[h, :, 1, LAST], W.at[h, :, 0, LAST], up_z)

    def spread_last(h):
        a, b = (None, None) if h else (top, base)
        recv(f"a3{h}", both(a, z >= 2), W.at[h, :, 8], down_z)
        recv(f"b3{h}", both(b, z < 2), W.at[h, :, 4], down_z)
        recv(f"a4{h}", both(a, z < 2), W.at[h, :, 12, HEAD], up_z)
        recv(f"b4{h}", both(b, z >= 2), W.at[h, :, 0, LAST], down_z)

    near_to, near_from = (low & (y > 0)) | (high & (y < 3)), (low & (y < 3)) | (high & (y > 0))
    near = at(xh, jnp.where(low, ym, yp), z)
    near_src = at(xh, jnp.where(low, yp, ym), z)
    across = at(xh, y, jnp.where(low, 3, 0))
    across_from = (high & (y < 3)) | (low & (y > 0))
    block, beside = jnp.where(low, 10, 2), jnp.where(low, 11, 1)
    far, far_part = jnp.where(low, 11, 1), jnp.where(low, 12, 0)
    got, got_part = jnp.where(low, 1, 11), jnp.where(low, 0, 12)

    def second(h):
        send(f"d{h}", near_to, W.at[h, :, block], X.at[0, h], near)

    def second_part(h, ok):
        send(f"dp{h}", near_to & ok, W.at[h, :, beside, tail(low)], X.at[1, h, :, tail(low)], near)

    crossed = jnp.where(y == 1, 3, 9)

    def cross():
        send("g0", crossing, W.at[0, :, crossed], S.at[0, 0], mirror)

    y_sends(0, 1)
    send("z-0", None, vec.at[0], W.at[0, :, 6 + z - zp], up_z)
    send("z+1", None, vec.at[1], W.at[1, :, 6 + z - zm], down_z)
    y_sends(0, 0)
    send("z-1", None, vec.at[1], W.at[1, :, 6 + z - zp], up_z)
    send("z+0", None, vec.at[0], W.at[0, :, 6 + z - zm], down_z)
    for h in HALVES:
        send(f"gp{h}", part_sender, vec.at[h, :, tail(y == 1)], S.at[1, h, :, tail(y == 1)], part_to)

    def pieces(c):
        if c < CHUNKS - 1:
            return ((f"{c}", None, pl.ds(c * PER, PER)),)
        end = SLOTS - AROUND
        return (("e", None, pl.ds(c * PER, end - c * PER)), ("f", ~outer, pl.ds(end, AROUND)))

    def chunk(c):
        for name, when, part in pieces(c):
            send(f"x{name}", when, hop.at[part], G.at[1, part], along(2))

    def forward(c):
        for name, when, part in pieces(c):
            recv(f"x{name}", when, G.at[1, part], along(2))
            send(f"o{name}", when, G.at[1, part], G.at[2, part], along(1))

    around = pl.ds(SLOTS - AROUND, AROUND)
    send("g1", split, vec.at[1], S.at[0, 1], mirror)
    send("r", outer, hop.at[around], R.at[0], beside_y)
    for c in range(3):
        chunk(c)
    for flip in (1, 2, 3):
        for i, (src, dst) in enumerate(lists):
            send(f"c{flip}{i}", None, src, dst.at[flip], along(flip))
    send("sib", None, hop, G.at[0], along(1))

    recv("z-0", None, W.at[0, :, 6 + zm - z], down_z)
    send("w0", None, W.at[0, :, 6 + zm - z], W.at[0, :, 6 + zm - zp], up_z)
    y_sends(-1, 0)
    recv("z+1", None, W.at[1, :, 6 + zp - z], up_z)
    send("w1", None, W.at[1, :, 6 + zp - z], W.at[1, :, 6 + zp - zm], down_z)
    recv("g1", split, S.at[0, 1], mirror)
    send("e1", split, S.at[0, 1], E.at[0, 1], over)
    y_recvs(0, 1)
    spread(1)
    second(1)
    recv("z+0", None, W.at[0, :, 6 + zp - z], up_z)
    y_sends(1, 0)
    recv("z-1", None, W.at[1, :, 6 + zm - z], down_z)
    cross()
    recv("r", ~outer, R.at[0], beside_y)
    send("q", ~outer, R.at[0], R.at[1], along(2))
    for c in range(3, CHUNKS):
        chunk(c)
    y_recvs(0, 0)
    second(0)
    spread(0)
    recv("w0", None, W.at[0, :, 6 + z2 - z], down_z)
    y_sends(2, 0, ~crossing)
    recv("w1", None, W.at[1, :, 6 + z2 - z], up_z)
    for h in (1, 0):
        recv(f"d{h}", near_from, X.at[0, h], near_src)
        send(f"f{h}", near_from, X.at[0, h], W.at[h, :, far], across)
    recv("g0", crossing, S.at[0, 0], mirror)
    send("e0", crossing, S.at[0, 0], E.at[0, 0], beside_y)
    y_sends(2, 0, crossing)
    for h in HALVES:
        recv(f"gp{h}", crossing, S.at[1, h, :, tail(y == 1)], part_from)
        send(f"ep{h}", crossing, S.at[1, h, :, tail(y == 1)], E.at[1, h, :, tail(y == 1)], beside_y)
    def onward(h):
        recv(f"e{h}", relay, E.at[0, h], split_from if h else over_from)
        send(f"f{h}", relay, E.at[0, h], W.at[h, :, got], inner_y)

    def onward_part(h):
        recv(f"ep{h}", relay, E.at[1, h, :, tail(high)], over_from)
        send(f"fp{h}", relay, E.at[1, h, :, tail(high)], W.at[h, :, got_part, tail(high)], inner_y)

    y_recvs(-1, 0)
    y_recvs(1, 0)
    second_part(0, (low & (y < 3)) | (high & (y > 0)))
    spread_on(1)
    second_part(1, low | high)
    onward(1)
    onward(0)
    spread_on(0)
    second_part(0, (low & top) | (high & base))
    for h in HALVES:
        onward_part(h)
    recv("q", ~outer, R.at[1], along(2))
    send("p", ~outer, R.at[1], G.at[1, around], beside_y)
    for c in range(3):
        forward(c)
    for h in HALVES:
        recv(f"dp{h}", near_from, X.at[1, h, :, tail(low)], near_src)
        send(f"fp{h}", near_from, X.at[1, h, :, tail(low)], W.at[h, :, far_part, tail(low)], across)
    rim = low | high
    next_to = at(xh, y, jnp.where(low, 1, 2))
    for h in (1, 0):
        recv(f"f{h}", rim, W.at[h, :, got], across)
        send(f"l{h}", rim, W.at[h, :, got, tail(high)], W.at[h, :, got_part, tail(high)], next_to)
    for c in range(3, CHUNKS - 2):
        forward(c)
    y_recvs(2, 0)
    for h in HALVES:
        spread_last(h)
        recv(f"fp{h}", rim, W.at[h, :, got_part, tail(high)], across)
        recv(f"l{h}", mid, W.at[h, :, jnp.where(z == 1, 0, 12), tail(z == 2)], at(xh, y, jnp.where(z == 1, 0, 3)))
    for flip in (1, 2, 3):
        for i, (_, dst) in enumerate(lists):
            recv(f"c{flip}{i}", None, dst.at[flip], along(flip))
    recv("sib", None, G.at[0], along(1))
    recv("p", outer, G.at[1, around], beside_y)
    send("of", outer, G.at[1, around], G.at[2, around], along(1))
    for c in range(CHUNKS - 2, CHUNKS):
        forward(c)
    for c in range(CHUNKS):
        for name, _, part in pieces(c):
            recv(f"o{name}", None, G.at[2, part], along(1))
    net.finish()
    for copy in local:
        copy.wait()


def gather_all(hop, lists, vec):
    block = vec.shape
    any_space = pl.BlockSpec(memory_space=pl.ANY)
    sems = 104
    return pl.pallas_call(
        gather_kernel,
        out_shape=(
            jax.ShapeDtypeStruct((3,) + hop.shape, hop.dtype),
            jax.ShapeDtypeStruct(block[:2] + (13,) + block[2:], vec.dtype),
            *[jax.ShapeDtypeStruct((4,) + a.shape, a.dtype) for a in lists],
            *[jax.ShapeDtypeStruct((2,) + block, vec.dtype)] * 3,
            jax.ShapeDtypeStruct((2, AROUND) + hop.shape[1:], hop.dtype),
        ),
        in_specs=[pl.BlockSpec(memory_space=pltpu.HBM)] * 6,
        out_specs=(any_space,) * 10,
        scratch_shapes=[
            pltpu.SemaphoreType.DMA((sems,)),
            pltpu.SemaphoreType.DMA((sems,)),
            pltpu.SemaphoreType.DMA((6,)),
        ],
        compiler_params=pltpu.CompilerParams(
            collective_id=0, has_side_effects=True, vmem_limit_bytes=1024 * 1024
        ),
        name="gather",
    )(hop, *lists, vec)[:6]


def product_kernel(phase, hop, G, W, CR, CC, CL, CN, out, H0, H1, O, NR, NC, NL, NN, factor, table, sems):
    row = lax.axis_index("rows")
    H = (H0, H1)
    scalars = [
        pltpu.make_async_copy(src, dst, sems.at[30 + i])
        for i, (src, dst) in enumerate(((CR, NR), (CC, NC), (CL, NL), (CN, NN)))
    ]
    for copy in scalars:
        copy.start()
    factor[0:2, :] = jnp.cos(phase[...])
    factor[2:4, :] = jnp.sin(phase[...])
    factors = pltpu.make_async_copy(factor, table, sems.at[34])
    factors.start()

    def clear(i, _):
        rows = pl.ds(pl.multiple_of(i * 8, 8), 8)
        for k in range(2):
            for r in range(TR):
                H[k][r, rows, :] = jnp.zeros((8, WIDE * TS), jnp.float32)
        return 0

    lax.fori_loop(0, 2 * TS // 8, clear, 0)
    for copy in scalars + [factors]:
        copy.wait()
    part = 32
    for m in range(4):
        count = NN[m, 0, 0]
        slots = G.at[m - 1] if m else hop

        def add(i, _, m=m, count=count, slots=slots):
            for one in [GROUP * i + j for j in range(GROUP)]:
                r = jnp.clip(NR[m, 0, one] - row * TR, 0, TR - 1)
                w = NC[m, 0, one] - (row * TR + r - BAND)
                w = jnp.where(w < 0, w + TORB, w)
                w = jnp.clip(jnp.where(w >= TORB, w - TORB, w), 0, WIDE - 1)
                cols = pl.ds(pl.multiple_of(w * TS, TS), TS)
                lat = NL[m, 0, one]
                scale = [jnp.where(one < count, table[2 * p + k, lat], 0.0) for k in range(2) for p in range(2)]
                for at in range(0, TS, part):
                    tile = slots[one, pl.ds(at, part), :].astype(jnp.float32)
                    for k in range(2):
                        for p in range(2):
                            H[k][r, pl.ds(p * TS + at, part), cols] += tile * scale[2 * k + p]
            return 0

        lax.fori_loop(0, (count + GROUP - 1) // GROUP, add, 0)
    done = []
    for k in range(2):
        for r in range(TR):
            left = H[k][r].astype(jnp.bfloat16)
            rows = pl.ds(r * TS, TS)
            first = (r + 2) * TS
            o = [
                jnp.dot(
                    left,
                    W[k, q].reshape(13 * BLK, NV)[first : first + WIDE * TS],
                    preferred_element_type=jnp.float32,
                )
                for q in range(2)
            ]
            O[k, 0, rows, :] = o[0][:TS] - o[1][TS:]
            O[k, 1, rows, :] = o[1][:TS] + o[0][TS:]
            done.append(pltpu.make_async_copy(O.at[k, :, rows], out.at[k, :, rows], sems.at[35 + TR * k + r]))
            done[-1].start()
    for copy in done:
        copy.wait()


def product(phase, hop, G, W, lists):
    any_space = pl.BlockSpec(memory_space=pl.ANY)
    vmem = pl.BlockSpec(memory_space=pltpu.VMEM)
    return pl.pallas_call(
        product_kernel,
        out_shape=jax.ShapeDtypeStruct((2, 2, BLK, NV), jnp.float32),
        in_specs=[vmem] * 4 + [any_space] * 4,
        out_specs=any_space,
        scratch_shapes=[
            *[pltpu.VMEM((TR, 2 * TS, WIDE * TS), jnp.float32)] * 2,
            pltpu.VMEM((2, 2, BLK, NV), jnp.float32),
            *[pltpu.SMEM((4, 1, SLOTS), jnp.int32)] * 3,
            pltpu.SMEM((4, 1, 1), jnp.int32),
            pltpu.VMEM((4, NLAT), jnp.float32),
            pltpu.SMEM((4, NLAT), jnp.float32),
            pltpu.SemaphoreType.DMA((41,)),
        ],
        compiler_params=pltpu.CompilerParams(vmem_limit_bytes=31 * 1024 * 1024),
        name="product",
    )(phase, hop, G, W, *lists)


def body(hoppings, tile_rows, tile_cols, tile_lats, tile_counts, phase_angle, vectors):
    hop = hoppings[0]
    G, W, *lists = gather_all(hop, (tile_rows, tile_cols, tile_lats, tile_counts), vectors)
    return product(phase_angle, hop, G, W, lists)


def solution(mesh):
    return jax.shard_map(
        body,
        mesh=mesh,
        in_specs=(
            P("rows", "ka", None, None),
            P("rows", "ka"),
            P("rows", "ka"),
            P("rows", "ka"),
            P("rows", "ka"),
            P("ka", None),
            P("ka", None, "rows", None),
        ),
        out_specs=P("ka", None, "rows", None),
        check_vma=False,
    )
```

```python
import functools

import jax
import jax.numpy as jnp
from jax import lax
from jax.experimental import pallas as pl
from jax.experimental.pallas import tpu as pltpu
from jax.sharding import PartitionSpec as P

MESH = pl.DeviceIdType.MESH
BAND = 16
NLAT = 9
TS = 128
NV = 256
TR = 3
BLK = TR * TS
SLOTS = 96
CHUNKS = 8
PER = SLOTS // CHUNKS
AROUND = 6
GATHER_VMEM = 1024 * 1024
GROUP = 4
WIDE = 2 * BAND + 1
SPAN = WIDE + TR - 1
TORB = 96
HALVES = (0, 1)


class Net:
    def __init__(self, send_sem, recv_sem):
        self.send_sem, self.recv_sem = send_sem, recv_sem
        self.index, self.sent = {}, []

    def copy(self, name, src, dst, device):
        at = self.index.setdefault(name, len(self.index))
        return pltpu.make_async_remote_copy(
            src_ref=src, dst_ref=dst, send_sem=self.send_sem.at[at], recv_sem=self.recv_sem.at[at],
            device_id=device, device_id_type=MESH,
        )

    def send(self, name, when, src, dst, device):
        copy = self.copy(name, src, dst, device)
        self.sent.append((when, copy))
        guarded(when, copy.start)

    def recv(self, name, when, dst, device):
        guarded(when, self.copy(name, dst, dst, device).wait_recv)

    def finish(self):
        for when, copy in self.sent:
            guarded(when, copy.wait_send)


def guarded(when, action):
    if when is None:
        action()
    else:
        pl.when(when)(action)


def gather_kernel(hop, rows, cols, lats, live, vec, G, W, CR, CC, CL, CN, S, X, E, R, send_sem, recv_sem, local_sem):
    ka = lax.axis_index("ka")
    row = lax.axis_index("rows")
    xh, y, z = row // 16, (row // 4) % 4, row % 4
    zp, zm, z2 = (z + 1) % 4, (z + 3) % 4, (z + 2) % 4
    yp, ym = (y + 1) % 4, (y + 3) % 4

    def at(h, i, j):
        return (ka, h * 16 + i * 4 + j)

    def along(flip):
        other = (1 - ka % 2) if flip % 2 else ka % 2
        pair = (1 - ka // 2) if flip // 2 else ka // 2
        return (pair * 2 + other, row)

    up_z, down_z, up_y, down_y = at(xh, y, zp), at(xh, y, zm), at(xh, yp, z), at(xh, ym, z)
    mirror = at(1 - xh, y, z)
    low, high = z == 0, z == 3
    mid = (z == 1) | (z == 2)
    top, base = y == 3, y == 0
    down_y = at(jnp.where(base, 1 - xh, xh), ym, z)
    up_y = at(jnp.where(top, 1 - xh, xh), yp, z)
    inner_y = at(xh, jnp.where(base, 3, jnp.where(top, 0, y)), z)
    crossing = ((y == 1) & high) | ((y == 2) & low)
    part_sender = ((y == 1) & (z == 1)) | ((y == 2) & (z == 2))
    part_to = at(1 - xh, y, jnp.where(y == 1, 3, 0))
    part_from = at(1 - xh, y, jnp.where(y == 1, 1, 2))
    split = ((y == 1) & low) | ((y == 2) & high)
    outer = base | top
    beside_y = at(xh, jnp.where(y < 2, 1 - y, 5 - y), z)
    over = at(xh, jnp.where(y == 1, 0, 3), jnp.where(y == 1, 3, 0))
    over_from = at(xh, jnp.where(base, 1, 2), z)
    split_from = at(xh, jnp.where(base, 1, 2), 3 - z)
    relay = (base & high) | (top & low)
    relayed = (top & high) | (base & low)
    barrier = pltpu.get_barrier_semaphore()

    def greet(peer):
        pl.semaphore_signal(barrier, inc=1, device_id=peer, device_id_type=MESH)

    for peer in (along(1), along(2), along(3), up_z, down_z, up_y, down_y):
        greet(peer)
    pl.when(part_sender)(lambda: greet(part_to))
    pl.when(crossing)(lambda: greet(part_from))
    pl.when(crossing | split)(lambda: greet(mirror))
    pl.when(split)(lambda: greet(over))
    pl.when(relay)(lambda: greet(split_from))
    pl.when(relay | relayed)(lambda: greet(inner_y))
    extra = jnp.where(part_sender, 1, 0) + jnp.where(crossing | split, 2, 0)
    extra = extra + jnp.where(relay | relayed, 1, 0) + jnp.where(relay, 1, 0)
    pl.semaphore_wait(barrier, 7 + extra)

    net = Net(send_sem, recv_sem)
    send, recv = net.send, net.recv
    HEAD, LAST = pl.ds(0, TS), pl.ds(2 * TS, TS)

    def tail(first):
        return pl.ds(pl.multiple_of(jnp.where(first, 0, 2 * TS), TS), TS)

    lists = ((rows, CR), (cols, CC), (lats, CL), (live, CN))
    local = [pltpu.make_async_copy(src, dst.at[0], local_sem.at[i]) for i, (src, dst) in enumerate(lists)]
    local += [pltpu.make_async_copy(vec.at[h], W.at[h, :, 6], local_sem.at[4 + h]) for h in HALVES]
    local.append(pltpu.make_async_copy(hop, G.at[0], local_sem.at[6]))
    for copy in local:
        copy.start()

    member = {0: z, -1: zm, 1: zp, 2: z2}

    def y_sends(u, h, only=None):
        dz = member[u] - z
        src = vec.at[h] if u == 0 else W.at[h, :, 6 + dz]
        down_dst, up_dst = W.at[h, :, 10 + dz], W.at[h, :, 2 + dz]
        down_ok, up_ok = (None, None) if u == 0 else (y > 0, y < 3)
        if only is not None:
            down_ok, up_ok = down_ok & only, up_ok & only
        if u == 2:
            send(f"y-{u}{h}", down_ok & (z >= 2), src, down_dst, down_y)
            send(f"y-{u}{h}", down_ok & (z < 2), src.at[:, HEAD], down_dst.at[:, HEAD], down_y)
            send(f"y+{u}{h}", up_ok & (z < 2), src, up_dst, up_y)
            send(f"y+{u}{h}", up_ok & (z >= 2), src.at[:, LAST], up_dst.at[:, LAST], up_y)
        else:
            send(f"y-{u}{h}", down_ok & (z != 0) if u == -1 else down_ok, src, down_dst, down_y)
            send(f"y+{u}{h}", up_ok & (z != 3) if u == 1 else up_ok, src, up_dst, up_y)

    def y_recvs(u, h):
        dz = member[u] - z
        down_dst, up_dst = W.at[h, :, 10 + dz], W.at[h, :, 2 + dz]
        down_ok, up_ok = (None, None) if u == 0 else (y < 3, y > 0)
        if u == 2:
            recv(f"y-{u}{h}", down_ok & (z >= 2), down_dst, up_y)
            recv(f"y-{u}{h}", down_ok & (z < 2), down_dst.at[:, HEAD], up_y)
            recv(f"y+{u}{h}", up_ok & (z < 2), up_dst, down_y)
            recv(f"y+{u}{h}", up_ok & (z >= 2), up_dst.at[:, LAST], down_y)
        else:
            recv(f"y-{u}{h}", down_ok & (z != 0) if u == -1 else down_ok, down_dst, up_y)
            recv(f"y+{u}{h}", up_ok & (z != 3) if u == 1 else up_ok, up_dst, down_y)

    def both(when, ok):
        return ok if when is None else when & ok

    def spread(h):
        a, b = (None, None) if h else (top, base)
        send(f"a1{h}", both(a, z < 3), W.at[h, :, 10], W.at[h, :, 9], up_z)
        send(f"b1{h}", both(b, z > 0), W.at[h, :, 2], W.at[h, :, 3], down_z)
        send(f"a2{h}", a, W.at[h, :, 10], W.at[h, :, jnp.where(low, 7, 11)], down_z)
        send(f"b2{h}", b, W.at[h, :, 2], W.at[h, :, jnp.where(high, 5, 1)], up_z)

    def spread_on(h):
        a, b = (None, None) if h else (top, base)
        recv(f"a1{h}", both(a, z > 0), W.at[h, :, 9], down_z)
        recv(f"b1{h}", both(b, z < 3), W.at[h, :, 3], up_z)
        recv(f"a2{h}", a, W.at[h, :, jnp.where(high, 7, 11)], up_z)
        recv(f"b2{h}", b, W.at[h, :, jnp.where(low, 5, 1)], down_z)
        if h:
            send(f"a3{h}", mid, W.at[h, :, 9], W.at[h, :, 8], up_z)
            send(f"b3{h}", mid, W.at[h, :, 3], W.at[h, :, 4], down_z)
        else:
            send(f"a3{h}", both(a, low | high), W.at[h, :, jnp.where(low, 11, 7)], W.at[h, :, 8], down_z)
            send(f"b3{h}", both(b, low | high), W.at[h, :, jnp.where(low, 5, 1)], W.at[h, :, 4], up_z)
        send(f"a4{h}", both(a, mid), W.at[h, :, 11, HEAD], W.at[h, :, 12, HEAD], down_z)
        send(f"b4{h}", both(b, mid), W.at[h, :, 1, LAST], W.at[h, :, 0, LAST], up_z)

    def spread_last(h):
        a, b = (None, None) if h else (top, base)
        recv(f"a3{h}", both(a, z >= 2), W.at[h, :, 8], down_z)
        recv(f"b3{h}", both(b, z < 2), W.at[h, :, 4], down_z)
        recv(f"a4{h}", both(a, z < 2), W.at[h, :, 12, HEAD], up_z)
        recv(f"b4{h}", both(b, z >= 2), W.at[h, :, 0, LAST], down_z)

    near_to, near_from = (low & (y > 0)) | (high & (y < 3)), (low & (y < 3)) | (high & (y > 0))
    near = at(xh, jnp.where(low, ym, yp), z)
    near_src = at(xh, jnp.where(low, yp, ym), z)
    across = at(xh, y, jnp.where(low, 3, 0))
    across_from = (high & (y < 3)) | (low & (y > 0))
    block, beside = jnp.where(low, 10, 2), jnp.where(low, 11, 1)
    far, far_part = jnp.where(low, 11, 1), jnp.where(low, 12, 0)
    got, got_part = jnp.where(low, 1, 11), jnp.where(low, 0, 12)

    def second(h):
        send(f"d{h}", near_to, W.at[h, :, block], X.at[0, h], near)

    def second_part(h, ok):
        send(f"dp{h}", near_to & ok, W.at[h, :, beside, tail(low)], X.at[1, h, :, tail(low)], near)

    crossed = jnp.where(y == 1, 3, 9)

    def cross():
        send("g0", crossing, W.at[0, :, crossed], S.at[0, 0], mirror)

    y_sends(0, 1)
    send("z-0", None, vec.at[0], W.at[0, :, 6 + z - zp], up_z)
    send("z+1", None, vec.at[1], W.at[1, :, 6 + z - zm], down_z)
    y_sends(0, 0)
    send("z-1", None, vec.at[1], W.at[1, :, 6 + z - zp], up_z)
    send("z+0", None, vec.at[0], W.at[0, :, 6 + z - zm], down_z)
    for h in HALVES:
        send(f"gp{h}", part_sender, vec.at[h, :, tail(y == 1)], S.at[1, h, :, tail(y == 1)], part_to)

    def pieces(c):
        if c < CHUNKS - 1:
            return ((f"{c}", None, pl.ds(c * PER, PER)),)
        end = SLOTS - AROUND
        return (("e", None, pl.ds(c * PER, end - c * PER)), ("f", ~outer, pl.ds(end, AROUND)))

    def chunk(c):
        for name, when, part in pieces(c):
            send(f"x{name}", when, hop.at[part], G.at[2, part], along(2))

    def forward(c):
        for name, when, part in pieces(c):
            recv(f"x{name}", when, G.at[2, part], along(2))
            send(f"o{name}", when, G.at[2, part], G.at[3, part], along(1))

    around = pl.ds(SLOTS - AROUND, AROUND)
    send("g1", split, vec.at[1], S.at[0, 1], mirror)
    send("r", outer, hop.at[around], R.at[0], beside_y)
    for c in range(3):
        chunk(c)
    for flip in (1, 2, 3):
        for i, (src, dst) in enumerate(lists):
            send(f"c{flip}{i}", None, src, dst.at[flip], along(flip))
    send("sib", None, hop, G.at[1], along(1))

    recv("z-0", None, W.at[0, :, 6 + zm - z], down_z)
    send("w0", None, W.at[0, :, 6 + zm - z], W.at[0, :, 6 + zm - zp], up_z)
    y_sends(-1, 0)
    recv("z+1", None, W.at[1, :, 6 + zp - z], up_z)
    send("w1", None, W.at[1, :, 6 + zp - z], W.at[1, :, 6 + zp - zm], down_z)
    recv("g1", split, S.at[0, 1], mirror)
    send("e1", split, S.at[0, 1], E.at[0, 1], over)
    y_recvs(0, 1)
    spread(1)
    second(1)
    recv("z+0", None, W.at[0, :, 6 + zp - z], up_z)
    y_sends(1, 0)
    recv("z-1", None, W.at[1, :, 6 + zm - z], down_z)
    cross()
    recv("r", ~outer, R.at[0], beside_y)
    send("q", ~outer, R.at[0], R.at[1], along(2))
    for c in range(3, CHUNKS):
        chunk(c)
    y_recvs(0, 0)
    second(0)
    spread(0)
    recv("w0", None, W.at[0, :, 6 + z2 - z], down_z)
    y_sends(2, 0, ~crossing)
    recv("w1", None, W.at[1, :, 6 + z2 - z], up_z)
    for h in (1, 0):
        recv(f"d{h}", near_from, X.at[0, h], near_src)
        send(f"f{h}", near_from, X.at[0, h], W.at[h, :, far], across)
    recv("g0", crossing, S.at[0, 0], mirror)
    send("e0", crossing, S.at[0, 0], E.at[0, 0], beside_y)
    y_sends(2, 0, crossing)
    for h in HALVES:
        recv(f"gp{h}", crossing, S.at[1, h, :, tail(y == 1)], part_from)
        send(f"ep{h}", crossing, S.at[1, h, :, tail(y == 1)], E.at[1, h, :, tail(y == 1)], beside_y)
    def onward(h):
        recv(f"e{h}", relay, E.at[0, h], split_from if h else over_from)
        send(f"f{h}", relay, E.at[0, h], W.at[h, :, got], inner_y)

    def onward_part(h):
        recv(f"ep{h}", relay, E.at[1, h, :, tail(high)], over_from)
        send(f"fp{h}", relay, E.at[1, h, :, tail(high)], W.at[h, :, got_part, tail(high)], inner_y)

    y_recvs(-1, 0)
    y_recvs(1, 0)
    second_part(0, (low & (y < 3)) | (high & (y > 0)))
    spread_on(1)
    second_part(1, low | high)
    onward(1)
    onward(0)
    spread_on(0)
    second_part(0, (low & top) | (high & base))
    for h in HALVES:
        onward_part(h)
    recv("q", ~outer, R.at[1], along(2))
    send("p", ~outer, R.at[1], G.at[2, around], beside_y)
    for c in range(3):
        forward(c)
    for h in HALVES:
        recv(f"dp{h}", near_from, X.at[1, h, :, tail(low)], near_src)
        send(f"fp{h}", near_from, X.at[1, h, :, tail(low)], W.at[h, :, far_part, tail(low)], across)
    rim = low | high
    next_to = at(xh, y, jnp.where(low, 1, 2))
    for h in (1, 0):
        recv(f"f{h}", rim, W.at[h, :, got], across)
        send(f"l{h}", rim, W.at[h, :, got, tail(high)], W.at[h, :, got_part, tail(high)], next_to)
    for c in range(3, CHUNKS - 2):
        forward(c)
    y_recvs(2, 0)
    for h in HALVES:
        spread_last(h)
        recv(f"fp{h}", rim, W.at[h, :, got_part, tail(high)], across)
        recv(f"l{h}", mid, W.at[h, :, jnp.where(z == 1, 0, 12), tail(z == 2)], at(xh, y, jnp.where(z == 1, 0, 3)))
    for flip in (1, 2, 3):
        for i, (_, dst) in enumerate(lists):
            recv(f"c{flip}{i}", None, dst.at[flip], along(flip))
    recv("sib", None, G.at[1], along(1))
    recv("p", outer, G.at[2, around], beside_y)
    send("of", outer, G.at[2, around], G.at[3, around], along(1))
    for c in range(CHUNKS - 2, CHUNKS):
        forward(c)
    for c in range(CHUNKS):
        for name, _, part in pieces(c):
            recv(f"o{name}", None, G.at[3, part], along(1))
    net.finish()
    for copy in local:
        copy.wait()


def gather_all(hop, lists, vec):
    block = vec.shape
    any_space = pl.BlockSpec(memory_space=pl.ANY)
    sems = 104
    return pl.pallas_call(
        gather_kernel,
        out_shape=(
            pltpu.VMEM((4,) + hop.shape, hop.dtype),
            pltpu.VMEM(block[:2] + (13,) + block[2:], vec.dtype),
            *[jax.ShapeDtypeStruct((4,) + a.shape, a.dtype) for a in lists],
            *[pltpu.VMEM((2,) + block, vec.dtype)] * 3,
            pltpu.VMEM((2, AROUND) + hop.shape[1:], hop.dtype),
        ),
        in_specs=[pl.BlockSpec(memory_space=pltpu.HBM)] * 6,
        out_specs=(any_space,) * 10,
        scratch_shapes=[
            pltpu.SemaphoreType.DMA((sems,)),
            pltpu.SemaphoreType.DMA((sems,)),
            pltpu.SemaphoreType.DMA((7,)),
        ],
        compiler_params=pltpu.CompilerParams(
            collective_id=0, has_side_effects=True, vmem_limit_bytes=GATHER_VMEM
        ),
        name="gather",
    )(*[a if a.size == 1 else pltpu.with_memory_space_constraint(a, pltpu.HBM) for a in (hop, *lists, vec)])[:6]


def product_kernel(phase, G, W, CR, CC, CL, CN, out, H0, H1, O, NR, NC, NL, NN, factor, table, sems):
    row = lax.axis_index("rows")
    H = (H0, H1)
    scalars = [
        pltpu.make_async_copy(src, dst, sems.at[30 + i])
        for i, (src, dst) in enumerate(((CR, NR), (CC, NC), (CL, NL), (CN, NN)))
    ]
    for copy in scalars:
        copy.start()
    factor[0:2, :] = jnp.cos(phase[...])
    factor[2:4, :] = jnp.sin(phase[...])
    factors = pltpu.make_async_copy(factor, table, sems.at[34])
    factors.start()

    def clear(i, _):
        rows = pl.ds(pl.multiple_of(i * 8, 8), 8)
        for k in range(2):
            for r in range(TR):
                H[k][r, rows, :] = jnp.zeros((8, WIDE * TS), jnp.float32)
        return 0

    lax.fori_loop(0, 2 * TS // 8, clear, 0)
    for copy in scalars + [factors]:
        copy.wait()
    part = 32
    for m in range(4):
        count = NN[m, 0, 0]
        slots = G.at[m]

        def add(i, _, m=m, count=count, slots=slots):
            for one in [GROUP * i + j for j in range(GROUP)]:
                r = jnp.clip(NR[m, 0, one] - row * TR, 0, TR - 1)
                w = NC[m, 0, one] - (row * TR + r - BAND)
                w = jnp.where(w < 0, w + TORB, w)
                w = jnp.clip(jnp.where(w >= TORB, w - TORB, w), 0, WIDE - 1)
                cols = pl.ds(pl.multiple_of(w * TS, TS), TS)
                lat = NL[m, 0, one]
                scale = [jnp.where(one < count, table[2 * p + k, lat], 0.0) for k in range(2) for p in range(2)]
                for at in range(0, TS, part):
                    tile = slots[one, pl.ds(at, part), :].astype(jnp.float32)
                    for k in range(2):
                        for p in range(2):
                            H[k][r, pl.ds(p * TS + at, part), cols] += tile * scale[2 * k + p]
            return 0

        lax.fori_loop(0, (count + GROUP - 1) // GROUP, add, 0)
    done = []
    for k in range(2):
        for r in range(TR):
            left = H[k][r].astype(jnp.bfloat16)
            rows = pl.ds(r * TS, TS)
            first = (r + 2) * TS
            o = [
                jnp.dot(
                    left,
                    W[k, q].reshape(13 * BLK, NV)[first : first + WIDE * TS],
                    preferred_element_type=jnp.float32,
                )
                for q in range(2)
            ]
            O[k, 0, rows, :] = o[0][:TS] - o[1][TS:]
            O[k, 1, rows, :] = o[1][:TS] + o[0][TS:]
            done.append(pltpu.make_async_copy(O.at[k, :, rows], out.at[k, :, rows], sems.at[35 + TR * k + r]))
            done[-1].start()
    for copy in done:
        copy.wait()


def product(phase, G, W, lists):
    any_space = pl.BlockSpec(memory_space=pl.ANY)
    vmem = pl.BlockSpec(memory_space=pltpu.VMEM)
    return pl.pallas_call(
        product_kernel,
        out_shape=jax.ShapeDtypeStruct((2, 2, BLK, NV), jnp.float32),
        in_specs=[vmem] * 3 + [any_space] * 4,
        out_specs=any_space,
        scratch_shapes=[
            *[pltpu.VMEM((TR, 2 * TS, WIDE * TS), jnp.float32)] * 2,
            pltpu.VMEM((2, 2, BLK, NV), jnp.float32),
            *[pltpu.SMEM((4, 1, SLOTS), jnp.int32)] * 3,
            pltpu.SMEM((4, 1, 1), jnp.int32),
            pltpu.VMEM((4, NLAT), jnp.float32),
            pltpu.SMEM((4, NLAT), jnp.float32),
            pltpu.SemaphoreType.DMA((41,)),
        ],
        compiler_params=pltpu.CompilerParams(vmem_limit_bytes=31 * 1024 * 1024),
        name="product",
    )(phase, G, W, *lists)


def body(hoppings, tile_rows, tile_cols, tile_lats, tile_counts, phase_angle, vectors):
    hop = hoppings[0]
    G, W, *lists = gather_all(hop, (tile_rows, tile_cols, tile_lats, tile_counts), vectors)
    return product(phase_angle, G, W, lists)


def solution(mesh):
    return jax.shard_map(
        body,
        mesh=mesh,
        in_specs=(
            P("rows", "ka", None, None),
            P("rows", "ka"),
            P("rows", "ka"),
            P("rows", "ka"),
            P("rows", "ka"),
            P("ka", None),
            P("ka", None, "rows", None),
        ),
        out_specs=P("ka", None, "rows", None),
        check_vma=False,
    )
```

```python
import functools

import jax
import jax.numpy as jnp
from jax import lax
from jax.experimental import pallas as pl
from jax.experimental.pallas import tpu as pltpu
from jax.sharding import PartitionSpec as P

MESH = pl.DeviceIdType.MESH
BAND = 16
NLAT = 9
TS = 128
NV = 256
TR = 3
BLK = TR * TS
SLOTS = 96
CHUNKS = 8
PER = SLOTS // CHUNKS
AROUND = 6
GATHER_VMEM = 1024 * 1024
GROUP = 4
DEPTH = 2
CUT = 16
WIDE = 2 * BAND + 1
MATRIX = (TR, 2 * TS, WIDE * TS)
SPAN = WIDE + TR - 1
TORB = 96
HALVES = (0, 1)


class Net:
    def __init__(self, send_sem, recv_sem):
        self.send_sem, self.recv_sem = send_sem, recv_sem
        self.index, self.sent = {}, []

    def copy(self, name, src, dst, device):
        at = self.index.setdefault(name, len(self.index))
        return pltpu.make_async_remote_copy(
            src_ref=src, dst_ref=dst, send_sem=self.send_sem.at[at], recv_sem=self.recv_sem.at[at],
            device_id=device, device_id_type=MESH,
        )

    def send(self, name, when, src, dst, device):
        copy = self.copy(name, src, dst, device)
        self.sent.append((when, copy))
        guarded(when, copy.start)

    def recv(self, name, when, dst, device):
        guarded(when, self.copy(name, dst, dst, device).wait_recv)

    def finish(self):
        for when, copy in self.sent:
            guarded(when, copy.wait_send)


def guarded(when, action):
    if when is None:
        action()
    else:
        pl.when(when)(action)


def gather_kernel(
    angles, hop, rows, cols, lats, live, vec, GA, GB, W, H0, H1, U, CR, CC, CL, CN, S, X, E, R,
    phase, picks, factors, pick, factor, send_sem, recv_sem, local_sem,
):
    ka = lax.axis_index("ka")
    row = lax.axis_index("rows")
    xh, y, z = row // 16, (row // 4) % 4, row % 4
    zp, zm, z2 = (z + 1) % 4, (z + 3) % 4, (z + 2) % 4
    yp, ym = (y + 1) % 4, (y + 3) % 4

    def at(h, i, j):
        return (ka, h * 16 + i * 4 + j)

    def along(flip):
        other = (1 - ka % 2) if flip % 2 else ka % 2
        pair = (1 - ka // 2) if flip // 2 else ka // 2
        return (pair * 2 + other, row)

    up_z, down_z, up_y, down_y = at(xh, y, zp), at(xh, y, zm), at(xh, yp, z), at(xh, ym, z)
    mirror = at(1 - xh, y, z)
    low, high = z == 0, z == 3
    mid = (z == 1) | (z == 2)
    top, base = y == 3, y == 0
    down_y = at(jnp.where(base, 1 - xh, xh), ym, z)
    up_y = at(jnp.where(top, 1 - xh, xh), yp, z)
    inner_y = at(xh, jnp.where(base, 3, jnp.where(top, 0, y)), z)
    crossing = ((y == 1) & high) | ((y == 2) & low)
    part_sender = ((y == 1) & (z == 1)) | ((y == 2) & (z == 2))
    part_to = at(1 - xh, y, jnp.where(y == 1, 3, 0))
    part_from = at(1 - xh, y, jnp.where(y == 1, 1, 2))
    split = ((y == 1) & low) | ((y == 2) & high)
    outer = base | top
    beside_y = at(xh, jnp.where(y < 2, 1 - y, 5 - y), z)
    over = at(xh, jnp.where(y == 1, 0, 3), jnp.where(y == 1, 3, 0))
    over_from = at(xh, jnp.where(base, 1, 2), z)
    split_from = at(xh, jnp.where(base, 1, 2), 3 - z)
    relay = (base & high) | (top & low)
    relayed = (top & high) | (base & low)
    barrier = pltpu.get_barrier_semaphore()

    def greet(peer):
        pl.semaphore_signal(barrier, inc=1, device_id=peer, device_id_type=MESH)

    for peer in (along(1), along(2), along(3), up_z, down_z, up_y, down_y):
        greet(peer)
    pl.when(part_sender)(lambda: greet(part_to))
    pl.when(crossing)(lambda: greet(part_from))
    pl.when(crossing | split)(lambda: greet(mirror))
    pl.when(split)(lambda: greet(over))
    pl.when(relay)(lambda: greet(split_from))
    pl.when(relay | relayed)(lambda: greet(inner_y))
    extra = jnp.where(part_sender, 1, 0) + jnp.where(crossing | split, 2, 0)
    extra = extra + jnp.where(relay | relayed, 1, 0) + jnp.where(relay, 1, 0)
    pl.semaphore_wait(barrier, 7 + extra)

    def window(j, h, part=None):
        shift, size = (0, BLK) if part is None else (part.start, part.size)
        return W.at[h, :, pl.ds(pl.multiple_of((TR * j - 2) * TS + shift, TS), size)]

    net = Net(send_sem, recv_sem)
    send, recv = net.send, net.recv
    HEAD, LAST = pl.ds(0, TS), pl.ds(2 * TS, TS)

    def tail(first):
        return pl.ds(pl.multiple_of(jnp.where(first, 0, 2 * TS), TS), TS)

    lists = ((rows, CR), (cols, CC), (lats, CL), (live, CN))
    local = [pltpu.make_async_copy(src, dst.at[0], local_sem.at[i]) for i, (src, dst) in enumerate(lists)]
    local += [pltpu.make_async_copy(vec.at[h], window(6, h), local_sem.at[4 + h]) for h in HALVES]
    local.append(pltpu.make_async_copy(angles, phase, local_sem.at[9]))
    local.append(pltpu.make_async_copy(hop, GA.at[pl.ds(0, SLOTS)], local_sem.at[6]))
    for copy in local:
        copy.start()

    member = {0: z, -1: zm, 1: zp, 2: z2}

    def y_sends(u, h, only=None):
        dz = member[u] - z
        src = vec.at[h] if u == 0 else window(6 + dz, h)
        down_dst, up_dst = window(10 + dz, h), window(2 + dz, h)
        down_ok, up_ok = (None, None) if u == 0 else (y > 0, y < 3)
        if only is not None:
            down_ok, up_ok = down_ok & only, up_ok & only
        if u == 2:
            send(f"y-{u}{h}", down_ok & (z >= 2), src, down_dst, down_y)
            send(f"y-{u}{h}", down_ok & (z < 2), src.at[:, HEAD], window(10 + dz, h, HEAD), down_y)
            send(f"y+{u}{h}", up_ok & (z < 2), src, up_dst, up_y)
            send(f"y+{u}{h}", up_ok & (z >= 2), src.at[:, LAST], window(2 + dz, h, LAST), up_y)
        else:
            send(f"y-{u}{h}", down_ok & (z != 0) if u == -1 else down_ok, src, down_dst, down_y)
            send(f"y+{u}{h}", up_ok & (z != 3) if u == 1 else up_ok, src, up_dst, up_y)

    def y_recvs(u, h):
        dz = member[u] - z
        down_dst, up_dst = window(10 + dz, h), window(2 + dz, h)
        down_ok, up_ok = (None, None) if u == 0 else (y < 3, y > 0)
        if u == 2:
            recv(f"y-{u}{h}", down_ok & (z >= 2), down_dst, up_y)
            recv(f"y-{u}{h}", down_ok & (z < 2), window(10 + dz, h, HEAD), up_y)
            recv(f"y+{u}{h}", up_ok & (z < 2), up_dst, down_y)
            recv(f"y+{u}{h}", up_ok & (z >= 2), window(2 + dz, h, LAST), down_y)
        else:
            recv(f"y-{u}{h}", down_ok & (z != 0) if u == -1 else down_ok, down_dst, up_y)
            recv(f"y+{u}{h}", up_ok & (z != 3) if u == 1 else up_ok, up_dst, down_y)

    def both(when, ok):
        return ok if when is None else when & ok

    def spread(h):
        a, b = (None, None) if h else (top, base)
        send(f"a1{h}", both(a, z < 3), window(10, h), window(9, h), up_z)
        send(f"b1{h}", both(b, z > 0), window(2, h), window(3, h), down_z)
        send(f"a2{h}", a, window(10, h), window(jnp.where(low, 7, 11), h), down_z)
        send(f"b2{h}", b, window(2, h), window(jnp.where(high, 5, 1), h), up_z)

    def spread_on(h):
        a, b = (None, None) if h else (top, base)
        recv(f"a1{h}", both(a, z > 0), window(9, h), down_z)
        recv(f"b1{h}", both(b, z < 3), window(3, h), up_z)
        recv(f"a2{h}", a, window(jnp.where(high, 7, 11), h), up_z)
        recv(f"b2{h}", b, window(jnp.where(low, 5, 1), h), down_z)
        if h:
            send(f"a3{h}", mid, window(9, h), window(8, h), up_z)
            send(f"b3{h}", mid, window(3, h), window(4, h), down_z)
        else:
            send(f"a3{h}", both(a, low | high), window(jnp.where(low, 11, 7), h), window(8, h), down_z)
            send(f"b3{h}", both(b, low | high), window(jnp.where(low, 5, 1), h), window(4, h), up_z)
        send(f"a4{h}", both(a, mid), window(11, h, HEAD), window(12, h, HEAD), down_z)
        send(f"b4{h}", both(b, mid), window(1, h, LAST), window(0, h, LAST), up_z)

    def spread_last(h):
        a, b = (None, None) if h else (top, base)
        recv(f"a3{h}", both(a, z >= 2), window(8, h), down_z)
        recv(f"b3{h}", both(b, z < 2), window(4, h), down_z)
        recv(f"a4{h}", both(a, z < 2), window(12, h, HEAD), up_z)
        recv(f"b4{h}", both(b, z >= 2), window(0, h, LAST), down_z)

    near_to, near_from = (low & (y > 0)) | (high & (y < 3)), (low & (y < 3)) | (high & (y > 0))
    near = at(xh, jnp.where(low, ym, yp), z)
    near_src = at(xh, jnp.where(low, yp, ym), z)
    across = at(xh, y, jnp.where(low, 3, 0))
    across_from = (high & (y < 3)) | (low & (y > 0))
    block, beside = jnp.where(low, 10, 2), jnp.where(low, 11, 1)
    far, far_part = jnp.where(low, 11, 1), jnp.where(low, 12, 0)
    got, got_part = jnp.where(low, 1, 11), jnp.where(low, 0, 12)

    def second(h):
        send(f"d{h}", near_to, window(block, h), X.at[0, h], near)

    def second_part(h, ok):
        send(f"dp{h}", near_to & ok, window(beside, h, tail(low)), X.at[1, h, :, tail(low)], near)

    crossed = jnp.where(y == 1, 3, 9)

    def cross():
        send("g0", crossing, window(crossed, 0), S.at[0, 0], mirror)

    y_sends(0, 1)
    send("z-0", None, vec.at[0], window(6 + z - zp, 0), up_z)
    send("z+1", None, vec.at[1], window(6 + z - zm, 1), down_z)
    y_sends(0, 0)
    send("z-1", None, vec.at[1], window(6 + z - zp, 1), up_z)
    send("z+0", None, vec.at[0], window(6 + z - zm, 0), down_z)
    for h in HALVES:
        send(f"gp{h}", part_sender, vec.at[h, :, tail(y == 1)], S.at[1, h, :, tail(y == 1)], part_to)

    def pieces(c):
        if c < CHUNKS - 1:
            return ((f"{c}", None, pl.ds(c * PER, PER)),)
        end = SLOTS - AROUND
        return (("e", None, pl.ds(c * PER, end - c * PER)), ("f", ~outer, pl.ds(end, AROUND)))

    def chunk(c):
        for name, when, part in pieces(c):
            send(f"x{name}", when, hop.at[part], GB.at[0, part], along(2))

    def forward(c):
        for name, when, part in pieces(c):
            recv(f"x{name}", when, GB.at[0, part], along(2))
            send(f"o{name}", when, GB.at[0, part], GB.at[1, part], along(1))

    around = pl.ds(SLOTS - AROUND, AROUND)
    send("g1", split, vec.at[1], S.at[0, 1], mirror)
    send("r", outer, hop.at[around], R.at[0], beside_y)
    for c in range(3):
        chunk(c)
    for flip in (1, 2, 3):
        for i, (src, dst) in enumerate(lists):
            send(f"c{flip}{i}", None, src, dst.at[flip], along(flip))
    send("sib", None, hop, GA.at[pl.ds(SLOTS, SLOTS)], along(1))

    def ranked():
        none = 2 * SLOTS
        blocks = lax.broadcasted_iota(jnp.int32, (TS, SLOTS), 0)
        place = lax.broadcasted_iota(jnp.int32, (TS, SLOTS), 1)
        waves = (jnp.cos(phase[...]), jnp.sin(phase[...]))
        found, scales = [], []
        for m in range(2):
            r = CR[m] - row * TR
            w = CC[m] - (row * TR + r - BAND)
            w = jnp.where(w < 0, w + TORB, w)
            w = jnp.where(w >= TORB, w - TORB, w)
            b = jnp.where(place[:1] < CN[m], r * WIDE + w, -1)
            found.append(jnp.where(blocks == b, place + m * SLOTS, none))
            scales.append(
                [
                    sum(jnp.where(CL[m] == n, waves[p][k : k + 1, n : n + 1], 0.0) for n in range(NLAT))
                    for k in range(2)
                    for p in range(2)
                ]
            )
        lane = lax.broadcasted_iota(jnp.int32, (TS, TS), 1)
        chosen, scaled = jnp.zeros((TS, TS), jnp.int32), jnp.zeros((TS, TS), jnp.float32)
        used = [jnp.zeros((TS, SLOTS), jnp.int32)] * 2
        for d in range(DEPTH):
            best = [jnp.min(f, axis=1, keepdims=True) for f in found]
            best = jnp.minimum(best[0], best[1])
            hits = [(f == best) & (f < none) for f in found]
            chosen = jnp.where(lane == d, jnp.where(best < none, best, 0), chosen)
            for j in range(4):
                total = sum(
                    jnp.sum(jnp.where(hits[m], scales[m][j], 0.0), axis=1, keepdims=True) for m in range(2)
                )
                scaled = jnp.where(lane == 4 * d + j, total, scaled)
            used = [jnp.where(hits[m], 1, used[m]) for m in range(2)]
            found = [jnp.where(hits[m], none, found[m]) for m in range(2)]
        picks[...] = chosen
        factors[...] = scaled
        for m in range(2):
            U[m] = jnp.max(used[m], axis=0, keepdims=True)

    tables = [
        pltpu.make_async_copy(picks, pick, local_sem.at[7]),
        pltpu.make_async_copy(factors, factor, local_sem.at[8]),
    ]

    def fill(b, _):
        r = b // WIDE
        columns = pl.ds(pl.multiple_of((b - r * WIDE) * TS, TS), TS)
        chosen = [pick[b, d] for d in range(DEPTH)]
        scale = [[factor[b, 4 * d + j] for j in range(4)] for d in range(DEPTH)]
        size = 32
        for at_row in range(0, TS, size):
            tiles = [GA[c, pl.ds(at_row, size), :].astype(jnp.float32) for c in chosen]
            for k in range(2):
                for p in range(2):
                    total = tiles[0] * scale[0][2 * k + p]
                    for d in range(1, DEPTH):
                        total += tiles[d] * scale[d][2 * k + p]
                    (H0, H1)[k][r, pl.ds(p * TS + at_row, size), columns] = total
        return 0

    filled = [0]

    def some(count):
        start, filled[0] = filled[0], min(filled[0] + count, TR * WIDE)
        lax.fori_loop(start, filled[0], fill, 0)

    recv("z-0", None, window(6 + zm - z, 0), down_z)
    send("w0", None, window(6 + zm - z, 0), window(6 + zm - zp, 0), up_z)
    y_sends(-1, 0)
    recv("z+1", None, window(6 + zp - z, 1), up_z)
    send("w1", None, window(6 + zp - z, 1), window(6 + zp - zm, 1), down_z)
    recv("g1", split, S.at[0, 1], mirror)
    send("e1", split, S.at[0, 1], E.at[0, 1], over)
    y_recvs(0, 1)
    spread(1)
    second(1)
    for i, (_, dst) in enumerate(lists):
        recv(f"c1{i}", None, dst.at[1], along(1))
    recv("sib", None, GA.at[pl.ds(SLOTS, SLOTS)], along(1))
    for copy in local:
        copy.wait()
    ranked()
    for copy in tables:
        copy.start()
    recv("z+0", None, window(6 + zp - z, 0), up_z)
    y_sends(1, 0)
    recv("z-1", None, window(6 + zm - z, 1), down_z)
    cross()
    recv("r", ~outer, R.at[0], beside_y)
    send("q", ~outer, R.at[0], R.at[1], along(2))
    for c in range(3, CHUNKS):
        chunk(c)
    for copy in tables:
        copy.wait()
    some(10)
    y_recvs(0, 0)
    second(0)
    spread(0)
    some(10)
    recv("w0", None, window(6 + z2 - z, 0), down_z)
    y_sends(2, 0, ~crossing)
    some(10)
    recv("w1", None, window(6 + z2 - z, 1), up_z)
    for h in (1, 0):
        recv(f"d{h}", near_from, X.at[0, h], near_src)
        send(f"f{h}", near_from, X.at[0, h], window(far, h), across)
    some(10)
    recv("g0", crossing, S.at[0, 0], mirror)
    send("e0", crossing, S.at[0, 0], E.at[0, 0], beside_y)
    y_sends(2, 0, crossing)
    for h in HALVES:
        recv(f"gp{h}", crossing, S.at[1, h, :, tail(y == 1)], part_from)
        send(f"ep{h}", crossing, S.at[1, h, :, tail(y == 1)], E.at[1, h, :, tail(y == 1)], beside_y)
    def onward(h):
        recv(f"e{h}", relay, E.at[0, h], split_from if h else over_from)
        send(f"f{h}", relay, E.at[0, h], window(got, h), inner_y)

    def onward_part(h):
        recv(f"ep{h}", relay, E.at[1, h, :, tail(high)], over_from)
        send(f"fp{h}", relay, E.at[1, h, :, tail(high)], window(got_part, h, tail(high)), inner_y)

    some(10)
    y_recvs(-1, 0)
    y_recvs(1, 0)
    second_part(0, (low & (y < 3)) | (high & (y > 0)))
    spread_on(1)
    second_part(1, low | high)
    some(10)
    onward(1)
    onward(0)
    some(10)
    spread_on(0)
    second_part(0, (low & top) | (high & base))
    for h in HALVES:
        onward_part(h)
    some(10)
    recv("q", ~outer, R.at[1], along(2))
    send("p", ~outer, R.at[1], GB.at[0, around], beside_y)
    for c in range(3):
        forward(c)
    some(TR * WIDE)
    for h in HALVES:
        recv(f"dp{h}", near_from, X.at[1, h, :, tail(low)], near_src)
        send(f"fp{h}", near_from, X.at[1, h, :, tail(low)], window(far_part, h, tail(low)), across)
    rim = low | high
    next_to = at(xh, y, jnp.where(low, 1, 2))
    for h in (1, 0):
        recv(f"f{h}", rim, window(got, h), across)
        send(f"l{h}", rim, window(got, h, tail(high)), window(got_part, h, tail(high)), next_to)
    for c in range(3, CHUNKS - 2):
        forward(c)
    y_recvs(2, 0)
    for h in HALVES:
        spread_last(h)
        recv(f"fp{h}", rim, window(got_part, h, tail(high)), across)
        recv(f"l{h}", mid, window(jnp.where(z == 1, 0, 12), h, tail(z == 2)), at(xh, y, jnp.where(z == 1, 0, 3)))
    for flip in (2, 3):
        for i, (_, dst) in enumerate(lists):
            recv(f"c{flip}{i}", None, dst.at[flip], along(flip))
    recv("p", outer, GB.at[0, around], beside_y)
    send("of", outer, GB.at[0, around], GB.at[1, around], along(1))
    for c in range(CHUNKS - 2, CHUNKS):
        forward(c)
    for c in range(CHUNKS):
        for name, _, part in pieces(c):
            recv(f"o{name}", None, GB.at[1, part], along(1))
    net.finish()


def gather_all(phase, hop, lists, vec):
    block = vec.shape
    any_space = pl.BlockSpec(memory_space=pl.ANY)
    vmem = pl.BlockSpec(memory_space=pltpu.VMEM)
    sems = 104
    return pl.pallas_call(
        gather_kernel,
        out_shape=(
            pltpu.VMEM((2 * SLOTS,) + hop.shape[1:], hop.dtype),
            pltpu.VMEM((2,) + hop.shape, hop.dtype),
            pltpu.VMEM(block[:2] + (SPAN * TS,) + block[3:], vec.dtype),
            *[pltpu.VMEM(MATRIX, jnp.float32)] * 2,
            pltpu.VMEM((2, 1, SLOTS), jnp.int32),
            *[pltpu.VMEM((4,) + a.shape, a.dtype) for a in lists],
            *[pltpu.HBM((2,) + block, vec.dtype)] * 3,
            pltpu.HBM((2, AROUND) + hop.shape[1:], hop.dtype),
        ),
        in_specs=[pl.BlockSpec(memory_space=pltpu.HBM)] * 7,
        out_specs=(vmem,) + (any_space,) * 2 + (vmem,) * 7 + (any_space,) * 4,
        scratch_shapes=[
            pltpu.VMEM(phase.shape, phase.dtype),
            pltpu.VMEM((TS, TS), jnp.int32),
            pltpu.VMEM((TS, TS), jnp.float32),
            pltpu.SMEM((TS, TS), jnp.int32),
            pltpu.SMEM((TS, TS), jnp.float32),
            pltpu.SemaphoreType.DMA((sems,)),
            pltpu.SemaphoreType.DMA((sems,)),
            pltpu.SemaphoreType.DMA((10,)),
        ],
        compiler_params=pltpu.CompilerParams(
            collective_id=0, has_side_effects=True, vmem_limit_bytes=GATHER_VMEM
        ),
        name="gather",
    )(*[a if a.size == 1 else pltpu.with_memory_space_constraint(a, pltpu.HBM) for a in (phase, hop, *lists, vec)])[:10]


def product_kernel(phase, GA, GB, W, Z0, Z1, U, CR, CC, CL, CN, out, H0, H1, O, NR, NC, NL, NN, NU, rest, factor, table, sems):
    row = lax.axis_index("rows")
    H = (H0, H1)
    scalars = [
        pltpu.make_async_copy(src, dst, sems.at[30 + i])
        for i, (src, dst) in enumerate(((CR, NR), (CC, NC), (CL, NL), (CN, NN), (U, NU)))
    ]
    for copy in scalars:
        copy.start()
    factor[0:2, :] = jnp.cos(phase[...])
    factor[2:4, :] = jnp.sin(phase[...])
    factors = pltpu.make_async_copy(factor, table, sems.at[35])
    factors.start()

    for copy in scalars + [factors]:
        copy.wait()
    part = 32
    left = 0
    for m in range(2):

        def keep(i, n, m=m):
            rest[n] = m * SLOTS + i
            return n + 1 - NU[m, 0, i]

        left = lax.fori_loop(0, NN[m, 0, 0], keep, left)
    for m in (1, 2, 3):
        count = left if m == 1 else NN[m, 0, 0]

        def add(i, _, m=m, count=count):
            for one in [GROUP * i + j for j in range(GROUP)]:
                if m == 1:
                    slot = jnp.where(one < count, rest[one], 0)
                    n = jnp.where(slot >= SLOTS, 1, 0)
                    item, tiles = slot - n * SLOTS, GA.at[slot]
                else:
                    n, item, tiles = m, one, GB.at[m - 2, one]
                r = jnp.clip(NR[n, 0, item] - row * TR, 0, TR - 1)
                w = NC[n, 0, item] - (row * TR + r - BAND)
                w = jnp.where(w < 0, w + TORB, w)
                w = jnp.clip(jnp.where(w >= TORB, w - TORB, w), 0, WIDE - 1)
                cols = pl.ds(pl.multiple_of(w * TS, TS), TS)
                lat = NL[n, 0, item]
                scale = [jnp.where(one < count, table[2 * p + k, lat], 0.0) for k in range(2) for p in range(2)]
                for at in range(0, TS, part):
                    tile = tiles[pl.ds(at, part), :].astype(jnp.float32)
                    for k in range(2):
                        for p in range(2):
                            H[k][r, pl.ds(p * TS + at, part), cols] += tile * scale[2 * k + p]
            return 0

        lax.fori_loop(0, (count + GROUP - 1) // GROUP, add, 0)
    done = []
    for k in range(2):
        for r in range(TR):
            step = TR * k + r
            if step >= 2:
                done[step - 2].wait()
            rows = pl.ds(r * TS, TS)
            o = [jnp.zeros((2 * TS, NV), jnp.float32)] * 2
            for start, size in ((0, CUT), (CUT, WIDE - CUT)):
                left = H[k][r, :, start * TS : (start + size) * TS].astype(jnp.bfloat16)
                first = (r + start) * TS
                o = [
                    o[q]
                    + jnp.dot(
                        left,
                        W[k, q, first : first + size * TS, :],
                        preferred_element_type=jnp.float32,
                    )
                    for q in range(2)
                ]
            O[step % 2, 0] = o[0][:TS] - o[1][TS:]
            O[step % 2, 1] = o[1][:TS] + o[0][TS:]
            done.append(pltpu.make_async_copy(O.at[step % 2], out.at[k, :, rows], sems.at[36 + step]))
            done[-1].start()
    for copy in done[-2:]:
        copy.wait()


def product(phase, GA, GB, W, H0, H1, lists):
    any_space = pl.BlockSpec(memory_space=pl.ANY)
    vmem = pl.BlockSpec(memory_space=pltpu.VMEM)
    return pl.pallas_call(
        product_kernel,
        out_shape=(jax.ShapeDtypeStruct((2, 2, BLK, NV), jnp.float32),) + (pltpu.VMEM(MATRIX, jnp.float32),) * 2,
        input_output_aliases={4: 1, 5: 2},
        in_specs=[vmem] * 6 + [any_space] * 5,
        out_specs=(any_space, vmem, vmem),
        scratch_shapes=[
            pltpu.VMEM((2, 2, TS, NV), jnp.float32),
            *[pltpu.SMEM((4, 1, SLOTS), jnp.int32)] * 3,
            pltpu.SMEM((4, 1, 1), jnp.int32),
            pltpu.SMEM((2, 1, SLOTS), jnp.int32),
            pltpu.SMEM((2 * SLOTS + 8,), jnp.int32),
            pltpu.VMEM((4, NLAT), jnp.float32),
            pltpu.SMEM((4, NLAT), jnp.float32),
            pltpu.SemaphoreType.DMA((42,)),
        ],
        compiler_params=pltpu.CompilerParams(vmem_limit_bytes=4900 * 1024),
        name="product",
    )(phase, GA, GB, W, H0, H1, *lists)[0]


def body(hoppings, tile_rows, tile_cols, tile_lats, tile_counts, phase_angle, vectors):
    hop = hoppings[0]
    GA, GB, W, H0, H1, U, *lists = gather_all(phase_angle, hop, (tile_rows, tile_cols, tile_lats, tile_counts), vectors)
    return product(phase_angle, GA, GB, W, H0, H1, (U, *lists))


def solution(mesh):
    return jax.shard_map(
        body,
        mesh=mesh,
        in_specs=(
            P("rows", "ka", None, None),
            P("rows", "ka"),
            P("rows", "ka"),
            P("rows", "ka"),
            P("rows", "ka"),
            P("ka", None),
            P("ka", None, "rows", None),
        ),
        out_specs=P("ka", None, "rows", None),
        check_vma=False,
    )
```

```python
import functools

import jax
import jax.numpy as jnp
from jax import lax
from jax.experimental import pallas as pl
from jax.experimental.pallas import tpu as pltpu
from jax.sharding import PartitionSpec as P

MESH = pl.DeviceIdType.MESH
BAND = 16
NLAT = 9
TS = 128
NV = 256
TR = 3
BLK = TR * TS
SLOTS = 96
CHUNKS = 8
PER = SLOTS // CHUNKS
AROUND = 6
GATHER_VMEM = 1024 * 1024
GROUP = 4
DEPTH = 3
WIDE = 2 * BAND + 1
MATRIX = (TR, 2 * TS, WIDE * TS)
SPAN = WIDE + TR - 1
TORB = 96
HALVES = (0, 1)


class Net:
    def __init__(self, send_sem, recv_sem):
        self.send_sem, self.recv_sem = send_sem, recv_sem
        self.index, self.sent = {}, []

    def copy(self, name, src, dst, device):
        at = self.index.setdefault(name, len(self.index))
        return pltpu.make_async_remote_copy(
            src_ref=src, dst_ref=dst, send_sem=self.send_sem.at[at], recv_sem=self.recv_sem.at[at],
            device_id=device, device_id_type=MESH,
        )

    def send(self, name, when, src, dst, device):
        copy = self.copy(name, src, dst, device)
        self.sent.append((when, copy))
        guarded(when, copy.start)

    def recv(self, name, when, dst, device):
        guarded(when, self.copy(name, dst, dst, device).wait_recv)

    def finish(self):
        for when, copy in self.sent:
            guarded(when, copy.wait_send)


def guarded(when, action):
    if when is None:
        action()
    else:
        pl.when(when)(action)


def gather_kernel(
    angles, hop, rows, cols, lats, live, vec, GA, GB, W, H0, H1, waves, U, CR, CC, CL, CN, S, X, E, R,
    phase, picks, factors, pick, factor, send_sem, recv_sem, local_sem,
):
    ka = lax.axis_index("ka")
    row = lax.axis_index("rows")
    xh, y, z = row // 16, (row // 4) % 4, row % 4
    zp, zm, z2 = (z + 1) % 4, (z + 3) % 4, (z + 2) % 4
    yp, ym = (y + 1) % 4, (y + 3) % 4

    def at(h, i, j):
        return (ka, h * 16 + i * 4 + j)

    def along(flip):
        other = (1 - ka % 2) if flip % 2 else ka % 2
        pair = (1 - ka // 2) if flip // 2 else ka // 2
        return (pair * 2 + other, row)

    up_z, down_z, up_y, down_y = at(xh, y, zp), at(xh, y, zm), at(xh, yp, z), at(xh, ym, z)
    mirror = at(1 - xh, y, z)
    low, high = z == 0, z == 3
    mid = (z == 1) | (z == 2)
    top, base = y == 3, y == 0
    down_y = at(jnp.where(base, 1 - xh, xh), ym, z)
    up_y = at(jnp.where(top, 1 - xh, xh), yp, z)
    inner_y = at(xh, jnp.where(base, 3, jnp.where(top, 0, y)), z)
    crossing = ((y == 1) & high) | ((y == 2) & low)
    part_sender = ((y == 1) & (z == 1)) | ((y == 2) & (z == 2))
    part_to = at(1 - xh, y, jnp.where(y == 1, 3, 0))
    part_from = at(1 - xh, y, jnp.where(y == 1, 1, 2))
    split = ((y == 1) & low) | ((y == 2) & high)
    outer = base | top
    beside_y = at(xh, jnp.where(y < 2, 1 - y, 5 - y), z)
    over = at(xh, jnp.where(y == 1, 0, 3), jnp.where(y == 1, 3, 0))
    over_from = at(xh, jnp.where(base, 1, 2), z)
    split_from = at(xh, jnp.where(base, 1, 2), 3 - z)
    relay = (base & high) | (top & low)
    relayed = (top & high) | (base & low)
    barrier = pltpu.get_barrier_semaphore()

    def greet(peer):
        pl.semaphore_signal(barrier, inc=1, device_id=peer, device_id_type=MESH)

    for peer in (along(1), along(2), along(3), up_z, down_z, up_y, down_y):
        greet(peer)
    pl.when(part_sender)(lambda: greet(part_to))
    pl.when(crossing)(lambda: greet(part_from))
    pl.when(crossing | split)(lambda: greet(mirror))
    pl.when(split)(lambda: greet(over))
    pl.when(relay)(lambda: greet(split_from))
    pl.when(relay | relayed)(lambda: greet(inner_y))
    extra = jnp.where(part_sender, 1, 0) + jnp.where(crossing | split, 2, 0)
    extra = extra + jnp.where(relay | relayed, 1, 0) + jnp.where(relay, 1, 0)
    pl.semaphore_wait(barrier, 7 + extra)

    def window(j, h, part=None):
        shift, size = (0, BLK) if part is None else (part.start, part.size)
        return W.at[h, :, pl.ds(pl.multiple_of((TR * j - 2) * TS + shift, TS), size)]

    net = Net(send_sem, recv_sem)
    send, recv = net.send, net.recv
    HEAD, LAST = pl.ds(0, TS), pl.ds(2 * TS, TS)

    def tail(first):
        return pl.ds(pl.multiple_of(jnp.where(first, 0, 2 * TS), TS), TS)

    lists = ((rows, CR), (cols, CC), (lats, CL), (live, CN))
    local = [pltpu.make_async_copy(src, dst.at[0], local_sem.at[i]) for i, (src, dst) in enumerate(lists)]
    local += [pltpu.make_async_copy(vec.at[h], window(6, h), local_sem.at[4 + h]) for h in HALVES]
    local.append(pltpu.make_async_copy(angles, phase, local_sem.at[9]))
    local.append(pltpu.make_async_copy(hop, GA.at[pl.ds(0, SLOTS)], local_sem.at[6]))
    for copy in local:
        copy.start()

    member = {0: z, -1: zm, 1: zp, 2: z2}

    def y_sends(u, h, only=None):
        dz = member[u] - z
        src = vec.at[h] if u == 0 else window(6 + dz, h)
        down_dst, up_dst = window(10 + dz, h), window(2 + dz, h)
        down_ok, up_ok = (None, None) if u == 0 else (y > 0, y < 3)
        if only is not None:
            down_ok, up_ok = down_ok & only, up_ok & only
        if u == 2:
            send(f"y-{u}{h}", down_ok & (z >= 2), src, down_dst, down_y)
            send(f"y-{u}{h}", down_ok & (z < 2), src.at[:, HEAD], window(10 + dz, h, HEAD), down_y)
            send(f"y+{u}{h}", up_ok & (z < 2), src, up_dst, up_y)
            send(f"y+{u}{h}", up_ok & (z >= 2), src.at[:, LAST], window(2 + dz, h, LAST), up_y)
        else:
            send(f"y-{u}{h}", down_ok & (z != 0) if u == -1 else down_ok, src, down_dst, down_y)
            send(f"y+{u}{h}", up_ok & (z != 3) if u == 1 else up_ok, src, up_dst, up_y)

    def y_recvs(u, h):
        dz = member[u] - z
        down_dst, up_dst = window(10 + dz, h), window(2 + dz, h)
        down_ok, up_ok = (None, None) if u == 0 else (y < 3, y > 0)
        if u == 2:
            recv(f"y-{u}{h}", down_ok & (z >= 2), down_dst, up_y)
            recv(f"y-{u}{h}", down_ok & (z < 2), window(10 + dz, h, HEAD), up_y)
            recv(f"y+{u}{h}", up_ok & (z < 2), up_dst, down_y)
            recv(f"y+{u}{h}", up_ok & (z >= 2), window(2 + dz, h, LAST), down_y)
        else:
            recv(f"y-{u}{h}", down_ok & (z != 0) if u == -1 else down_ok, down_dst, up_y)
            recv(f"y+{u}{h}", up_ok & (z != 3) if u == 1 else up_ok, up_dst, down_y)

    def both(when, ok):
        return ok if when is None else when & ok

    def spread(h):
        a, b = (None, None) if h else (top, base)
        send(f"a1{h}", both(a, z < 3), window(10, h), window(9, h), up_z)
        send(f"b1{h}", both(b, z > 0), window(2, h), window(3, h), down_z)
        send(f"a2{h}", a, window(10, h), window(jnp.where(low, 7, 11), h), down_z)
        send(f"b2{h}", b, window(2, h), window(jnp.where(high, 5, 1), h), up_z)

    def spread_on(h):
        a, b = (None, None) if h else (top, base)
        recv(f"a1{h}", both(a, z > 0), window(9, h), down_z)
        recv(f"b1{h}", both(b, z < 3), window(3, h), up_z)
        recv(f"a2{h}", a, window(jnp.where(high, 7, 11), h), up_z)
        recv(f"b2{h}", b, window(jnp.where(low, 5, 1), h), down_z)
        if h:
            send(f"a3{h}", mid, window(9, h), window(8, h), up_z)
            send(f"b3{h}", mid, window(3, h), window(4, h), down_z)
        else:
            send(f"a3{h}", both(a, low | high), window(jnp.where(low, 11, 7), h), window(8, h), down_z)
            send(f"b3{h}", both(b, low | high), window(jnp.where(low, 5, 1), h), window(4, h), up_z)
        send(f"a4{h}", both(a, mid), window(11, h, HEAD), window(12, h, HEAD), down_z)
        send(f"b4{h}", both(b, mid), window(1, h, LAST), window(0, h, LAST), up_z)

    def spread_last(h):
        a, b = (None, None) if h else (top, base)
        recv(f"a3{h}", both(a, z >= 2), window(8, h), down_z)
        recv(f"b3{h}", both(b, z < 2), window(4, h), down_z)
        recv(f"a4{h}", both(a, z < 2), window(12, h, HEAD), up_z)
        recv(f"b4{h}", both(b, z >= 2), window(0, h, LAST), down_z)

    near_to, near_from = (low & (y > 0)) | (high & (y < 3)), (low & (y < 3)) | (high & (y > 0))
    near = at(xh, jnp.where(low, ym, yp), z)
    near_src = at(xh, jnp.where(low, yp, ym), z)
    across = at(xh, y, jnp.where(low, 3, 0))
    across_from = (high & (y < 3)) | (low & (y > 0))
    block, beside = jnp.where(low, 10, 2), jnp.where(low, 11, 1)
    far, far_part = jnp.where(low, 11, 1), jnp.where(low, 12, 0)
    got, got_part = jnp.where(low, 1, 11), jnp.where(low, 0, 12)

    def second(h):
        send(f"d{h}", near_to, window(block, h), X.at[0, h], near)

    def second_part(h, ok):
        send(f"dp{h}", near_to & ok, window(beside, h, tail(low)), X.at[1, h, :, tail(low)], near)

    crossed = jnp.where(y == 1, 3, 9)

    def cross():
        send("g0", crossing, window(crossed, 0), S.at[0, 0], mirror)

    y_sends(0, 1)
    send("z-0", None, vec.at[0], window(6 + z - zp, 0), up_z)
    send("z+1", None, vec.at[1], window(6 + z - zm, 1), down_z)
    y_sends(0, 0)
    send("z-1", None, vec.at[1], window(6 + z - zp, 1), up_z)
    send("z+0", None, vec.at[0], window(6 + z - zm, 0), down_z)
    for h in HALVES:
        send(f"gp{h}", part_sender, vec.at[h, :, tail(y == 1)], S.at[1, h, :, tail(y == 1)], part_to)

    def pieces(c):
        if c < CHUNKS - 1:
            return ((f"{c}", None, pl.ds(c * PER, PER)),)
        end = SLOTS - AROUND
        return (("e", None, pl.ds(c * PER, end - c * PER)), ("f", ~outer, pl.ds(end, AROUND)))

    def chunk(c):
        for name, when, part in pieces(c):
            send(f"x{name}", when, hop.at[part], GB.at[0, part], along(2))

    def forward(c):
        for name, when, part in pieces(c):
            recv(f"x{name}", when, GB.at[0, part], along(2))
            send(f"o{name}", when, GB.at[0, part], GB.at[1, part], along(1))

    around = pl.ds(SLOTS - AROUND, AROUND)
    send("g1", split, vec.at[1], S.at[0, 1], mirror)
    send("r", outer, hop.at[around], R.at[0], beside_y)
    for c in range(3):
        chunk(c)
    for flip in (1, 2, 3):
        for i, (src, dst) in enumerate(lists):
            send(f"c{flip}{i}", None, src, dst.at[flip], along(flip))
    send("sib", None, hop, GA.at[pl.ds(SLOTS, SLOTS)], along(1))

    def ranked():
        none = 2 * SLOTS
        blocks = lax.broadcasted_iota(jnp.int32, (TS, SLOTS), 0)
        place = lax.broadcasted_iota(jnp.int32, (TS, SLOTS), 1)
        wave = (jnp.cos(phase[...]), jnp.sin(phase[...]))
        waves[0:2, :], waves[2:4, :] = wave
        found, scales = [], []
        for m in range(2):
            r = CR[m] - row * TR
            w = CC[m] - (row * TR + r - BAND)
            w = jnp.where(w < 0, w + TORB, w)
            w = jnp.where(w >= TORB, w - TORB, w)
            b = jnp.where(place[:1] < CN[m], r * WIDE + w, -1)
            found.append(jnp.where(blocks == b, place + m * SLOTS, none))
            scales.append(
                [
                    sum(jnp.where(CL[m] == n, wave[p][k : k + 1, n : n + 1], 0.0) for n in range(NLAT))
                    for k in range(2)
                    for p in range(2)
                ]
            )
        lane = lax.broadcasted_iota(jnp.int32, (TS, TS), 1)
        chosen, scaled = jnp.zeros((TS, TS), jnp.int32), jnp.zeros((TS, TS), jnp.float32)
        used = [jnp.zeros((TS, SLOTS), jnp.int32)] * 2
        for d in range(DEPTH):
            best = [jnp.min(f, axis=1, keepdims=True) for f in found]
            best = jnp.minimum(best[0], best[1])
            hits = [(f == best) & (f < none) for f in found]
            chosen = jnp.where(lane == d, jnp.where(best < none, best, 0), chosen)
            for j in range(4):
                total = sum(
                    jnp.sum(jnp.where(hits[m], scales[m][j], 0.0), axis=1, keepdims=True) for m in range(2)
                )
                scaled = jnp.where(lane == 4 * d + j, total, scaled)
            used = [jnp.where(hits[m], 1, used[m]) for m in range(2)]
            found = [jnp.where(hits[m], none, found[m]) for m in range(2)]
        picks[...] = chosen
        factors[...] = scaled
        for m in range(2):
            U[m] = jnp.max(used[m], axis=0, keepdims=True)

    tables = [
        pltpu.make_async_copy(picks, pick, local_sem.at[7]),
        pltpu.make_async_copy(factors, factor, local_sem.at[8]),
    ]

    def fill(b, _):
        r = b // WIDE
        columns = pl.ds(pl.multiple_of((b - r * WIDE) * TS, TS), TS)
        chosen = [pick[b, d] for d in range(DEPTH)]
        scale = [[factor[b, 4 * d + j] for j in range(4)] for d in range(DEPTH)]
        size = 32
        for at_row in range(0, TS, size):
            tiles = [GA[c, pl.ds(at_row, size), :].astype(jnp.float32) for c in chosen]
            for k in range(2):
                for p in range(2):
                    total = tiles[0] * scale[0][2 * k + p]
                    for d in range(1, DEPTH):
                        total += tiles[d] * scale[d][2 * k + p]
                    (H0, H1)[k][r, pl.ds(p * TS + at_row, size), columns] = total
        return 0

    filled = [0]

    def some(count):
        start, filled[0] = filled[0], min(filled[0] + count, TR * WIDE)
        lax.fori_loop(start, filled[0], fill, 0)

    recv("z-0", None, window(6 + zm - z, 0), down_z)
    send("w0", None, window(6 + zm - z, 0), window(6 + zm - zp, 0), up_z)
    y_sends(-1, 0)
    recv("z+1", None, window(6 + zp - z, 1), up_z)
    send("w1", None, window(6 + zp - z, 1), window(6 + zp - zm, 1), down_z)
    recv("g1", split, S.at[0, 1], mirror)
    send("e1", split, S.at[0, 1], E.at[0, 1], over)
    y_recvs(0, 1)
    spread(1)
    second(1)
    for i, (_, dst) in enumerate(lists):
        recv(f"c1{i}", None, dst.at[1], along(1))
    recv("sib", None, GA.at[pl.ds(SLOTS, SLOTS)], along(1))
    for copy in local:
        copy.wait()
    ranked()
    for copy in tables:
        copy.start()
    recv("z+0", None, window(6 + zp - z, 0), up_z)
    y_sends(1, 0)
    recv("z-1", None, window(6 + zm - z, 1), down_z)
    cross()
    recv("r", ~outer, R.at[0], beside_y)
    send("q", ~outer, R.at[0], R.at[1], along(2))
    for c in range(3, CHUNKS):
        chunk(c)
    for copy in tables:
        copy.wait()
    some(10)
    y_recvs(0, 0)
    second(0)
    spread(0)
    some(10)
    recv("w0", None, window(6 + z2 - z, 0), down_z)
    y_sends(2, 0, ~crossing)
    some(10)
    recv("w1", None, window(6 + z2 - z, 1), up_z)
    for h in (1, 0):
        recv(f"d{h}", near_from, X.at[0, h], near_src)
        send(f"f{h}", near_from, X.at[0, h], window(far, h), across)
    some(10)
    recv("g0", crossing, S.at[0, 0], mirror)
    send("e0", crossing, S.at[0, 0], E.at[0, 0], beside_y)
    y_sends(2, 0, crossing)
    for h in HALVES:
        recv(f"gp{h}", crossing, S.at[1, h, :, tail(y == 1)], part_from)
        send(f"ep{h}", crossing, S.at[1, h, :, tail(y == 1)], E.at[1, h, :, tail(y == 1)], beside_y)
    def onward(h):
        recv(f"e{h}", relay, E.at[0, h], split_from if h else over_from)
        send(f"f{h}", relay, E.at[0, h], window(got, h), inner_y)

    def onward_part(h):
        recv(f"ep{h}", relay, E.at[1, h, :, tail(high)], over_from)
        send(f"fp{h}", relay, E.at[1, h, :, tail(high)], window(got_part, h, tail(high)), inner_y)

    some(10)
    y_recvs(-1, 0)
    y_recvs(1, 0)
    second_part(0, (low & (y < 3)) | (high & (y > 0)))
    spread_on(1)
    second_part(1, low | high)
    some(10)
    onward(1)
    onward(0)
    some(10)
    spread_on(0)
    second_part(0, (low & top) | (high & base))
    for h in HALVES:
        onward_part(h)
    some(10)
    recv("q", ~outer, R.at[1], along(2))
    send("p", ~outer, R.at[1], GB.at[0, around], beside_y)
    for c in range(3):
        forward(c)
    some(TR * WIDE)
    for h in HALVES:
        recv(f"dp{h}", near_from, X.at[1, h, :, tail(low)], near_src)
        send(f"fp{h}", near_from, X.at[1, h, :, tail(low)], window(far_part, h, tail(low)), across)
    rim = low | high
    next_to = at(xh, y, jnp.where(low, 1, 2))
    for h in (1, 0):
        recv(f"f{h}", rim, window(got, h), across)
        send(f"l{h}", rim, window(got, h, tail(high)), window(got_part, h, tail(high)), next_to)
    for c in range(3, CHUNKS - 2):
        forward(c)
    y_recvs(2, 0)
    for h in HALVES:
        spread_last(h)
        recv(f"fp{h}", rim, window(got_part, h, tail(high)), across)
        recv(f"l{h}", mid, window(jnp.where(z == 1, 0, 12), h, tail(z == 2)), at(xh, y, jnp.where(z == 1, 0, 3)))
    for flip in (2, 3):
        for i, (_, dst) in enumerate(lists):
            recv(f"c{flip}{i}", None, dst.at[flip], along(flip))
    recv("p", outer, GB.at[0, around], beside_y)
    send("of", outer, GB.at[0, around], GB.at[1, around], along(1))
    for c in range(CHUNKS - 2, CHUNKS):
        forward(c)
    for c in range(CHUNKS):
        for name, _, part in pieces(c):
            recv(f"o{name}", None, GB.at[1, part], along(1))
    net.finish()


def gather_all(phase, hop, lists, vec):
    block = vec.shape
    any_space = pl.BlockSpec(memory_space=pl.ANY)
    vmem = pl.BlockSpec(memory_space=pltpu.VMEM)
    sems = 104
    return pl.pallas_call(
        gather_kernel,
        out_shape=(
            pltpu.VMEM((2 * SLOTS,) + hop.shape[1:], hop.dtype),
            pltpu.VMEM((2,) + hop.shape, hop.dtype),
            pltpu.VMEM(block[:2] + (SPAN * TS,) + block[3:], vec.dtype),
            *[pltpu.VMEM(MATRIX, jnp.float32)] * 2,
            pltpu.VMEM((4, NLAT), jnp.float32),
            pltpu.VMEM((2, 1, SLOTS), jnp.int32),
            *[pltpu.VMEM((4,) + a.shape, a.dtype) for a in lists],
            *[pltpu.HBM((2,) + block, vec.dtype)] * 3,
            pltpu.HBM((2, AROUND) + hop.shape[1:], hop.dtype),
        ),
        in_specs=[pl.BlockSpec(memory_space=pltpu.HBM)] * 7,
        out_specs=(vmem,) + (any_space,) * 2 + (vmem,) * 8 + (any_space,) * 4,
        scratch_shapes=[
            pltpu.VMEM(phase.shape, phase.dtype),
            pltpu.VMEM((TS, TS), jnp.int32),
            pltpu.VMEM((TS, TS), jnp.float32),
            pltpu.SMEM((TS, TS), jnp.int32),
            pltpu.SMEM((TS, TS), jnp.float32),
            pltpu.SemaphoreType.DMA((sems,)),
            pltpu.SemaphoreType.DMA((sems,)),
            pltpu.SemaphoreType.DMA((10,)),
        ],
        compiler_params=pltpu.CompilerParams(
            collective_id=0, has_side_effects=True, vmem_limit_bytes=GATHER_VMEM
        ),
        name="gather",
    )(*[a if a.size == 1 else pltpu.with_memory_space_constraint(a, pltpu.HBM) for a in (phase, hop, *lists, vec)])[:11]


def product_kernel(GA, GB, W, Z0, Z1, waves, U, CR, CC, CL, CN, out, H0, H1, O, NR, NC, NL, NN, NU, rest, table, sems):
    row = lax.axis_index("rows")
    H = (H0, H1)
    scalars = [
        pltpu.make_async_copy(src, dst, sems.at[30 + i])
        for i, (src, dst) in enumerate(((CR, NR), (CC, NC), (CL, NL), (CN, NN), (U, NU), (waves, table)))
    ]
    for copy in scalars:
        copy.start()
    for copy in scalars:
        copy.wait()
    part = 32
    left = 0
    for m in range(2):

        def keep(i, n, m=m):
            rest[n] = m * SLOTS + i
            return n + 1 - NU[m, 0, i]

        left = lax.fori_loop(0, NN[m, 0, 0], keep, left)
    for m in (1, 2, 3):
        count = left if m == 1 else NN[m, 0, 0]

        def add(i, _, m=m, count=count):
            for one in [GROUP * i + j for j in range(GROUP)]:
                if m == 1:
                    slot = jnp.where(one < count, rest[one], 0)
                    n = jnp.where(slot >= SLOTS, 1, 0)
                    item, tiles = slot - n * SLOTS, GA.at[slot]
                else:
                    n, item, tiles = m, one, GB.at[m - 2, one]
                r = jnp.clip(NR[n, 0, item] - row * TR, 0, TR - 1)
                w = NC[n, 0, item] - (row * TR + r - BAND)
                w = jnp.where(w < 0, w + TORB, w)
                w = jnp.clip(jnp.where(w >= TORB, w - TORB, w), 0, WIDE - 1)
                cols = pl.ds(pl.multiple_of(w * TS, TS), TS)
                lat = NL[n, 0, item]
                scale = [jnp.where(one < count, table[2 * p + k, lat], 0.0) for k in range(2) for p in range(2)]
                for at in range(0, TS, part):
                    tile = tiles[pl.ds(at, part), :].astype(jnp.float32)
                    for k in range(2):
                        for p in range(2):
                            H[k][r, pl.ds(p * TS + at, part), cols] += tile * scale[2 * k + p]
            return 0

        lax.fori_loop(0, (count + GROUP - 1) // GROUP, add, 0)
    done = []
    for k in range(2):
        for r in range(TR):
            left = H[k][r].astype(jnp.bfloat16)
            rows = pl.ds(r * TS, TS)
            o = [
                jnp.dot(
                    left,
                    W[k, q, r * TS : (r + WIDE) * TS, :],
                    preferred_element_type=jnp.float32,
                )
                for q in range(2)
            ]
            O[k, 0, rows, :] = o[0][:TS] - o[1][TS:]
            O[k, 1, rows, :] = o[1][:TS] + o[0][TS:]
            done.append(pltpu.make_async_copy(O.at[k, :, rows], out.at[k, :, rows], sems.at[36 + TR * k + r]))
            done[-1].start()
    for copy in done:
        copy.wait()


def product(GA, GB, W, H0, H1, lists):
    any_space = pl.BlockSpec(memory_space=pl.ANY)
    vmem = pl.BlockSpec(memory_space=pltpu.VMEM)
    return pl.pallas_call(
        product_kernel,
        out_shape=(jax.ShapeDtypeStruct((2, 2, BLK, NV), jnp.float32),) + (pltpu.VMEM(MATRIX, jnp.float32),) * 2,
        input_output_aliases={3: 1, 4: 2},
        in_specs=[vmem] * 5 + [any_space] * 6,
        out_specs=(any_space, vmem, vmem),
        scratch_shapes=[
            pltpu.VMEM((2, 2, BLK, NV), jnp.float32),
            *[pltpu.SMEM((4, 1, SLOTS), jnp.int32)] * 3,
            pltpu.SMEM((4, 1, 1), jnp.int32),
            pltpu.SMEM((2, 1, SLOTS), jnp.int32),
            pltpu.SMEM((2 * SLOTS + 8,), jnp.int32),
            pltpu.SMEM((4, NLAT), jnp.float32),
            pltpu.SemaphoreType.DMA((42,)),
        ],
        compiler_params=pltpu.CompilerParams(vmem_limit_bytes=5860 * 1024),
        name="product",
    )(GA, GB, W, H0, H1, *lists)[0]


def body(hoppings, tile_rows, tile_cols, tile_lats, tile_counts, phase_angle, vectors):
    hop = hoppings[0]
    GA, GB, W, H0, H1, waves, U, *lists = gather_all(phase_angle, hop, (tile_rows, tile_cols, tile_lats, tile_counts), vectors)
    return product(GA, GB, W, H0, H1, (waves, U, *lists))


def solution(mesh):
    return jax.shard_map(
        body,
        mesh=mesh,
        in_specs=(
            P("rows", "ka", None, None),
            P("rows", "ka"),
            P("rows", "ka"),
            P("rows", "ka"),
            P("rows", "ka"),
            P("ka", None),
            P("ka", None, "rows", None),
        ),
        out_specs=P("ka", None, "rows", None),
        check_vma=False,
    )
```

```python
import functools

import jax
import jax.numpy as jnp
from jax import lax
from jax.experimental import pallas as pl
from jax.experimental.pallas import tpu as pltpu
from jax.sharding import PartitionSpec as P

MESH = pl.DeviceIdType.MESH
BAND = 16
NLAT = 9
TS = 128
NV = 256
TR = 3
BLK = TR * TS
SLOTS = 96
CHUNKS = 8
PER = SLOTS // CHUNKS
AROUND = 6
GATHER_VMEM = 1024 * 1024
GROUP = 4
DEPTH = 3
EARLY = 60
WIDE = 2 * BAND + 1
MATRIX = (TR, 2 * TS, WIDE * TS)
SPAN = WIDE + TR - 1
TORB = 96
HALVES = (0, 1)


class Net:
    def __init__(self, send_sem, recv_sem):
        self.send_sem, self.recv_sem = send_sem, recv_sem
        self.index, self.sent = {}, []

    def copy(self, name, src, dst, device):
        at = self.index.setdefault(name, len(self.index))
        return pltpu.make_async_remote_copy(
            src_ref=src, dst_ref=dst, send_sem=self.send_sem.at[at], recv_sem=self.recv_sem.at[at],
            device_id=device, device_id_type=MESH,
        )

    def send(self, name, when, src, dst, device):
        copy = self.copy(name, src, dst, device)
        self.sent.append((when, copy))
        guarded(when, copy.start)

    def recv(self, name, when, dst, device):
        guarded(when, self.copy(name, dst, dst, device).wait_recv)

    def finish(self):
        for when, copy in self.sent:
            guarded(when, copy.wait_send)


def guarded(when, action):
    if when is None:
        action()
    else:
        pl.when(when)(action)


def gather_kernel(
    angles, hop, rows, cols, lats, live, vec, GA, GE, GL, W, H0, H1, waves, U, CR, CC, CL, CN, S, X, E, R,
    phase, picks, factors, pick, factor, send_sem, recv_sem, local_sem,
):
    ka = lax.axis_index("ka")
    row = lax.axis_index("rows")
    xh, y, z = row // 16, (row // 4) % 4, row % 4
    zp, zm, z2 = (z + 1) % 4, (z + 3) % 4, (z + 2) % 4
    yp, ym = (y + 1) % 4, (y + 3) % 4

    def at(h, i, j):
        return (ka, h * 16 + i * 4 + j)

    def along(flip):
        other = (1 - ka % 2) if flip % 2 else ka % 2
        pair = (1 - ka // 2) if flip // 2 else ka // 2
        return (pair * 2 + other, row)

    up_z, down_z, up_y, down_y = at(xh, y, zp), at(xh, y, zm), at(xh, yp, z), at(xh, ym, z)
    mirror = at(1 - xh, y, z)
    low, high = z == 0, z == 3
    mid = (z == 1) | (z == 2)
    top, base = y == 3, y == 0
    down_y = at(jnp.where(base, 1 - xh, xh), ym, z)
    up_y = at(jnp.where(top, 1 - xh, xh), yp, z)
    inner_y = at(xh, jnp.where(base, 3, jnp.where(top, 0, y)), z)
    crossing = ((y == 1) & high) | ((y == 2) & low)
    part_sender = ((y == 1) & (z == 1)) | ((y == 2) & (z == 2))
    part_to = at(1 - xh, y, jnp.where(y == 1, 3, 0))
    part_from = at(1 - xh, y, jnp.where(y == 1, 1, 2))
    split = ((y == 1) & low) | ((y == 2) & high)
    outer = base | top
    beside_y = at(xh, jnp.where(y < 2, 1 - y, 5 - y), z)
    over = at(xh, jnp.where(y == 1, 0, 3), jnp.where(y == 1, 3, 0))
    over_from = at(xh, jnp.where(base, 1, 2), z)
    split_from = at(xh, jnp.where(base, 1, 2), 3 - z)
    relay = (base & high) | (top & low)
    relayed = (top & high) | (base & low)
    barrier = pltpu.get_barrier_semaphore()

    def greet(peer):
        pl.semaphore_signal(barrier, inc=1, device_id=peer, device_id_type=MESH)

    for peer in (along(1), along(2), along(3), up_z, down_z, up_y, down_y):
        greet(peer)
    pl.when(part_sender)(lambda: greet(part_to))
    pl.when(crossing)(lambda: greet(part_from))
    pl.when(crossing | split)(lambda: greet(mirror))
    pl.when(split)(lambda: greet(over))
    pl.when(relay)(lambda: greet(split_from))
    pl.when(relay | relayed)(lambda: greet(inner_y))
    extra = jnp.where(part_sender, 1, 0) + jnp.where(crossing | split, 2, 0)
    extra = extra + jnp.where(relay | relayed, 1, 0) + jnp.where(relay, 1, 0)
    pl.semaphore_wait(barrier, 7 + extra)

    def window(j, h, part=None):
        shift, size = (0, BLK) if part is None else (part.start, part.size)
        return W.at[h, :, pl.ds(pl.multiple_of((TR * j - 2) * TS + shift, TS), size)]

    net = Net(send_sem, recv_sem)
    send, recv = net.send, net.recv
    HEAD, LAST = pl.ds(0, TS), pl.ds(2 * TS, TS)

    def tail(first):
        return pl.ds(pl.multiple_of(jnp.where(first, 0, 2 * TS), TS), TS)

    lists = ((rows, CR), (cols, CC), (lats, CL), (live, CN))
    local = [pltpu.make_async_copy(src, dst.at[0], local_sem.at[i]) for i, (src, dst) in enumerate(lists)]
    local += [pltpu.make_async_copy(vec.at[h], window(6, h), local_sem.at[4 + h]) for h in HALVES]
    local.append(pltpu.make_async_copy(angles, phase, local_sem.at[9]))
    local.append(pltpu.make_async_copy(hop, GA.at[pl.ds(0, SLOTS)], local_sem.at[6]))
    for copy in local:
        copy.start()

    member = {0: z, -1: zm, 1: zp, 2: z2}

    def y_sends(u, h, only=None):
        dz = member[u] - z
        src = vec.at[h] if u == 0 else window(6 + dz, h)
        down_dst, up_dst = window(10 + dz, h), window(2 + dz, h)
        down_ok, up_ok = (None, None) if u == 0 else (y > 0, y < 3)
        if only is not None:
            down_ok, up_ok = down_ok & only, up_ok & only
        if u == 2:
            send(f"y-{u}{h}", down_ok & (z >= 2), src, down_dst, down_y)
            send(f"y-{u}{h}", down_ok & (z < 2), src.at[:, HEAD], window(10 + dz, h, HEAD), down_y)
            send(f"y+{u}{h}", up_ok & (z < 2), src, up_dst, up_y)
            send(f"y+{u}{h}", up_ok & (z >= 2), src.at[:, LAST], window(2 + dz, h, LAST), up_y)
        else:
            send(f"y-{u}{h}", down_ok & (z != 0) if u == -1 else down_ok, src, down_dst, down_y)
            send(f"y+{u}{h}", up_ok & (z != 3) if u == 1 else up_ok, src, up_dst, up_y)

    def y_recvs(u, h):
        dz = member[u] - z
        down_dst, up_dst = window(10 + dz, h), window(2 + dz, h)
        down_ok, up_ok = (None, None) if u == 0 else (y < 3, y > 0)
        if u == 2:
            recv(f"y-{u}{h}", down_ok & (z >= 2), down_dst, up_y)
            recv(f"y-{u}{h}", down_ok & (z < 2), window(10 + dz, h, HEAD), up_y)
            recv(f"y+{u}{h}", up_ok & (z < 2), up_dst, down_y)
            recv(f"y+{u}{h}", up_ok & (z >= 2), window(2 + dz, h, LAST), down_y)
        else:
            recv(f"y-{u}{h}", down_ok & (z != 0) if u == -1 else down_ok, down_dst, up_y)
            recv(f"y+{u}{h}", up_ok & (z != 3) if u == 1 else up_ok, up_dst, down_y)

    def both(when, ok):
        return ok if when is None else when & ok

    def spread(h):
        a, b = (None, None) if h else (top, base)
        send(f"a1{h}", both(a, z < 3), window(10, h), window(9, h), up_z)
        send(f"b1{h}", both(b, z > 0), window(2, h), window(3, h), down_z)
        send(f"a2{h}", a, window(10, h), window(jnp.where(low, 7, 11), h), down_z)
        send(f"b2{h}", b, window(2, h), window(jnp.where(high, 5, 1), h), up_z)

    def spread_on(h):
        a, b = (None, None) if h else (top, base)
        recv(f"a1{h}", both(a, z > 0), window(9, h), down_z)
        recv(f"b1{h}", both(b, z < 3), window(3, h), up_z)
        recv(f"a2{h}", a, window(jnp.where(high, 7, 11), h), up_z)
        recv(f"b2{h}", b, window(jnp.where(low, 5, 1), h), down_z)
        if h:
            send(f"a3{h}", mid, window(9, h), window(8, h), up_z)
            send(f"b3{h}", mid, window(3, h), window(4, h), down_z)
        else:
            send(f"a3{h}", both(a, low | high), window(jnp.where(low, 11, 7), h), window(8, h), down_z)
            send(f"b3{h}", both(b, low | high), window(jnp.where(low, 5, 1), h), window(4, h), up_z)
        send(f"a4{h}", both(a, mid), window(11, h, HEAD), window(12, h, HEAD), down_z)
        send(f"b4{h}", both(b, mid), window(1, h, LAST), window(0, h, LAST), up_z)

    def spread_last(h):
        a, b = (None, None) if h else (top, base)
        recv(f"a3{h}", both(a, z >= 2), window(8, h), down_z)
        recv(f"b3{h}", both(b, z < 2), window(4, h), down_z)
        recv(f"a4{h}", both(a, z < 2), window(12, h, HEAD), up_z)
        recv(f"b4{h}", both(b, z >= 2), window(0, h, LAST), down_z)

    near_to, near_from = (low & (y > 0)) | (high & (y < 3)), (low & (y < 3)) | (high & (y > 0))
    near = at(xh, jnp.where(low, ym, yp), z)
    near_src = at(xh, jnp.where(low, yp, ym), z)
    across = at(xh, y, jnp.where(low, 3, 0))
    across_from = (high & (y < 3)) | (low & (y > 0))
    block, beside = jnp.where(low, 10, 2), jnp.where(low, 11, 1)
    far, far_part = jnp.where(low, 11, 1), jnp.where(low, 12, 0)
    got, got_part = jnp.where(low, 1, 11), jnp.where(low, 0, 12)

    def second(h):
        send(f"d{h}", near_to, window(block, h), X.at[0, h], near)

    def second_part(h, ok):
        send(f"dp{h}", near_to & ok, window(beside, h, tail(low)), X.at[1, h, :, tail(low)], near)

    crossed = jnp.where(y == 1, 3, 9)

    def cross():
        send("g0", crossing, window(crossed, 0), S.at[0, 0], mirror)

    y_sends(0, 1)
    send("z-0", None, vec.at[0], window(6 + z - zp, 0), up_z)
    send("z+1", None, vec.at[1], window(6 + z - zm, 1), down_z)
    y_sends(0, 0)
    send("z-1", None, vec.at[1], window(6 + z - zp, 1), up_z)
    send("z+0", None, vec.at[0], window(6 + z - zm, 0), down_z)
    for h in HALVES:
        send(f"gp{h}", part_sender, vec.at[h, :, tail(y == 1)], S.at[1, h, :, tail(y == 1)], part_to)

    def remote(n, part):
        if part.start < EARLY:
            return GE.at[pl.ds(n * EARLY + part.start, part.size)]
        return GL.at[n, pl.ds(part.start - EARLY, part.size)]

    def pieces(c):
        if c < CHUNKS - 1:
            return ((f"{c}", None, pl.ds(c * PER, PER)),)
        end = SLOTS - AROUND
        return (("e", None, pl.ds(c * PER, end - c * PER)), ("f", ~outer, pl.ds(end, AROUND)))

    def chunk(c):
        for name, when, part in pieces(c):
            send(f"x{name}", when, hop.at[part], remote(0, part), along(2))

    def forward(c):
        for name, when, part in pieces(c):
            recv(f"x{name}", when, remote(0, part), along(2))
            send(f"o{name}", when, remote(0, part), remote(1, part), along(1))

    around = pl.ds(SLOTS - AROUND, AROUND)
    send("g1", split, vec.at[1], S.at[0, 1], mirror)
    send("r", outer, hop.at[around], R.at[0], beside_y)
    for c in range(3):
        chunk(c)
    for flip in (1, 2, 3):
        for i, (src, dst) in enumerate(lists):
            send(f"c{flip}{i}", None, src, dst.at[flip], along(flip))
    send("sib", None, hop, GA.at[pl.ds(SLOTS, SLOTS)], along(1))

    def ranked(pair, extent, depth):
        none = 2 * extent
        blocks = lax.broadcasted_iota(jnp.int32, (TS, SLOTS), 0)
        place = lax.broadcasted_iota(jnp.int32, (TS, SLOTS), 1)
        wave = (jnp.cos(phase[...]), jnp.sin(phase[...]))
        waves[0:2, :], waves[2:4, :] = wave
        found, scales = [], []
        for n, m in enumerate(pair):
            r = CR[m] - row * TR
            w = CC[m] - (row * TR + r - BAND)
            w = jnp.where(w < 0, w + TORB, w)
            w = jnp.where(w >= TORB, w - TORB, w)
            b = jnp.where(place[:1] < jnp.minimum(CN[m], extent), r * WIDE + w, -1)
            found.append(jnp.where(blocks == b, place + n * extent, none))
            scales.append(
                [
                    sum(jnp.where(CL[m] == v, wave[p][k : k + 1, v : v + 1], 0.0) for v in range(NLAT))
                    for k in range(2)
                    for p in range(2)
                ]
            )
        lane = lax.broadcasted_iota(jnp.int32, (TS, TS), 1)
        chosen, scaled = jnp.zeros((TS, TS), jnp.int32), jnp.zeros((TS, TS), jnp.float32)
        used = [jnp.zeros((TS, SLOTS), jnp.int32)] * 2
        for d in range(depth):
            best = [jnp.min(f, axis=1, keepdims=True) for f in found]
            best = jnp.minimum(best[0], best[1])
            hits = [(f == best) & (f < none) for f in found]
            chosen = jnp.where(lane == d, jnp.where(best < none, best, 0), chosen)
            for j in range(4):
                total = sum(
                    jnp.sum(jnp.where(hits[m], scales[m][j], 0.0), axis=1, keepdims=True) for m in range(2)
                )
                scaled = jnp.where(lane == 4 * d + j, total, scaled)
            used = [jnp.where(hits[m], 1, used[m]) for m in range(2)]
            found = [jnp.where(hits[m], none, found[m]) for m in range(2)]
        picks[...] = chosen
        factors[...] = scaled
        for n, m in enumerate(pair):
            U[m] = jnp.max(used[n], axis=0, keepdims=True)

    tables = [
        pltpu.make_async_copy(picks, pick, local_sem.at[7]),
        pltpu.make_async_copy(factors, factor, local_sem.at[8]),
    ]

    def fill(b, source, depth, more):
        r = b // WIDE
        columns = pl.ds(pl.multiple_of((b - r * WIDE) * TS, TS), TS)
        chosen = [pick[b, d] for d in range(depth)]
        scale = [[factor[b, 4 * d + j] for j in range(4)] for d in range(depth)]
        size = 32
        for at_row in range(0, TS, size):
            tiles = [source[c, pl.ds(at_row, size), :].astype(jnp.float32) for c in chosen]
            for k in range(2):
                for p in range(2):
                    total = tiles[0] * scale[0][2 * k + p]
                    for d in range(1, depth):
                        total += tiles[d] * scale[d][2 * k + p]
                    where = (r, pl.ds(p * TS + at_row, size), columns)
                    if more:
                        total += (H0, H1)[k][where]
                    (H0, H1)[k][where] = total
        return 0

    filled = [0]

    def some(count):
        start, filled[0] = filled[0], min(filled[0] + count, TR * WIDE)
        lax.fori_loop(start, filled[0], lambda b, _: fill(b, GA, DEPTH, False), 0)

    recv("z-0", None, window(6 + zm - z, 0), down_z)
    send("w0", None, window(6 + zm - z, 0), window(6 + zm - zp, 0), up_z)
    y_sends(-1, 0)
    recv("z+1", None, window(6 + zp - z, 1), up_z)
    send("w1", None, window(6 + zp - z, 1), window(6 + zp - zm, 1), down_z)
    recv("g1", split, S.at[0, 1], mirror)
    send("e1", split, S.at[0, 1], E.at[0, 1], over)
    y_recvs(0, 1)
    spread(1)
    second(1)
    for i, (_, dst) in enumerate(lists):
        recv(f"c1{i}", None, dst.at[1], along(1))
    recv("sib", None, GA.at[pl.ds(SLOTS, SLOTS)], along(1))
    for copy in local:
        copy.wait()
    ranked((0, 1), SLOTS, DEPTH)
    for copy in tables:
        copy.start()
    recv("z+0", None, window(6 + zp - z, 0), up_z)
    y_sends(1, 0)
    recv("z-1", None, window(6 + zm - z, 1), down_z)
    cross()
    recv("r", ~outer, R.at[0], beside_y)
    send("q", ~outer, R.at[0], R.at[1], along(2))
    for c in range(3, CHUNKS):
        chunk(c)
    for copy in tables:
        copy.wait()
    some(10)
    y_recvs(0, 0)
    second(0)
    spread(0)
    some(10)
    recv("w0", None, window(6 + z2 - z, 0), down_z)
    y_sends(2, 0, ~crossing)
    some(10)
    recv("w1", None, window(6 + z2 - z, 1), up_z)
    for h in (1, 0):
        recv(f"d{h}", near_from, X.at[0, h], near_src)
        send(f"f{h}", near_from, X.at[0, h], window(far, h), across)
    some(10)
    recv("g0", crossing, S.at[0, 0], mirror)
    send("e0", crossing, S.at[0, 0], E.at[0, 0], beside_y)
    y_sends(2, 0, crossing)
    for h in HALVES:
        recv(f"gp{h}", crossing, S.at[1, h, :, tail(y == 1)], part_from)
        send(f"ep{h}", crossing, S.at[1, h, :, tail(y == 1)], E.at[1, h, :, tail(y == 1)], beside_y)
    def onward(h):
        recv(f"e{h}", relay, E.at[0, h], split_from if h else over_from)
        send(f"f{h}", relay, E.at[0, h], window(got, h), inner_y)

    def onward_part(h):
        recv(f"ep{h}", relay, E.at[1, h, :, tail(high)], over_from)
        send(f"fp{h}", relay, E.at[1, h, :, tail(high)], window(got_part, h, tail(high)), inner_y)

    some(10)
    y_recvs(-1, 0)
    y_recvs(1, 0)
    second_part(0, (low & (y < 3)) | (high & (y > 0)))
    spread_on(1)
    second_part(1, low | high)
    some(10)
    onward(1)
    onward(0)
    some(10)
    spread_on(0)
    second_part(0, (low & top) | (high & base))
    for h in HALVES:
        onward_part(h)
    some(10)
    recv("q", ~outer, R.at[1], along(2))
    send("p", ~outer, R.at[1], remote(0, around), beside_y)
    for c in range(3):
        forward(c)
    some(TR * WIDE)
    for h in HALVES:
        recv(f"dp{h}", near_from, X.at[1, h, :, tail(low)], near_src)
        send(f"fp{h}", near_from, X.at[1, h, :, tail(low)], window(far_part, h, tail(low)), across)
    rim = low | high
    next_to = at(xh, y, jnp.where(low, 1, 2))
    for h in (1, 0):
        recv(f"f{h}", rim, window(got, h), across)
        send(f"l{h}", rim, window(got, h, tail(high)), window(got_part, h, tail(high)), next_to)
    for c in range(3, EARLY // PER):
        forward(c)
    for flip in (2, 3):
        for i, (_, dst) in enumerate(lists):
            recv(f"c{flip}{i}", None, dst.at[flip], along(flip))
    for c in range(EARLY // PER):
        for name, _, part in pieces(c):
            recv(f"o{name}", None, remote(1, part), along(1))
    ranked((2, 3), EARLY, DEPTH - 1)
    for copy in tables:
        copy.start()
    for copy in tables:
        copy.wait()
    lax.fori_loop(0, TR * WIDE, lambda b, _: fill(b, GE, DEPTH - 1, True), 0)
    for c in range(EARLY // PER, CHUNKS - 2):
        forward(c)
    y_recvs(2, 0)
    for h in HALVES:
        spread_last(h)
        recv(f"fp{h}", rim, window(got_part, h, tail(high)), across)
        recv(f"l{h}", mid, window(jnp.where(z == 1, 0, 12), h, tail(z == 2)), at(xh, y, jnp.where(z == 1, 0, 3)))
    recv("p", outer, remote(0, around), beside_y)
    send("of", outer, remote(0, around), remote(1, around), along(1))
    for c in range(CHUNKS - 2, CHUNKS):
        forward(c)
    for c in range(EARLY // PER, CHUNKS):
        for name, _, part in pieces(c):
            recv(f"o{name}", None, remote(1, part), along(1))
    net.finish()


def gather_all(phase, hop, lists, vec):
    block = vec.shape
    any_space = pl.BlockSpec(memory_space=pl.ANY)
    vmem = pl.BlockSpec(memory_space=pltpu.VMEM)
    sems = 104
    return pl.pallas_call(
        gather_kernel,
        out_shape=(
            pltpu.VMEM((2 * SLOTS,) + hop.shape[1:], hop.dtype),
            pltpu.VMEM((2 * EARLY,) + hop.shape[1:], hop.dtype),
            pltpu.VMEM((2, SLOTS - EARLY) + hop.shape[1:], hop.dtype),
            pltpu.VMEM(block[:2] + (SPAN * TS,) + block[3:], vec.dtype),
            *[pltpu.VMEM(MATRIX, jnp.float32)] * 2,
            pltpu.VMEM((4, NLAT), jnp.float32),
            pltpu.VMEM((4, 1, SLOTS), jnp.int32),
            *[pltpu.VMEM((4,) + a.shape, a.dtype) for a in lists],
            *[pltpu.HBM((2,) + block, vec.dtype)] * 3,
            pltpu.HBM((2, AROUND) + hop.shape[1:], hop.dtype),
        ),
        in_specs=[pl.BlockSpec(memory_space=pltpu.HBM)] * 7,
        out_specs=(vmem,) * 2 + (any_space,) * 2 + (vmem,) * 8 + (any_space,) * 4,
        scratch_shapes=[
            pltpu.VMEM(phase.shape, phase.dtype),
            pltpu.VMEM((TS, TS), jnp.int32),
            pltpu.VMEM((TS, TS), jnp.float32),
            pltpu.SMEM((TS, TS), jnp.int32),
            pltpu.SMEM((TS, TS), jnp.float32),
            pltpu.SemaphoreType.DMA((sems,)),
            pltpu.SemaphoreType.DMA((sems,)),
            pltpu.SemaphoreType.DMA((10,)),
        ],
        compiler_params=pltpu.CompilerParams(
            collective_id=0, has_side_effects=True, vmem_limit_bytes=GATHER_VMEM
        ),
        name="gather",
    )(*[a if a.size == 1 else pltpu.with_memory_space_constraint(a, pltpu.HBM) for a in (phase, hop, *lists, vec)])[:12]


def product_kernel(GA, GE, GL, W, Z0, Z1, waves, U, CR, CC, CL, CN, out, H0, H1, O, NR, NC, NL, NN, NU, rest, table, sems):
    row = lax.axis_index("rows")
    H = (H0, H1)
    scalars = [
        pltpu.make_async_copy(src, dst, sems.at[30 + i])
        for i, (src, dst) in enumerate(((CR, NR), (CC, NC), (CL, NL), (CN, NN), (U, NU), (waves, table)))
    ]
    for copy in scalars:
        copy.start()
    for copy in scalars:
        copy.wait()
    part = 32
    def passed(pair, extent):
        count = 0
        for m in pair:

            def keep(i, n, m=m):
                rest[n] = m * SLOTS + i
                return n + 1 - NU[m, 0, i]

            count = lax.fori_loop(0, jnp.minimum(NN[m, 0, 0], extent), keep, count)
        return count

    for group in range(4):
        if group < 2:
            count = passed((2 * group, 2 * group + 1), (SLOTS, EARLY)[group])
        else:
            count = jnp.maximum(NN[group, 0, 0] - EARLY, 0)

        def add(i, _, group=group, count=count):
            for one in [GROUP * i + j for j in range(GROUP)]:
                if group < 2:
                    slot = jnp.where(one < count, rest[one], 2 * group * SLOTS)
                    n = jnp.where(slot >= (2 * group + 1) * SLOTS, 2 * group + 1, 2 * group)
                    item = slot - n * SLOTS
                    tiles = GE.at[item + (n - 2) * EARLY] if group else GA.at[slot]
                else:
                    late = jnp.minimum(one, SLOTS - EARLY - 1)
                    n, item, tiles = group, late + EARLY, GL.at[group - 2, late]
                r = jnp.clip(NR[n, 0, item] - row * TR, 0, TR - 1)
                w = NC[n, 0, item] - (row * TR + r - BAND)
                w = jnp.where(w < 0, w + TORB, w)
                w = jnp.clip(jnp.where(w >= TORB, w - TORB, w), 0, WIDE - 1)
                cols = pl.ds(pl.multiple_of(w * TS, TS), TS)
                lat = NL[n, 0, item]
                scale = [jnp.where(one < count, table[2 * p + k, lat], 0.0) for k in range(2) for p in range(2)]
                for at in range(0, TS, part):
                    tile = tiles[pl.ds(at, part), :].astype(jnp.float32)
                    for k in range(2):
                        for p in range(2):
                            H[k][r, pl.ds(p * TS + at, part), cols] += tile * scale[2 * k + p]
            return 0

        lax.fori_loop(0, (count + GROUP - 1) // GROUP, add, 0)
    done = []
    for k in range(2):
        for r in range(TR):
            left = H[k][r].astype(jnp.bfloat16)
            rows = pl.ds(r * TS, TS)
            o = [
                jnp.dot(
                    left,
                    W[k, q, r * TS : (r + WIDE) * TS, :],
                    preferred_element_type=jnp.float32,
                )
                for q in range(2)
            ]
            O[k, 0, rows, :] = o[0][:TS] - o[1][TS:]
            O[k, 1, rows, :] = o[1][:TS] + o[0][TS:]
            done.append(pltpu.make_async_copy(O.at[k, :, rows], out.at[k, :, rows], sems.at[36 + TR * k + r]))
            done[-1].start()
    for copy in done:
        copy.wait()


def product(GA, GE, GL, W, H0, H1, lists):
    any_space = pl.BlockSpec(memory_space=pl.ANY)
    vmem = pl.BlockSpec(memory_space=pltpu.VMEM)
    return pl.pallas_call(
        product_kernel,
        out_shape=(jax.ShapeDtypeStruct((2, 2, BLK, NV), jnp.float32),) + (pltpu.VMEM(MATRIX, jnp.float32),) * 2,
        input_output_aliases={4: 1, 5: 2},
        in_specs=[vmem] * 6 + [any_space] * 6,
        out_specs=(any_space, vmem, vmem),
        scratch_shapes=[
            pltpu.VMEM((2, 2, BLK, NV), jnp.float32),
            *[pltpu.SMEM((4, 1, SLOTS), jnp.int32)] * 3,
            pltpu.SMEM((4, 1, 1), jnp.int32),
            pltpu.SMEM((4, 1, SLOTS), jnp.int32),
            pltpu.SMEM((2 * SLOTS + 8,), jnp.int32),
            pltpu.SMEM((4, NLAT), jnp.float32),
            pltpu.SemaphoreType.DMA((42,)),
        ],
        compiler_params=pltpu.CompilerParams(vmem_limit_bytes=5860 * 1024),
        name="product",
    )(GA, GE, GL, W, H0, H1, *lists)[0]


def body(hoppings, tile_rows, tile_cols, tile_lats, tile_counts, phase_angle, vectors):
    hop = hoppings[0]
    GA, GE, GL, W, H0, H1, waves, U, *lists = gather_all(phase_angle, hop, (tile_rows, tile_cols, tile_lats, tile_counts), vectors)
    return product(GA, GE, GL, W, H0, H1, (waves, U, *lists))


def solution(mesh):
    return jax.shard_map(
        body,
        mesh=mesh,
        in_specs=(
            P("rows", "ka", None, None),
            P("rows", "ka"),
            P("rows", "ka"),
            P("rows", "ka"),
            P("rows", "ka"),
            P("ka", None),
            P("ka", None, "rows", None),
        ),
        out_specs=P("ka", None, "rows", None),
        check_vma=False,
    )
```

```python
import functools

import jax
import jax.numpy as jnp
from jax import lax
from jax.experimental import pallas as pl
from jax.experimental.pallas import tpu as pltpu
from jax.sharding import PartitionSpec as P

MESH = pl.DeviceIdType.MESH
BAND = 16
NLAT = 9
TS = 128
NV = 256
TR = 3
BLK = TR * TS
SLOTS = 96
CHUNKS = 8
PER = SLOTS // CHUNKS
AROUND = 6
GATHER_VMEM = 2 * 1024 * 1024
GROUP = 4
DEPTH = 3
EARLY = 60
WIDE = 2 * BAND + 1
MATRIX = (TR, 2 * TS, WIDE * TS)
SPAN = WIDE + TR - 1
TORB = 96
HALVES = (0, 1)


class Net:
    def __init__(self, send_sem, recv_sem):
        self.send_sem, self.recv_sem = send_sem, recv_sem
        self.index, self.sent = {}, []

    def copy(self, name, src, dst, device):
        at = self.index.setdefault(name, len(self.index))
        return pltpu.make_async_remote_copy(
            src_ref=src, dst_ref=dst, send_sem=self.send_sem.at[at], recv_sem=self.recv_sem.at[at],
            device_id=device, device_id_type=MESH,
        )

    def send(self, name, when, src, dst, device):
        copy = self.copy(name, src, dst, device)
        self.sent.append((when, copy))
        guarded(when, copy.start)

    def recv(self, name, when, dst, device):
        guarded(when, self.copy(name, dst, dst, device).wait_recv)

    def finish(self):
        for when, copy in self.sent:
            guarded(when, copy.wait_send)


def guarded(when, action):
    if when is None:
        action()
    else:
        pl.when(when)(action)


def gather_kernel(
    angles, hop, rows, cols, lats, live, vec, GA, GE, GL, W, H0, H1, waves, U, CR, CC, CL, CN, S, X, E, R,
    phase, picks, factors, pick, factor, send_sem, recv_sem, local_sem,
):
    ka = lax.axis_index("ka")
    row = lax.axis_index("rows")
    xh, y, z = row // 16, (row // 4) % 4, row % 4
    zp, zm, z2 = (z + 1) % 4, (z + 3) % 4, (z + 2) % 4
    yp, ym = (y + 1) % 4, (y + 3) % 4

    def at(h, i, j):
        return (ka, h * 16 + i * 4 + j)

    def along(flip):
        other = (1 - ka % 2) if flip % 2 else ka % 2
        pair = (1 - ka // 2) if flip // 2 else ka // 2
        return (pair * 2 + other, row)

    up_z, down_z, up_y, down_y = at(xh, y, zp), at(xh, y, zm), at(xh, yp, z), at(xh, ym, z)
    mirror = at(1 - xh, y, z)
    low, high = z == 0, z == 3
    mid = (z == 1) | (z == 2)
    top, base = y == 3, y == 0
    down_y = at(jnp.where(base, 1 - xh, xh), ym, z)
    up_y = at(jnp.where(top, 1 - xh, xh), yp, z)
    inner_y = at(xh, jnp.where(base, 3, jnp.where(top, 0, y)), z)
    crossing = ((y == 1) & high) | ((y == 2) & low)
    part_sender = ((y == 1) & (z == 1)) | ((y == 2) & (z == 2))
    part_to = at(1 - xh, y, jnp.where(y == 1, 3, 0))
    part_from = at(1 - xh, y, jnp.where(y == 1, 1, 2))
    split = ((y == 1) & low) | ((y == 2) & high)
    outer = base | top
    beside_y = at(xh, jnp.where(y < 2, 1 - y, 5 - y), z)
    over = at(xh, jnp.where(y == 1, 0, 3), jnp.where(y == 1, 3, 0))
    over_from = at(xh, jnp.where(base, 1, 2), z)
    split_from = at(xh, jnp.where(base, 1, 2), 3 - z)
    relay = (base & high) | (top & low)
    relayed = (top & high) | (base & low)
    barrier = pltpu.get_barrier_semaphore()

    def greet(peer):
        pl.semaphore_signal(barrier, inc=1, device_id=peer, device_id_type=MESH)

    for peer in (along(1), along(2), along(3), up_z, down_z, up_y, down_y):
        greet(peer)
    pl.when(part_sender)(lambda: greet(part_to))
    pl.when(crossing)(lambda: greet(part_from))
    pl.when(crossing | split)(lambda: greet(mirror))
    pl.when(split)(lambda: greet(over))
    pl.when(relay)(lambda: greet(split_from))
    pl.when(relay | relayed)(lambda: greet(inner_y))
    extra = jnp.where(part_sender, 1, 0) + jnp.where(crossing | split, 2, 0)
    extra = extra + jnp.where(relay | relayed, 1, 0) + jnp.where(relay, 1, 0)
    pl.semaphore_wait(barrier, 7 + extra)

    def window(j, h, part=None):
        shift, size = (0, BLK) if part is None else (part.start, part.size)
        return W.at[h, :, pl.ds(pl.multiple_of((TR * j - 2) * TS + shift, TS), size)]

    net = Net(send_sem, recv_sem)
    send, recv = net.send, net.recv
    HEAD, LAST = pl.ds(0, TS), pl.ds(2 * TS, TS)

    def tail(first):
        return pl.ds(pl.multiple_of(jnp.where(first, 0, 2 * TS), TS), TS)

    lists = ((rows, CR), (cols, CC), (lats, CL), (live, CN))
    local = [pltpu.make_async_copy(src, dst.at[0], local_sem.at[i]) for i, (src, dst) in enumerate(lists)]
    local += [pltpu.make_async_copy(vec.at[h], window(6, h), local_sem.at[4 + h]) for h in HALVES]
    local.append(pltpu.make_async_copy(angles, phase, local_sem.at[9]))
    local.append(pltpu.make_async_copy(hop, GA.at[pl.ds(0, SLOTS)], local_sem.at[6]))
    for copy in local:
        copy.start()

    member = {0: z, -1: zm, 1: zp, 2: z2}

    def y_sends(u, h, only=None):
        dz = member[u] - z
        src = vec.at[h] if u == 0 else window(6 + dz, h)
        down_dst, up_dst = window(10 + dz, h), window(2 + dz, h)
        down_ok, up_ok = (None, None) if u == 0 else (y > 0, y < 3)
        if only is not None:
            down_ok, up_ok = down_ok & only, up_ok & only
        if u == 2:
            send(f"y-{u}{h}", down_ok & (z >= 2), src, down_dst, down_y)
            send(f"y-{u}{h}", down_ok & (z < 2), src.at[:, HEAD], window(10 + dz, h, HEAD), down_y)
            send(f"y+{u}{h}", up_ok & (z < 2), src, up_dst, up_y)
            send(f"y+{u}{h}", up_ok & (z >= 2), src.at[:, LAST], window(2 + dz, h, LAST), up_y)
        else:
            send(f"y-{u}{h}", down_ok & (z != 0) if u == -1 else down_ok, src, down_dst, down_y)
            send(f"y+{u}{h}", up_ok & (z != 3) if u == 1 else up_ok, src, up_dst, up_y)

    def y_recvs(u, h):
        dz = member[u] - z
        down_dst, up_dst = window(10 + dz, h), window(2 + dz, h)
        down_ok, up_ok = (None, None) if u == 0 else (y < 3, y > 0)
        if u == 2:
            recv(f"y-{u}{h}", down_ok & (z >= 2), down_dst, up_y)
            recv(f"y-{u}{h}", down_ok & (z < 2), window(10 + dz, h, HEAD), up_y)
            recv(f"y+{u}{h}", up_ok & (z < 2), up_dst, down_y)
            recv(f"y+{u}{h}", up_ok & (z >= 2), window(2 + dz, h, LAST), down_y)
        else:
            recv(f"y-{u}{h}", down_ok & (z != 0) if u == -1 else down_ok, down_dst, up_y)
            recv(f"y+{u}{h}", up_ok & (z != 3) if u == 1 else up_ok, up_dst, down_y)

    def both(when, ok):
        return ok if when is None else when & ok

    def spread(h):
        a, b = (None, None) if h else (top, base)
        send(f"a1{h}", both(a, z < 3), window(10, h), window(9, h), up_z)
        send(f"b1{h}", both(b, z > 0), window(2, h), window(3, h), down_z)
        send(f"a2{h}", a, window(10, h), window(jnp.where(low, 7, 11), h), down_z)
        send(f"b2{h}", b, window(2, h), window(jnp.where(high, 5, 1), h), up_z)

    def spread_on(h):
        a, b = (None, None) if h else (top, base)
        recv(f"a1{h}", both(a, z > 0), window(9, h), down_z)
        recv(f"b1{h}", both(b, z < 3), window(3, h), up_z)
        recv(f"a2{h}", a, window(jnp.where(high, 7, 11), h), up_z)
        recv(f"b2{h}", b, window(jnp.where(low, 5, 1), h), down_z)
        if h:
            send(f"a3{h}", mid, window(9, h), window(8, h), up_z)
            send(f"b3{h}", mid, window(3, h), window(4, h), down_z)
        else:
            send(f"a3{h}", both(a, low | high), window(jnp.where(low, 11, 7), h), window(8, h), down_z)
            send(f"b3{h}", both(b, low | high), window(jnp.where(low, 5, 1), h), window(4, h), up_z)
        send(f"a4{h}", both(a, mid), window(11, h, HEAD), window(12, h, HEAD), down_z)
        send(f"b4{h}", both(b, mid), window(1, h, LAST), window(0, h, LAST), up_z)

    def spread_last(h):
        a, b = (None, None) if h else (top, base)
        recv(f"a3{h}", both(a, z >= 2), window(8, h), down_z)
        recv(f"b3{h}", both(b, z < 2), window(4, h), down_z)
        recv(f"a4{h}", both(a, z < 2), window(12, h, HEAD), up_z)
        recv(f"b4{h}", both(b, z >= 2), window(0, h, LAST), down_z)

    near_to, near_from = (low & (y > 0)) | (high & (y < 3)), (low & (y < 3)) | (high & (y > 0))
    near = at(xh, jnp.where(low, ym, yp), z)
    near_src = at(xh, jnp.where(low, yp, ym), z)
    across = at(xh, y, jnp.where(low, 3, 0))
    across_from = (high & (y < 3)) | (low & (y > 0))
    block, beside = jnp.where(low, 10, 2), jnp.where(low, 11, 1)
    far, far_part = jnp.where(low, 11, 1), jnp.where(low, 12, 0)
    got, got_part = jnp.where(low, 1, 11), jnp.where(low, 0, 12)

    def second(h):
        send(f"d{h}", near_to, window(block, h), X.at[0, h], near)

    def second_part(h, ok):
        send(f"dp{h}", near_to & ok, window(beside, h, tail(low)), X.at[1, h, :, tail(low)], near)

    crossed = jnp.where(y == 1, 3, 9)

    def cross():
        send("g0", crossing, window(crossed, 0), S.at[0, 0], mirror)

    y_sends(0, 1)
    send("z-0", None, vec.at[0], window(6 + z - zp, 0), up_z)
    send("z+1", None, vec.at[1], window(6 + z - zm, 1), down_z)
    y_sends(0, 0)
    send("z-1", None, vec.at[1], window(6 + z - zp, 1), up_z)
    send("z+0", None, vec.at[0], window(6 + z - zm, 0), down_z)
    for h in HALVES:
        send(f"gp{h}", part_sender, vec.at[h, :, tail(y == 1)], S.at[1, h, :, tail(y == 1)], part_to)

    def remote(n, part):
        if part.start < EARLY:
            return GE.at[pl.ds(n * EARLY + part.start, part.size)]
        return GL.at[n, pl.ds(part.start - EARLY, part.size)]

    def pieces(c):
        if c < CHUNKS - 1:
            return ((f"{c}", None, pl.ds(c * PER, PER)),)
        end = SLOTS - AROUND
        return (("e", None, pl.ds(c * PER, end - c * PER)), ("f", ~outer, pl.ds(end, AROUND)))

    def chunk(c):
        for name, when, part in pieces(c):
            send(f"x{name}", when, hop.at[part], remote(0, part), along(2))

    def forward(c):
        for name, when, part in pieces(c):
            recv(f"x{name}", when, remote(0, part), along(2))
            send(f"o{name}", when, remote(0, part), remote(1, part), along(1))

    around = pl.ds(SLOTS - AROUND, AROUND)
    send("g1", split, vec.at[1], S.at[0, 1], mirror)
    send("r", outer, hop.at[around], R.at[0], beside_y)
    for c in range(3):
        chunk(c)
    for flip in (1, 2, 3):
        for i, (src, dst) in enumerate(lists):
            send(f"c{flip}{i}", None, src, dst.at[flip], along(flip))
    send("sib", None, hop, GA.at[pl.ds(SLOTS, SLOTS)], along(1))

    def ranked(pair, extent, depth):
        none = 2 * extent
        blocks = lax.broadcasted_iota(jnp.int32, (TS, SLOTS), 0)
        place = lax.broadcasted_iota(jnp.int32, (TS, SLOTS), 1)
        wave = (jnp.cos(phase[...]), jnp.sin(phase[...]))
        waves[0:2, :], waves[2:4, :] = wave
        found, scales = [], []
        for n, m in enumerate(pair):
            r = CR[m] - row * TR
            w = CC[m] - (row * TR + r - BAND)
            w = jnp.where(w < 0, w + TORB, w)
            w = jnp.where(w >= TORB, w - TORB, w)
            b = jnp.where(place[:1] < jnp.minimum(CN[m], extent), r * WIDE + w, -1)
            found.append(jnp.where(blocks == b, place + n * extent, none))
            scales.append(
                [
                    sum(jnp.where(CL[m] == v, wave[p][k : k + 1, v : v + 1], 0.0) for v in range(NLAT))
                    for k in range(2)
                    for p in range(2)
                ]
            )
        lane = lax.broadcasted_iota(jnp.int32, (TS, TS), 1)
        chosen, scaled = jnp.zeros((TS, TS), jnp.int32), jnp.zeros((TS, TS), jnp.float32)
        used = [jnp.zeros((TS, SLOTS), jnp.int32)] * 2
        for d in range(depth):
            best = [jnp.min(f, axis=1, keepdims=True) for f in found]
            best = jnp.minimum(best[0], best[1])
            hits = [(f == best) & (f < none) for f in found]
            chosen = jnp.where(lane == d, jnp.where(best < none, best, 0), chosen)
            for j in range(4):
                total = sum(
                    jnp.sum(jnp.where(hits[m], scales[m][j], 0.0), axis=1, keepdims=True) for m in range(2)
                )
                scaled = jnp.where(lane == 4 * d + j, total, scaled)
            used = [jnp.where(hits[m], 1, used[m]) for m in range(2)]
            found = [jnp.where(hits[m], none, found[m]) for m in range(2)]
        picks[...] = chosen
        factors[...] = scaled
        for n, m in enumerate(pair):
            U[m] = jnp.max(used[n], axis=0, keepdims=True)

    tables = [
        pltpu.make_async_copy(picks, pick, local_sem.at[7]),
        pltpu.make_async_copy(factors, factor, local_sem.at[8]),
    ]

    def fill(b, source, depth, more):
        r = b // WIDE
        columns = pl.ds(pl.multiple_of((b - r * WIDE) * TS, TS), TS)
        chosen = [pick[b, d] for d in range(depth)]
        scale = [[factor[b, 4 * d + j] for j in range(4)] for d in range(depth)]
        size = 32
        for at_row in range(0, TS, size):
            tiles = [source[c, pl.ds(at_row, size), :].astype(jnp.float32) for c in chosen]
            for k in range(2):
                for p in range(2):
                    total = tiles[0] * scale[0][2 * k + p]
                    for d in range(1, depth):
                        total += tiles[d] * scale[d][2 * k + p]
                    where = (r, pl.ds(p * TS + at_row, size), columns)
                    if more:
                        total += (H0, H1)[k][where]
                    (H0, H1)[k][where] = total
        return 0

    filled = [0]

    def some(count):
        start, filled[0] = filled[0], min(filled[0] + count, TR * WIDE)
        lax.fori_loop(start, filled[0], lambda b, _: fill(b, GA, DEPTH, False), 0)

    recv("z-0", None, window(6 + zm - z, 0), down_z)
    send("w0", None, window(6 + zm - z, 0), window(6 + zm - zp, 0), up_z)
    y_sends(-1, 0)
    recv("z+1", None, window(6 + zp - z, 1), up_z)
    send("w1", None, window(6 + zp - z, 1), window(6 + zp - zm, 1), down_z)
    recv("g1", split, S.at[0, 1], mirror)
    send("e1", split, S.at[0, 1], E.at[0, 1], over)
    y_recvs(0, 1)
    spread(1)
    second(1)
    for i, (_, dst) in enumerate(lists):
        recv(f"c1{i}", None, dst.at[1], along(1))
    recv("sib", None, GA.at[pl.ds(SLOTS, SLOTS)], along(1))
    for copy in local:
        copy.wait()
    ranked((0, 1), SLOTS, DEPTH)
    for copy in tables:
        copy.start()
    recv("z+0", None, window(6 + zp - z, 0), up_z)
    y_sends(1, 0)
    recv("z-1", None, window(6 + zm - z, 1), down_z)
    cross()
    recv("r", ~outer, R.at[0], beside_y)
    send("q", ~outer, R.at[0], R.at[1], along(2))
    for c in range(3, CHUNKS):
        chunk(c)
    for copy in tables:
        copy.wait()
    some(10)
    y_recvs(0, 0)
    second(0)
    spread(0)
    some(10)
    recv("w0", None, window(6 + z2 - z, 0), down_z)
    y_sends(2, 0, ~crossing)
    some(10)
    recv("w1", None, window(6 + z2 - z, 1), up_z)
    for h in (1, 0):
        recv(f"d{h}", near_from, X.at[0, h], near_src)
        send(f"f{h}", near_from, X.at[0, h], window(far, h), across)
    some(10)
    recv("g0", crossing, S.at[0, 0], mirror)
    send("e0", crossing, S.at[0, 0], E.at[0, 0], beside_y)
    y_sends(2, 0, crossing)
    for h in HALVES:
        recv(f"gp{h}", crossing, S.at[1, h, :, tail(y == 1)], part_from)
        send(f"ep{h}", crossing, S.at[1, h, :, tail(y == 1)], E.at[1, h, :, tail(y == 1)], beside_y)
    def onward(h):
        recv(f"e{h}", relay, E.at[0, h], split_from if h else over_from)
        send(f"f{h}", relay, E.at[0, h], window(got, h), inner_y)

    def onward_part(h):
        recv(f"ep{h}", relay, E.at[1, h, :, tail(high)], over_from)
        send(f"fp{h}", relay, E.at[1, h, :, tail(high)], window(got_part, h, tail(high)), inner_y)

    some(10)
    y_recvs(-1, 0)
    y_recvs(1, 0)
    second_part(0, (low & (y < 3)) | (high & (y > 0)))
    spread_on(1)
    second_part(1, low | high)
    some(10)
    onward(1)
    onward(0)
    some(10)
    spread_on(0)
    second_part(0, (low & top) | (high & base))
    for h in HALVES:
        onward_part(h)
    some(10)
    recv("q", ~outer, R.at[1], along(2))
    send("p", ~outer, R.at[1], remote(0, around), beside_y)
    for c in range(3):
        forward(c)
    some(TR * WIDE)
    for h in HALVES:
        recv(f"dp{h}", near_from, X.at[1, h, :, tail(low)], near_src)
        send(f"fp{h}", near_from, X.at[1, h, :, tail(low)], window(far_part, h, tail(low)), across)
    rim = low | high
    next_to = at(xh, y, jnp.where(low, 1, 2))
    for h in (1, 0):
        recv(f"f{h}", rim, window(got, h), across)
        send(f"l{h}", rim, window(got, h, tail(high)), window(got_part, h, tail(high)), next_to)
    for c in range(3, EARLY // PER):
        forward(c)
    for flip in (2, 3):
        for i, (_, dst) in enumerate(lists):
            recv(f"c{flip}{i}", None, dst.at[flip], along(flip))
    for c in range(EARLY // PER):
        for name, _, part in pieces(c):
            recv(f"o{name}", None, remote(1, part), along(1))

    @pl.when(relay)
    def _():
        for m in (2, 3):
            U[m] = jnp.zeros((1, SLOTS), jnp.int32)

    @pl.when(~relay)
    def _():
        ranked((2, 3), EARLY, DEPTH - 1)
        for copy in tables:
            copy.start()
        for copy in tables:
            copy.wait()
        lax.fori_loop(0, TR * WIDE, lambda b, _: fill(b, GE, DEPTH - 1, True), 0)

    for c in range(EARLY // PER, CHUNKS - 2):
        forward(c)
    y_recvs(2, 0)
    for h in HALVES:
        spread_last(h)
        recv(f"fp{h}", rim, window(got_part, h, tail(high)), across)
        recv(f"l{h}", mid, window(jnp.where(z == 1, 0, 12), h, tail(z == 2)), at(xh, y, jnp.where(z == 1, 0, 3)))
    recv("p", outer, remote(0, around), beside_y)
    send("of", outer, remote(0, around), remote(1, around), along(1))
    for c in range(CHUNKS - 2, CHUNKS):
        forward(c)
    for c in range(EARLY // PER, CHUNKS):
        for name, _, part in pieces(c):
            recv(f"o{name}", None, remote(1, part), along(1))
    net.finish()


def gather_all(phase, hop, lists, vec):
    block = vec.shape
    any_space = pl.BlockSpec(memory_space=pl.ANY)
    vmem = pl.BlockSpec(memory_space=pltpu.VMEM)
    sems = 104
    return pl.pallas_call(
        gather_kernel,
        out_shape=(
            pltpu.VMEM((2 * SLOTS,) + hop.shape[1:], hop.dtype),
            pltpu.VMEM((2 * EARLY,) + hop.shape[1:], hop.dtype),
            pltpu.VMEM((2, SLOTS - EARLY) + hop.shape[1:], hop.dtype),
            pltpu.VMEM(block[:2] + (SPAN * TS,) + block[3:], vec.dtype),
            *[pltpu.VMEM(MATRIX, jnp.float32)] * 2,
            pltpu.VMEM((4, NLAT), jnp.float32),
            pltpu.VMEM((4, 1, SLOTS), jnp.int32),
            *[pltpu.VMEM((4,) + a.shape, a.dtype) for a in lists],
            *[pltpu.HBM((2,) + block, vec.dtype)] * 3,
            pltpu.HBM((2, AROUND) + hop.shape[1:], hop.dtype),
        ),
        in_specs=[pl.BlockSpec(memory_space=pltpu.HBM)] * 7,
        out_specs=(vmem,) * 2 + (any_space,) * 2 + (vmem,) * 8 + (any_space,) * 4,
        scratch_shapes=[
            pltpu.VMEM(phase.shape, phase.dtype),
            pltpu.VMEM((TS, TS), jnp.int32),
            pltpu.VMEM((TS, TS), jnp.float32),
            pltpu.SMEM((TS, TS), jnp.int32),
            pltpu.SMEM((TS, TS), jnp.float32),
            pltpu.SemaphoreType.DMA((sems,)),
            pltpu.SemaphoreType.DMA((sems,)),
            pltpu.SemaphoreType.DMA((10,)),
        ],
        compiler_params=pltpu.CompilerParams(
            collective_id=0, has_side_effects=True, vmem_limit_bytes=GATHER_VMEM
        ),
        name="gather",
    )(*[a if a.size == 1 else pltpu.with_memory_space_constraint(a, pltpu.HBM) for a in (phase, hop, *lists, vec)])[:12]


def product_kernel(GA, GE, GL, W, Z0, Z1, waves, U, CR, CC, CL, CN, out, H0, H1, O, NR, NC, NL, NN, NU, rest, table, sems):
    row = lax.axis_index("rows")
    H = (H0, H1)
    scalars = [
        pltpu.make_async_copy(src, dst, sems.at[30 + i])
        for i, (src, dst) in enumerate(((CR, NR), (CC, NC), (CL, NL), (CN, NN), (U, NU), (waves, table)))
    ]
    for copy in scalars:
        copy.start()
    for copy in scalars:
        copy.wait()
    part = 32
    def passed(pair, extent):
        count = 0
        for m in pair:

            def keep(i, n, m=m):
                rest[n] = m * SLOTS + i
                return n + 1 - NU[m, 0, i]

            count = lax.fori_loop(0, jnp.minimum(NN[m, 0, 0], extent), keep, count)
        return count

    for group in range(4):
        if group < 2:
            count = passed((2 * group, 2 * group + 1), (SLOTS, EARLY)[group])
        else:
            count = jnp.maximum(NN[group, 0, 0] - EARLY, 0)

        def add(i, _, group=group, count=count):
            for one in [GROUP * i + j for j in range(GROUP)]:
                if group < 2:
                    slot = jnp.where(one < count, rest[one], 2 * group * SLOTS)
                    n = jnp.where(slot >= (2 * group + 1) * SLOTS, 2 * group + 1, 2 * group)
                    item = slot - n * SLOTS
                    tiles = GE.at[item + (n - 2) * EARLY] if group else GA.at[slot]
                else:
                    late = jnp.minimum(one, SLOTS - EARLY - 1)
                    n, item, tiles = group, late + EARLY, GL.at[group - 2, late]
                r = jnp.clip(NR[n, 0, item] - row * TR, 0, TR - 1)
                w = NC[n, 0, item] - (row * TR + r - BAND)
                w = jnp.where(w < 0, w + TORB, w)
                w = jnp.clip(jnp.where(w >= TORB, w - TORB, w), 0, WIDE - 1)
                cols = pl.ds(pl.multiple_of(w * TS, TS), TS)
                lat = NL[n, 0, item]
                scale = [jnp.where(one < count, table[2 * p + k, lat], 0.0) for k in range(2) for p in range(2)]
                for at in range(0, TS, part):
                    tile = tiles[pl.ds(at, part), :].astype(jnp.float32)
                    for k in range(2):
                        for p in range(2):
                            H[k][r, pl.ds(p * TS + at, part), cols] += tile * scale[2 * k + p]
            return 0

        lax.fori_loop(0, (count + GROUP - 1) // GROUP, add, 0)
    done = []
    for k in range(2):
        for r in range(TR):
            left = H[k][r].astype(jnp.bfloat16)
            rows = pl.ds(r * TS, TS)
            o = [
                jnp.dot(
                    left,
                    W[k, q, r * TS : (r + WIDE) * TS, :],
                    preferred_element_type=jnp.float32,
                )
                for q in range(2)
            ]
            O[k, 0, rows, :] = o[0][:TS] - o[1][TS:]
            O[k, 1, rows, :] = o[1][:TS] + o[0][TS:]
            done.append(pltpu.make_async_copy(O.at[k, :, rows], out.at[k, :, rows], sems.at[36 + TR * k + r]))
            done[-1].start()
    for copy in done:
        copy.wait()


def product(GA, GE, GL, W, H0, H1, lists):
    any_space = pl.BlockSpec(memory_space=pl.ANY)
    vmem = pl.BlockSpec(memory_space=pltpu.VMEM)
    return pl.pallas_call(
        product_kernel,
        out_shape=(jax.ShapeDtypeStruct((2, 2, BLK, NV), jnp.float32),) + (pltpu.VMEM(MATRIX, jnp.float32),) * 2,
        input_output_aliases={4: 1, 5: 2},
        in_specs=[vmem] * 6 + [any_space] * 6,
        out_specs=(any_space, vmem, vmem),
        scratch_shapes=[
            pltpu.VMEM((2, 2, BLK, NV), jnp.float32),
            *[pltpu.SMEM((4, 1, SLOTS), jnp.int32)] * 3,
            pltpu.SMEM((4, 1, 1), jnp.int32),
            pltpu.SMEM((4, 1, SLOTS), jnp.int32),
            pltpu.SMEM((2 * SLOTS + 8,), jnp.int32),
            pltpu.SMEM((4, NLAT), jnp.float32),
            pltpu.SemaphoreType.DMA((42,)),
        ],
        compiler_params=pltpu.CompilerParams(vmem_limit_bytes=5860 * 1024),
        name="product",
    )(GA, GE, GL, W, H0, H1, *lists)[0]


def body(hoppings, tile_rows, tile_cols, tile_lats, tile_counts, phase_angle, vectors):
    hop = hoppings[0]
    GA, GE, GL, W, H0, H1, waves, U, *lists = gather_all(phase_angle, hop, (tile_rows, tile_cols, tile_lats, tile_counts), vectors)
    return product(GA, GE, GL, W, H0, H1, (waves, U, *lists))


def solution(mesh):
    return jax.shard_map(
        body,
        mesh=mesh,
        in_specs=(
            P("rows", "ka", None, None),
            P("rows", "ka"),
            P("rows", "ka"),
            P("rows", "ka"),
            P("rows", "ka"),
            P("ka", None),
            P("ka", None, "rows", None),
        ),
        out_specs=P("ka", None, "rows", None),
        check_vma=False,
    )
```
